32 devices in a mesh: tok: 8 (over y, x, core), blk: 4 (over z).
Axes of the slice: x: 2, y: 2, z: 4, core: 2. Of those that a mesh axis runs over, the one named last changes fastest.
Arguments:
- activations: bfloat16 [4096, 4096], P('tok', 'blk'), may hold values from -52 to 52, as said below
- out_grads: bfloat16 [4096, 4096], P('tok', 'blk'), may hold values from -52 to 52, as said below
Outputs:
- act_inverse: float32 [4096, 4096], P(('tok', 'blk'))
- grad_inverse: float32 [4096, 4096], P(('tok', 'blk'))
The draws below stay inside these ranges and needn't reach their ends.
Inputs may be any that keep to these rules, and one draw needn't show every extreme that they name: `activations`: real entries. `out_grads`: real entries.
All inputs are finite; a program needn't handle non-finite values.
Results may differ from the reference program's by a relative error of at most 0.02.
Values may be sent and summed in bfloat16 or wider, within the bound.
A program may use at most 64 MiB of HBM per device.

```python
import jax
import jax.numpy as jnp
from jax import lax

D = 4096
TOK_DEV = 512
TOKENS = 4096
N_TOK = 8


def scaled_draw(key):
    row_key, col_key, value_key = jax.random.split(key, 3)
    positions = jnp.arange(TOKENS, dtype=jnp.float32) / TOKENS
    values = jax.random.truncated_normal(value_key, -5.0, 5.0, (TOKENS, D), jnp.float32)
    row_scale = jnp.exp(jax.random.uniform(row_key, (TOKENS, 1), jnp.float32, 0.0, jnp.log(3.0)))
    ramp = jnp.exp(positions * 0.5 * jnp.log(3.0))
    col_scale = jnp.exp(jax.random.uniform(col_key, (1, D), jnp.float32, 0.0, jnp.log(10.0)))
    return values * row_scale * ramp[:, None] * col_scale / 10.0


def draw_activations(key, part):
    return scaled_draw(jax.random.fold_in(key, 11)).astype(jnp.bfloat16)


def draw_out_grads(key, part):
    return scaled_draw(jax.random.fold_in(key, 23)).astype(jnp.bfloat16)


def setup_inputs(seed: int = 0) -> dict:
    streams_of = jax.random.split(jax.random.key(seed), 3)
    activations = draw_activations(jax.random.fold_in(streams_of[2], 71), 0)
    out_grads = draw_out_grads(jax.random.fold_in(streams_of[2], 71), 0)
    return dict(activations=activations, out_grads=out_grads)


damping = 0.3
epsilon = 1e-06
divisor = 2.0

def factor_gram(data):
    shards = data.reshape(N_TOK, TOK_DEV, D)

    def add_shard(total, shard):
        partial_value = jnp.dot(shard.T, shard, preferred_element_type=jnp.float32)
        rounded = lax.optimization_barrier(partial_value.astype(jnp.bfloat16))
        return (total + rounded.astype(jnp.float32), None)
    total, unused = lax.scan(add_shard, jnp.zeros((D, D), jnp.float32), shards)
    return total

def factor_inverse(data):
    gram = factor_gram(data)
    values = data.astype(jnp.float32)
    sums = lax.optimization_barrier(jnp.sum(values * values, axis=0))
    inverse = lax.rsqrt(sums / TOKENS + epsilon)
    identity = jnp.eye(D, dtype=jnp.float32)
    damped = gram / TOKENS * inverse[:, None] * inverse[None, :] + damping * identity
    scaled = damped / divisor
    half = scaled.astype(jnp.bfloat16)
    square = jnp.dot(half, half, preferred_element_type=jnp.float32)
    cube = jnp.dot(half, square.astype(jnp.bfloat16), preferred_element_type=jnp.float32)
    return 4.0 * identity - 6.0 * scaled + 4.0 * square - cube

def reference(activations, out_grads):
    return (factor_inverse(activations), factor_inverse(out_grads))
```

```python
import functools

import jax
import jax.numpy as jnp
import numpy as np
from jax import lax
from jax.experimental import pallas as pl
from jax.experimental.pallas import tpu as pltpu
from jax.sharding import PartitionSpec as P

damping = 0.3
epsilon = 1e-06
divisor = 2.0
gathered_budget = 32 * 1024 * 1024
LANES = 128
MESH = pl.DeviceIdType.MESH


def column_squares(data):
    values = data.astype(jnp.float32)
    return jnp.sum(values * values, axis=0)


def fold_product(row_block, tile):
    return jnp.dot(
        row_block,
        lax.all_gather(tile, "tok", axis=0, tiled=True),
        preferred_element_type=jnp.float32,
    )


def newton_steps(scaled, identity):
    half = scaled.astype(jnp.bfloat16)
    row_block = lax.all_gather(half, "blk", axis=1, tiled=True)
    square = fold_product(row_block, half)
    cube = fold_product(row_block, square.astype(jnp.bfloat16))
    return 4.0 * identity - 6.0 * scaled + 4.0 * square - cube


def tiled_body(activations, out_grads):
    tok_count = lax.axis_size("tok")
    blk_count = lax.axis_size("blk")
    tok_id = lax.axis_index("tok")
    blk_id = lax.axis_index("blk")
    token_count = activations.shape[0] * tok_count
    tile_cols = activations.shape[1]
    tile_rows = tile_cols * blk_count // tok_count
    row_ids = tok_id * tile_rows + jnp.arange(tile_rows, dtype=jnp.int32)
    col_ids = blk_id * tile_cols + jnp.arange(tile_cols, dtype=jnp.int32)
    identity = (row_ids[:, None] == col_ids[None, :]).astype(jnp.float32)

    def inverse_tile(local):
        full = lax.all_gather(local, "blk", axis=1, tiled=True)
        sums = lax.psum(column_squares(full).astype(jnp.bfloat16), "tok").astype(jnp.float32)
        gram_tile = lax.psum_scatter(
            lax.dot_general(
                full, local, (((0,), (0,)), ((), ())), preferred_element_type=jnp.float32
            ).astype(jnp.bfloat16),
            "tok",
            scatter_dimension=0,
            tiled=True,
        ).astype(jnp.float32)
        inverse = lax.rsqrt(sums / token_count + epsilon)
        inverse_rows = lax.dynamic_slice_in_dim(inverse, tok_id * tile_rows, tile_rows)
        inverse_cols = lax.dynamic_slice_in_dim(inverse, blk_id * tile_cols, tile_cols)
        damped = (
            gram_tile / token_count * inverse_rows[:, None] * inverse_cols[None, :]
            + damping * identity
        )
        result_tile = newton_steps(damped / divisor, identity)
        return lax.all_to_all(
            result_tile.astype(jnp.bfloat16), "blk", split_axis=0, concat_axis=1, tiled=True
        ).astype(result_tile.dtype)

    return inverse_tile(activations), inverse_tile(out_grads)


DIRECT = {
    (0, 0): (0, 0), (0, 1): (0, 1), (0, 3): (0, 2), (1, 3): (0, 3), (3, 3): (0, 4),
    (1, 1): (1, 0), (1, 2): (1, 1), (2, 0): (1, 2), (2, 3): (1, 3), (2, 2): (1, 4),
}
TASKS = 5
CUTS = 4
LAG = 4


def pick(index, values):
    out = values[-1]
    for i in range(len(values) - 2, -1, -1):
        out = jnp.where(index == i, values[i], out)
    return out


def remote(src, dst, send, recv, device):
    return pltpu.make_async_remote_copy(
        src_ref=src, dst_ref=dst, send_sem=send, recv_sem=recv,
        device_id=device, device_id_type=MESH,
    )


def meet(peers):
    barrier = pltpu.get_barrier_semaphore()
    for peer in peers:
        pl.semaphore_signal(barrier, inc=1, device_id=peer, device_id_type=MESH)
    pl.semaphore_wait(barrier, len(peers))


def gram_kernel(
    tok, blk, acts, grads, out,
    x, other, passed, turned, part, first_in, second_out, second_in, keep,
    load_sem, near_send, near_recv, pass_send, pass_recv, core_send, core_recv,
    one_send, one_recv, two_send, two_recv,
):
    t = lax.axis_index("tok")
    b = lax.axis_index("blk")
    low = b < blk // 2
    place = jnp.where(low, b, blk - 1 - b)
    outer = place == 0
    inner = place == 1
    core, col, row = t % 2, t // 2 % 2, t // 4
    mate = (jnp.bitwise_xor(t, 1), b)
    beside = (jnp.bitwise_xor(t, 2), b)
    below = (jnp.bitwise_xor(t, 4), b)
    near = (t, jnp.bitwise_xor(b, 1))
    facing = (t, blk - 1 - b)
    depth, feats = other.shape
    wide = feats // CUTS
    halfway = feats // 2
    count = TASKS * CUTS

    def load(ref, dst, index):
        return pltpu.make_async_copy(ref, dst, load_sem.at[index])

    @pl.when(low)
    def _():
        load(acts, x.at[place, core], 0).start()
        load(grads, other, 1).start()

    @pl.when(jnp.logical_not(low))
    def _():
        load(grads, x.at[place, core], 0).start()
        load(acts, other, 1).start()

    meet([mate, beside, below, near, facing])
    load(acts, x.at[place, core], 0).wait()
    load(grads, other, 1).wait()

    def columns(h):
        return pl.ds(h * wide, wide)

    def to_mate(label, h):
        here = x.at[label, core, :, columns(h)]
        return remote(
            here, here, core_send.at[label, h], core_recv.at[label, h], mate
        )

    def from_mate(label, h):
        there = x.at[label, 1 - core, :, columns(h)]
        return remote(
            there, there, core_send.at[label, h], core_recv.at[label, h], mate
        )

    def along(label, h, src, device):
        return remote(
            src, x.at[label, core, :, columns(h)],
            near_send.at[label, h], near_recv.at[label, h], device,
        )

    def arrived(label, h):
        here = x.at[label, core, :, columns(h)]
        return remote(here, here, near_send.at[label, h], near_recv.at[label, h], near)

    def give(h):
        return remote(
            other.at[:, columns(h)], passed.at[:, columns(h)],
            pass_send.at[h], pass_recv.at[h], near,
        )

    def onward(h):
        return remote(
            passed.at[:, columns(h)], x.at[3, core, :, columns(h)],
            pass_send.at[h], near_recv.at[3, h], facing,
        )

    for h in range(CUTS):
        to_mate(place, h).start()

    @pl.when(outer)
    def _():
        for h in range(CUTS):
            give(h).start()
        for h in range(CUTS):
            along(0, h, x.at[0, core, :, columns(h)], near).start()

    @pl.when(inner)
    def _():
        for h in range(CUTS):
            along(1, h, x.at[1, core, :, columns(h)], near).start()
            along(2, h, other.at[:, columns(h)], facing).start()

    def turn(slot, label):
        for c in range(2):
            for r in range(0, depth, 256):
                turned[slot, :, c * depth + r : c * depth + r + 256] = x[
                    label, c, r : r + 256, pl.ds(pl.multiple_of(core * halfway, LANES), halfway)
                ].T

    def share(label, h):
        arrived(label, h).wait_recv()
        to_mate(label, h).start()

    def piece(n):
        late = n - jnp.where(outer, 2, 3) * CUTS
        pairs = late // 2
        paired = jnp.where(outer, (n >= 2 * CUTS) & (n < 4 * CUTS), n >= 3 * CUTS)
        task = jnp.where(paired, 2 + late % 2, jnp.where(n < 2 * CUTS, n // CUTS, 4))
        h = jnp.where(paired, pairs, n % CUTS)
        slot = jnp.where(outer, pick(task, [0, 0, 0, 1, 2]), pick(task, [0, 0, 1, 1, 1]))
        label = jnp.where(outer, pick(task, [0, 1, 3, 3, 3]), pick(task, [1, 2, 0, 3, 2]))
        return task, h, slot, label

    def one(n, side):
        if side == 0:
            src, device = part.at[n, :, 1 - col, :, pl.ds(0, wide // 2)], beside
        else:
            src, device = part.at[n, 1 - row, :, :, pl.ds(wide // 2, wide // 2)], below
        return remote(
            src, first_in.at[n, side], one_send.at[n, side], one_recv.at[n, side], device
        )

    def two(n, side):
        return remote(
            second_out.at[n, side], second_in.at[n, side],
            two_send.at[n, side], two_recv.at[n, side], below if side == 0 else beside,
        )

    for h in range(CUTS):
        from_mate(place, h).wait_recv()
    turn(0, place)

    @pl.loop(0, count + 2 * LAG)
    def _(n):
        @pl.when(n == CUTS)
        def _():
            @pl.when(inner)
            def _():
                for h in range(CUTS):
                    give(h).wait_recv()
                    onward(h).start()

            label = place + 1
            for h in range(CUTS):
                share(label, h)
            for h in range(CUTS):
                from_mate(label, h).wait_recv()
            turn(1, label)

        late = n - jnp.where(outer, 2, 3) * CUTS
        paired = jnp.where(outer, (n >= 2 * CUTS) & (n < 4 * CUTS), n >= 3 * CUTS)

        @pl.when(paired & (late % 2 == 0) & (n < count))
        def _():
            h = late // 2
            arrived(3, h).wait_recv()
            to_mate(3, h).start()

            @pl.when(inner)
            def _():
                along(3, h, x.at[3, core, :, columns(h)], near).start()
                share(0, h)
                from_mate(0, h).wait_recv()

            from_mate(3, h).wait_recv()

        @pl.when(outer & (n == 4 * CUTS))
        def _():
            turn(2, 3)

        @pl.when(n < count)
        def _():
            task, h, slot, label = piece(n)
            at = pl.ds(pl.multiple_of(h * wide, LANES), wide)
            right = x[label, :, :, at].reshape(2 * depth, wide)
            product = jnp.dot(turned[slot], right, preferred_element_type=jnp.float32)
            part[n] = product.astype(jnp.bfloat16).reshape(2, 2, LANES, wide)
            one(n, 0).start()
            one(n, 1).start()

        @pl.when((n >= LAG) & (n < count + LAG))
        def _():
            m = n - LAG
            left, right = pl.ds(0, wide // 2), pl.ds(wide // 2, wide // 2)
            one(m, 0).wait_recv()
            one(m, 1).wait_recv()
            wider = jnp.float32
            second_out[m, 0] = (
                part[m, 1 - row, col, :, left].astype(wider)
                + first_in[m, 0, 1 - row].astype(wider)
            ).astype(jnp.bfloat16)
            second_out[m, 1] = (
                part[m, row, 1 - col, :, right].astype(wider)
                + first_in[m, 1, 1 - col].astype(wider)
            ).astype(jnp.bfloat16)
            two(m, 0).start()
            two(m, 1).start()
            keep[m, 0] = part[m, row, col, :, left].astype(wider) + first_in[
                m, 0, row
            ].astype(wider)
            keep[m, 1] = part[m, row, col, :, right].astype(wider) + first_in[
                m, 1, col
            ].astype(wider)

        @pl.when(n >= 2 * LAG)
        def _():
            m = n - 2 * LAG
            task, h, _, _ = piece(m)
            two(m, 0).wait_recv()
            two(m, 1).wait_recv()
            rows = pl.ds(pl.multiple_of(task * LANES, LANES), LANES)
            for side in range(2):
                at = pl.ds(pl.multiple_of(h * wide + side * (wide // 2), LANES), wide // 2)
                total = keep[m, side] + second_in[m, side].astype(jnp.float32)
                out[rows, at] = total.astype(jnp.bfloat16)

    @pl.loop(0, count)
    def _(n):
        for side in range(2):
            one(n, side).wait_send()
            two(n, side).wait_send()

    for h in range(CUTS):
        to_mate(place, h).wait_send()
        to_mate(place + 1, h).wait_send()
        to_mate(3, h).wait_send()

    @pl.when(outer)
    def _():
        for h in range(CUTS):
            give(h).wait_send()
            along(0, h, x.at[0, core, :, columns(h)], near).wait_send()

    @pl.when(inner)
    def _():
        for h in range(CUTS):
            along(1, h, x.at[1, core, :, columns(h)], near).wait_send()
            along(2, h, other.at[:, columns(h)], facing).wait_send()
            along(3, h, x.at[3, core, :, columns(h)], near).wait_send()
            onward(h).wait_send()
            to_mate(0, h).wait_send()


def newton_kernel(
    tok, blk, tokens, mine, kept, came, g, mixed, square, left, inverse, sent,
    send_sem, recv_sem, pass_send, pass_recv, local_sem, out_sem, in_sem,
):
    t = lax.axis_index("tok")
    b = lax.axis_index("blk")
    low = b < blk // 2
    half = blk // 2
    feats = g.shape[2]
    owners = g.shape[0]
    width = square.shape[1]
    labels = width // feats
    rows = LANES
    factor = 1.0 / (tokens * divisor)
    shift = damping / divisor
    dims = [(2, 0), (4, 0), (0, 1)]
    count = len(dims)

    def owner(device):
        tt, bb = device
        place = jnp.where(low, bb, blk - 1 - bb)
        return place * (owners // 2) + tt % 2 * (owners // 4) + tt // 2

    height = mine.shape[0]
    groups = cut(height, 16, 2)
    parts = [[(o + a, n) for a, n in cut(size, 16, count)] for o, size in groups]

    def flip(j, steps, tok_bits=0):
        blk_bits = 0
        for s in range(count):
            if steps >> s & 1:
                dt, db = dims[(j + s) % count]
                tok_bits ^= dt
                blk_bits ^= db
        return jnp.bitwise_xor(t, tok_bits), jnp.bitwise_xor(b, blk_bits)

    def spot(q, j, device):
        o, n = parts[q][j]
        return g.at[owner(device), pl.ds(o, n)]

    def own(q, j):
        o, n = parts[q][j]
        return mine.at[pl.ds(o, n)]

    def slot(q, j, steps):
        return (q * count + j) * 2**count + steps

    def hop(q, j, steps, s):
        index = slot(q, j, steps | 1 << s)
        where = spot(q, j, flip(j, steps))
        src = own(q, j) if steps == 0 else where
        return remote(src, where, send_sem.at[index], recv_sem.at[index], flip(j, 1 << s))

    def arrival(q, j, steps):
        index = slot(q, j, steps)
        where = spot(q, j, flip(j, steps))
        return remote(where, where, send_sem.at[index], recv_sem.at[index], flip(j, 1))

    mate = (jnp.bitwise_xor(t, 1), b)
    across = (t, jnp.bitwise_xor(b, half))

    def handed(q, j, steps, sender):
        index = slot(q, j, steps)
        where = spot(q, j, flip(j, steps, 0 if sender else 1))
        src = own(q, j) if sender and steps == 0 else where
        return remote(src, where, pass_send.at[index], pass_recv.at[index], mate)

    meet([flip(0, 1 << s) for s in range(count)] + [mate, across])
    pending = []

    def start(copy):
        copy.start()
        pending.append(copy)

    def begin(q):
        for s in range(count):
            for j in range(count):
                start(hop(q, j, 0, s))
        for j in range(count):
            start(handed(q, j, 0, True))

    def advance(q, p):
        for steps in range(2**p, 2 ** (p + 1)):
            for j in range(count):
                arrival(q, j, steps).wait_recv()
                for s in range(p + 1, count):
                    start(hop(q, j, steps, s))
                start(handed(q, j, steps, True))

    begin(0)
    local = pltpu.make_async_copy(mine, g.at[owner((t, b))], local_sem)
    local.start()
    for p in range(count - 1):
        advance(0, p)
    begin(1)
    advance(0, count - 1)
    for p in range(count):
        advance(1, p)
    local.wait()
    for q in range(len(groups)):
        for j in range(count):
            for steps in range(2**count):
                handed(q, j, steps, False).wait_recv()

    eye = lax.broadcasted_iota(jnp.int32, (LANES, LANES), 0) == lax.broadcasted_iota(
        jnp.int32, (LANES, LANES), 1
    )
    eighth = owners // 2

    def diagonal(o, k, sub, axis):
        at = pl.ds(pl.multiple_of(sub * LANES, LANES), LANES)
        own_rows = pl.ds(pl.multiple_of(k * LANES, LANES), LANES)
        block = jnp.where(eye, g[o, own_rows, at].astype(jnp.float32), 0.0)
        total = jnp.sum(block, axis=axis, keepdims=True)
        return lax.rsqrt(total / tokens + epsilon)

    for label in range(labels):
        place, k = DIRECT[label, label]

        @pl.loop(0, eighth)
        def _(sub):
            at = pl.ds(pl.multiple_of(label * feats + sub * LANES, LANES), LANES)
            inverse[:, at] = diagonal(place * eighth + sub, k, sub, 0)

    block_of_rows = t // 2
    row_label = jnp.where(low, block_of_rows, labels - 1 - block_of_rows)
    subs = [t % 2 * blk + bb for bb in (b, jnp.bitwise_xor(b, half))]
    diag_place = pick(row_label, [DIRECT[i, i][0] for i in range(labels)])
    diag_task = pick(row_label, [DIRECT[i, i][1] for i in range(labels)])
    inverse_rows = jnp.concatenate(
        [diagonal(diag_place * eighth + sub, diag_task, sub, 1) for sub in subs], axis=0
    )

    for label in range(labels):

        @pl.when(row_label == label)
        def _():
            for j in range(labels):
                cols = slice(j * feats, (j + 1) * feats)
                for s, sub in enumerate(subs):
                    if (label, j) in DIRECT:
                        place, k = DIRECT[label, j]
                        value = g[place * eighth + sub, k * LANES : (k + 1) * LANES, :]
                    else:
                        place, k = DIRECT[j, label]
                        at = pl.ds(pl.multiple_of(sub * LANES, LANES), LANES)
                        value = g[
                            place * eighth : (place + 1) * eighth, k * LANES : (k + 1) * LANES, at
                        ]
                        value = value.reshape(feats, LANES).T
                    mixed[s * rows : (s + 1) * rows, cols] = value

    step = feats // CUTS
    starts = [row_label * feats + sub * LANES for sub in subs]

    def identity(first_col, size):
        at = first_col + lax.broadcasted_iota(jnp.int32, (rows, size), 1)
        row = lax.broadcasted_iota(jnp.int32, (rows, size), 0)
        return jnp.concatenate(
            [(at - start == row).astype(jnp.float32) for start in starts], axis=0
        )

    def scaled(first_col, size):
        at = pl.ds(first_col, size)
        return mixed[:, at].astype(jnp.float32) * (
            factor * inverse_rows
        ) * inverse[:, at] + shift * identity(first_col, size)

    def fold(label, h):
        total = None
        for k in range(labels):
            lhs = left[:, k * feats : (k + 1) * feats]
            if (k, label) in DIRECT:
                place, task = DIRECT[k, label]
                rhs = g[
                    place * eighth : (place + 1) * eighth,
                    task * LANES : (task + 1) * LANES,
                    pl.ds(pl.multiple_of(h * step, LANES), step),
                ].reshape(feats, step)
                product = jnp.dot(lhs, rhs, preferred_element_type=jnp.float32)
            else:
                place, task = DIRECT[label, k]
                few = step // LANES
                rhs = g[
                    pl.ds(place * eighth + h * few, few), task * LANES : (task + 1) * LANES, :
                ].reshape(step, feats)
                product = lax.dot_general(
                    lhs, rhs, (((1,), (1,)), ((), ())), preferred_element_type=jnp.float32
                )
            total = product if total is None else total + product
        return total

    @pl.loop(0, labels * CUTS)
    def _(i):
        start_col = pl.multiple_of(i * step, step)
        at = pl.ds(start_col, step)
        left[:, at] = (scaled(start_col, step) * inverse[:, at]).astype(jnp.bfloat16)

    for label in range(labels):

        @pl.loop(0, CUTS)
        def _(h):
            start_col = pl.multiple_of(label * feats + h * step, step)
            at = pl.ds(start_col, step)
            square[:, at] = fold(label, h) * (inverse[:, at] * factor) + shift * scaled(
                start_col, step
            )

    @pl.loop(0, labels * CUTS)
    def _(i):
        start_col = pl.multiple_of(i * step, step)
        at = pl.ds(start_col, step)
        left[:, at] = (square[:, at] * inverse[:, at]).astype(jnp.bfloat16)

    def swap(label, h):
        to = jnp.where(low, label, labels - 1 - label)
        at = pl.ds(pl.multiple_of(to * feats + h * step, LANES), step)
        index = label * CUTS + h
        return at, remote(
            sent.at[:, at], came.at[:, at], out_sem.at[index], in_sem.at[index], across
        )

    for label in range(labels):

        @pl.loop(0, CUTS)
        def _(h):
            start_col = pl.multiple_of(label * feats + h * step, step)
            at = pl.ds(start_col, step)
            squared = square[:, at]
            cube = fold(label, h) * (inverse[:, at] * factor) + shift * squared
            result = (
                4.0 * identity(start_col, step) - 6.0 * scaled(start_col, step)
                + 4.0 * squared - cube
            )
            to, copy = swap(label, h)
            kept[:, to] = result[:rows]
            sent[:, to] = result[rows:].astype(jnp.bfloat16)
            copy.start()

    for label in range(labels):

        @pl.loop(0, CUTS)
        def _(h):
            _, copy = swap(label, h)
            copy.wait_recv()
            copy.wait_send()

    for copy in pending:
        copy.wait_send()


def cut(length, unit, pieces):
    units = length // unit
    sizes = [(units // pieces + (1 if i < units % pieces else 0)) * unit for i in range(pieces)]
    return [(sum(sizes[:i]), sizes[i]) for i in range(pieces)]


def call(kernel, outs, scratch, collective_id, space, *operands):
    return pl.pallas_call(
        kernel,
        out_shape=outs,
        in_specs=[pl.BlockSpec(memory_space=space)] * len(operands),
        out_specs=[pl.BlockSpec(memory_space=pltpu.VMEM)] * len(outs),
        scratch_shapes=scratch,
        compiler_params=pltpu.CompilerParams(
            collective_id=collective_id, has_side_effects=True, vmem_limit_bytes=60 * 1024 * 1024
        ),
    )(*operands)


def split_body(tok, blk, activations, out_grads):
    depth, feats = activations.shape
    tokens = depth * tok
    width = feats * blk
    rows = width // (tok * blk)
    low = lax.axis_index("blk") < blk // 2
    count = TASKS * CUTS
    wide = feats // CUTS
    bf16, f32 = jnp.bfloat16, jnp.float32
    dma = pltpu.SemaphoreType.DMA
    (mine,) = call(
        functools.partial(gram_kernel, tok, blk),
        [jax.ShapeDtypeStruct((TASKS * rows, feats), bf16)],
        [
            pltpu.VMEM((blk, 2, depth, feats), bf16),
            pltpu.VMEM((depth, feats), bf16),
            pltpu.VMEM((depth, feats), bf16),
            pltpu.VMEM((3, feats // 2, 2 * depth), bf16),
            pltpu.VMEM((count, 2, 2, rows, wide), bf16),
            pltpu.VMEM((count, 2, 2, rows, wide // 2), bf16),
            pltpu.VMEM((count, 2, rows, wide // 2), bf16),
            pltpu.VMEM((count, 2, rows, wide // 2), bf16),
            pltpu.VMEM((count, 2, rows, wide // 2), f32),
            dma((2,)),
            dma((blk, CUTS)), dma((blk, CUTS)),
            dma((CUTS,)), dma((CUTS,)),
            dma((blk, CUTS)), dma((blk, CUTS)),
            dma((count, 2)), dma((count, 2)), dma((count, 2)), dma((count, 2)),
        ],
        0, pl.ANY, activations, out_grads,
    )
    slots = 2 * 3 * 8
    steps = blk * CUTS
    kept, came = call(
        functools.partial(newton_kernel, tok, blk, tokens),
        [jax.ShapeDtypeStruct((rows, width), f32), jax.ShapeDtypeStruct((rows, width), bf16)],
        [
            pltpu.VMEM((2 * tok, TASKS * rows, feats), bf16),
            pltpu.VMEM((2 * rows, width), bf16),
            pltpu.VMEM((2 * rows, width), f32),
            pltpu.VMEM((2 * rows, width), bf16),
            pltpu.VMEM((1, width), f32),
            pltpu.VMEM((rows, width), bf16),
            dma((slots,)), dma((slots,)), dma((slots,)), dma((slots,)), dma,
            dma((steps,)), dma((steps,)),
        ],
        1, pltpu.VMEM, mine,
    )
    came = came.astype(f32)
    return jnp.where(low, kept, came), jnp.where(low, came, kept)


def solution(mesh):
    tok, blk = mesh.shape["tok"], mesh.shape["blk"]
    placed = (P("tok", "blk"), P("tok", "blk"))

    def body(activations, out_grads):
        depth, feats = activations.shape
        whole = max(depth * tok, feats * blk) * feats * blk * activations.dtype.itemsize
        cube = tok == 2 * blk and blk == 4 and feats == tok * LANES
        if whole <= gathered_budget and cube:
            return split_body(tok, blk, activations, out_grads)
        return tiled_body(activations, out_grads)

    return jax.shard_map(
        body,
        mesh=mesh,
        in_specs=placed,
        out_specs=(P(("tok", "blk"), None), P(("tok", "blk"), None)),
        check_vma=False,
    )
```

```python
import functools

import jax
import jax.numpy as jnp
import numpy as np
from jax import lax
from jax.experimental import pallas as pl
from jax.experimental.pallas import tpu as pltpu
from jax.sharding import PartitionSpec as P

damping = 0.3
epsilon = 1e-06
divisor = 2.0
gathered_budget = 32 * 1024 * 1024
LANES = 128
MESH = pl.DeviceIdType.MESH


def column_squares(data):
    values = data.astype(jnp.float32)
    return jnp.sum(values * values, axis=0)


def fold_product(row_block, tile):
    return jnp.dot(
        row_block,
        lax.all_gather(tile, "tok", axis=0, tiled=True),
        preferred_element_type=jnp.float32,
    )


def newton_steps(scaled, identity):
    half = scaled.astype(jnp.bfloat16)
    row_block = lax.all_gather(half, "blk", axis=1, tiled=True)
    square = fold_product(row_block, half)
    cube = fold_product(row_block, square.astype(jnp.bfloat16))
    return 4.0 * identity - 6.0 * scaled + 4.0 * square - cube


def tiled_body(activations, out_grads):
    tok_count = lax.axis_size("tok")
    blk_count = lax.axis_size("blk")
    tok_id = lax.axis_index("tok")
    blk_id = lax.axis_index("blk")
    token_count = activations.shape[0] * tok_count
    tile_cols = activations.shape[1]
    tile_rows = tile_cols * blk_count // tok_count
    row_ids = tok_id * tile_rows + jnp.arange(tile_rows, dtype=jnp.int32)
    col_ids = blk_id * tile_cols + jnp.arange(tile_cols, dtype=jnp.int32)
    identity = (row_ids[:, None] == col_ids[None, :]).astype(jnp.float32)

    def inverse_tile(local):
        full = lax.all_gather(local, "blk", axis=1, tiled=True)
        sums = lax.psum(column_squares(full).astype(jnp.bfloat16), "tok").astype(jnp.float32)
        gram_tile = lax.psum_scatter(
            lax.dot_general(
                full, local, (((0,), (0,)), ((), ())), preferred_element_type=jnp.float32
            ).astype(jnp.bfloat16),
            "tok",
            scatter_dimension=0,
            tiled=True,
        ).astype(jnp.float32)
        inverse = lax.rsqrt(sums / token_count + epsilon)
        inverse_rows = lax.dynamic_slice_in_dim(inverse, tok_id * tile_rows, tile_rows)
        inverse_cols = lax.dynamic_slice_in_dim(inverse, blk_id * tile_cols, tile_cols)
        damped = (
            gram_tile / token_count * inverse_rows[:, None] * inverse_cols[None, :]
            + damping * identity
        )
        result_tile = newton_steps(damped / divisor, identity)
        return lax.all_to_all(
            result_tile.astype(jnp.bfloat16), "blk", split_axis=0, concat_axis=1, tiled=True
        ).astype(result_tile.dtype)

    return inverse_tile(activations), inverse_tile(out_grads)


DIRECT = {
    (0, 0): (0, 0), (0, 1): (0, 1), (0, 3): (0, 2), (1, 3): (0, 3), (3, 3): (0, 4),
    (1, 1): (1, 0), (1, 2): (1, 1), (2, 0): (1, 2), (2, 3): (1, 3), (2, 2): (1, 4),
}
TASKS = 5
CUTS = 4
ADD_LAG = 3
END_LAG = 6


def pick(index, values):
    out = values[-1]
    for i in range(len(values) - 2, -1, -1):
        out = jnp.where(index == i, values[i], out)
    return out


def remote(src, dst, send, recv, device):
    return pltpu.make_async_remote_copy(
        src_ref=src, dst_ref=dst, send_sem=send, recv_sem=recv,
        device_id=device, device_id_type=MESH,
    )


def meet(peers):
    barrier = pltpu.get_barrier_semaphore()
    for peer in peers:
        pl.semaphore_signal(barrier, inc=1, device_id=peer, device_id_type=MESH)
    pl.semaphore_wait(barrier, len(peers))


def gram_kernel(
    tok, blk, acts, grads, out,
    x, other, passed, turned, part, first_in, second_out, second_in, keep,
    load_sem, near_send, near_recv, pass_send, pass_recv, core_send, core_recv,
    one_send, one_recv, two_send, two_recv,
):
    t = lax.axis_index("tok")
    b = lax.axis_index("blk")
    low = b < blk // 2
    place = jnp.where(low, b, blk - 1 - b)
    outer = place == 0
    inner = place == 1
    core, col, row = t % 2, t // 2 % 2, t // 4
    mate = (jnp.bitwise_xor(t, 1), b)
    beside = (jnp.bitwise_xor(t, 2), b)
    below = (jnp.bitwise_xor(t, 4), b)
    near = (t, jnp.bitwise_xor(b, 1))
    facing = (t, blk - 1 - b)
    depth, feats = other.shape
    wide = feats // CUTS
    halfway = feats // 2
    count = TASKS * CUTS

    def load(ref, dst, index):
        return pltpu.make_async_copy(ref, dst, load_sem.at[index])

    @pl.when(low)
    def _():
        load(acts, x.at[place, core], 0).start()
        load(grads, other, 1).start()

    @pl.when(jnp.logical_not(low))
    def _():
        load(grads, x.at[place, core], 0).start()
        load(acts, other, 1).start()

    meet([mate, beside, below, near, facing])
    load(acts, x.at[place, core], 0).wait()
    load(grads, other, 1).wait()

    def columns(h):
        return pl.ds(pl.multiple_of(h * wide, LANES), wide)

    def to_mate(label, h):
        here = x.at[label, core, :, columns(h)]
        return remote(
            here, here, core_send.at[label, h], core_recv.at[label, h], mate
        )

    def from_mate(label, h):
        there = x.at[label, 1 - core, :, columns(h)]
        return remote(
            there, there, core_send.at[label, h], core_recv.at[label, h], mate
        )

    def along(label, h, src, device):
        return remote(
            src, x.at[label, core, :, columns(h)],
            near_send.at[label, h], near_recv.at[label, h], device,
        )

    def arrived(label, h):
        here = x.at[label, core, :, columns(h)]
        return remote(here, here, near_send.at[label, h], near_recv.at[label, h], near)

    def give(h):
        return remote(
            other.at[:, columns(h)], passed.at[:, columns(h)],
            pass_send.at[h], pass_recv.at[h], near,
        )

    def onward(h):
        return remote(
            passed.at[:, columns(h)], x.at[3, core, :, columns(h)],
            pass_send.at[h], near_recv.at[3, h], facing,
        )

    for h in range(CUTS):
        to_mate(place, h).start()

    @pl.when(outer)
    def _():
        for h in range(CUTS):
            give(h).start()
        for h in range(CUTS):
            along(0, h, x.at[0, core, :, columns(h)], near).start()

    @pl.when(inner)
    def _():
        for h in range(CUTS):
            along(1, h, x.at[1, core, :, columns(h)], near).start()
            along(2, h, other.at[:, columns(h)], facing).start()

    def turn(slot, label):
        for c in range(2):
            for r in range(0, depth, 256):
                turned[slot, :, c * depth + r : c * depth + r + 256] = x[
                    label, c, r : r + 256, pl.ds(pl.multiple_of(core * halfway, LANES), halfway)
                ].T

    def share(label, h):
        arrived(label, h).wait_recv()
        to_mate(label, h).start()

    def piece(n):
        late = n - jnp.where(outer, 2, 3) * CUTS
        pairs = late // 2
        paired = jnp.where(outer, (n >= 2 * CUTS) & (n < 4 * CUTS), n >= 3 * CUTS)
        task = jnp.where(paired, 2 + late % 2, jnp.where(n < 2 * CUTS, n // CUTS, 4))
        h = jnp.where(paired, pairs, n % CUTS)
        slot = jnp.where(outer, pick(task, [0, 0, 0, 1, 2]), pick(task, [0, 0, 1, 1, 1]))
        label = jnp.where(outer, pick(task, [0, 1, 3, 3, 3]), pick(task, [1, 2, 0, 3, 2]))
        return task, h, slot, label

    def one(n, side):
        if side == 0:
            src, device = part.at[n, :, 1 - col, :, pl.ds(0, wide // 2)], beside
        else:
            src, device = part.at[n, 1 - row, :, :, pl.ds(wide // 2, wide // 2)], below
        return remote(
            src, first_in.at[n, side], one_send.at[n, side], one_recv.at[n, side], device
        )

    def two(n, side):
        return remote(
            second_out.at[n, side], second_in.at[n, side],
            two_send.at[n, side], two_recv.at[n, side], below if side == 0 else beside,
        )

    for h in range(CUTS):
        from_mate(place, h).wait_recv()
    turn(0, place)

    @pl.loop(0, count + END_LAG)
    def _(n):
        @pl.when((n >= CUTS) & (n < 2 * CUTS))
        def _():
            h = n - CUTS

            @pl.when(inner)
            def _():
                give(h).wait_recv()
                onward(h).start()

            share(place + 1, h)
            from_mate(place + 1, h).wait_recv()

        @pl.when(n == 2 * CUTS)
        def _():
            turn(1, place + 1)

        late = n - jnp.where(outer, 2, 3) * CUTS
        paired = jnp.where(outer, (n >= 2 * CUTS) & (n < 4 * CUTS), n >= 3 * CUTS)

        @pl.when(paired & (late % 2 == 0) & (n < count))
        def _():
            h = late // 2
            arrived(3, h).wait_recv()
            to_mate(3, h).start()

            @pl.when(inner)
            def _():
                along(3, h, x.at[3, core, :, columns(h)], near).start()
                share(0, h)
                from_mate(0, h).wait_recv()

            from_mate(3, h).wait_recv()

        @pl.when(outer & (n == 4 * CUTS))
        def _():
            turn(2, 3)

        @pl.when(n < count)
        def _():
            task, h, slot, label = piece(n)
            at = pl.ds(pl.multiple_of(h * wide, LANES), wide)
            right = x[label, :, :, at].reshape(2 * depth, wide)
            product = jnp.dot(turned[slot], right, preferred_element_type=jnp.float32)
            part[n] = product.astype(jnp.bfloat16).reshape(2, 2, LANES, wide)
            one(n, 0).start()
            one(n, 1).start()

        @pl.when((n >= ADD_LAG) & (n < count + ADD_LAG))
        def _():
            m = n - ADD_LAG
            left, right = pl.ds(0, wide // 2), pl.ds(wide // 2, wide // 2)
            one(m, 0).wait_recv()
            one(m, 1).wait_recv()
            wider = jnp.float32
            second_out[m, 0] = (
                part[m, 1 - row, col, :, left].astype(wider)
                + first_in[m, 0, 1 - row].astype(wider)
            ).astype(jnp.bfloat16)
            second_out[m, 1] = (
                part[m, row, 1 - col, :, right].astype(wider)
                + first_in[m, 1, 1 - col].astype(wider)
            ).astype(jnp.bfloat16)
            two(m, 0).start()
            two(m, 1).start()
            keep[m, 0] = part[m, row, col, :, left].astype(wider) + first_in[
                m, 0, row
            ].astype(wider)
            keep[m, 1] = part[m, row, col, :, right].astype(wider) + first_in[
                m, 1, col
            ].astype(wider)

        @pl.when(n >= END_LAG)
        def _():
            m = n - END_LAG
            task, h, _, _ = piece(m)
            two(m, 0).wait_recv()
            two(m, 1).wait_recv()
            rows = pl.ds(pl.multiple_of(task * LANES, LANES), LANES)
            for side in range(2):
                at = pl.ds(pl.multiple_of(h * wide + side * (wide // 2), LANES), wide // 2)
                total = keep[m, side] + second_in[m, side].astype(jnp.float32)
                out[rows, at] = total.astype(jnp.bfloat16)

    @pl.loop(0, count)
    def _(n):
        for side in range(2):
            one(n, side).wait_send()
            two(n, side).wait_send()

    for h in range(CUTS):
        to_mate(place, h).wait_send()
        to_mate(place + 1, h).wait_send()
        to_mate(3, h).wait_send()

    @pl.when(outer)
    def _():
        for h in range(CUTS):
            give(h).wait_send()
            along(0, h, x.at[0, core, :, columns(h)], near).wait_send()

    @pl.when(inner)
    def _():
        for h in range(CUTS):
            along(1, h, x.at[1, core, :, columns(h)], near).wait_send()
            along(2, h, other.at[:, columns(h)], facing).wait_send()
            along(3, h, x.at[3, core, :, columns(h)], near).wait_send()
            onward(h).wait_send()
            to_mate(0, h).wait_send()


def newton_kernel(
    tok, blk, tokens, mine, kept, came, g, mixed, square, left, inverse, sent,
    send_sem, recv_sem, pass_send, pass_recv, local_sem, out_sem, in_sem,
):
    t = lax.axis_index("tok")
    b = lax.axis_index("blk")
    low = b < blk // 2
    half = blk // 2
    feats = g.shape[2]
    owners = g.shape[0]
    width = square.shape[1]
    labels = width // feats
    rows = LANES
    factor = 1.0 / (tokens * divisor)
    shift = damping / divisor
    dims = [(2, 0), (4, 0), (0, 1)]
    count = len(dims)

    def owner(device):
        tt, bb = device
        place = jnp.where(low, bb, blk - 1 - bb)
        return place * (owners // 2) + tt % 2 * (owners // 4) + tt // 2

    height = mine.shape[0]
    groups = cut(height, 16, 2)
    parts = [[(o + a, n) for a, n in cut(size, 16, count)] for o, size in groups]

    def flip(j, steps, tok_bits=0):
        blk_bits = 0
        for s in range(count):
            if steps >> s & 1:
                dt, db = dims[(j + s) % count]
                tok_bits ^= dt
                blk_bits ^= db
        return jnp.bitwise_xor(t, tok_bits), jnp.bitwise_xor(b, blk_bits)

    def spot(q, j, device):
        o, n = parts[q][j]
        return g.at[owner(device), pl.ds(o, n)]

    def own(q, j):
        o, n = parts[q][j]
        return mine.at[pl.ds(o, n)]

    def slot(q, j, steps):
        return (q * count + j) * 2**count + steps

    def hop(q, j, steps, s):
        index = slot(q, j, steps | 1 << s)
        where = spot(q, j, flip(j, steps))
        src = own(q, j) if steps == 0 else where
        return remote(src, where, send_sem.at[index], recv_sem.at[index], flip(j, 1 << s))

    def arrival(q, j, steps):
        index = slot(q, j, steps)
        where = spot(q, j, flip(j, steps))
        return remote(where, where, send_sem.at[index], recv_sem.at[index], flip(j, 1))

    mate = (jnp.bitwise_xor(t, 1), b)
    across = (t, jnp.bitwise_xor(b, half))

    def handed(q, j, steps, sender):
        index = slot(q, j, steps)
        where = spot(q, j, flip(j, steps, 0 if sender else 1))
        src = own(q, j) if sender and steps == 0 else where
        return remote(src, where, pass_send.at[index], pass_recv.at[index], mate)

    meet([flip(0, 1 << s) for s in range(count)] + [mate, across])
    pending = []

    def start(copy):
        copy.start()
        pending.append(copy)

    def begin(q):
        for s in range(count):
            for j in range(count):
                start(hop(q, j, 0, s))
        for j in range(count):
            start(handed(q, j, 0, True))

    def advance(q, p):
        for steps in range(2**p, 2 ** (p + 1)):
            for j in range(count):
                arrival(q, j, steps).wait_recv()
                for s in range(p + 1, count):
                    start(hop(q, j, steps, s))
                start(handed(q, j, steps, True))

    begin(0)
    local = pltpu.make_async_copy(mine, g.at[owner((t, b))], local_sem)
    local.start()
    for p in range(count - 1):
        advance(0, p)
    begin(1)
    advance(0, count - 1)
    for p in range(count):
        advance(1, p)
    local.wait()
    for q in range(len(groups)):
        for j in range(count):
            for steps in range(2**count):
                handed(q, j, steps, False).wait_recv()

    eye = lax.broadcasted_iota(jnp.int32, (LANES, LANES), 0) == lax.broadcasted_iota(
        jnp.int32, (LANES, LANES), 1
    )
    eighth = owners // 2

    def diagonal(o, k, sub, axis):
        at = pl.ds(pl.multiple_of(sub * LANES, LANES), LANES)
        own_rows = pl.ds(pl.multiple_of(k * LANES, LANES), LANES)
        block = jnp.where(eye, g[o, own_rows, at].astype(jnp.float32), 0.0)
        total = jnp.sum(block, axis=axis, keepdims=True)
        return lax.rsqrt(total / tokens + epsilon)

    for label in range(labels):
        place, k = DIRECT[label, label]

        @pl.loop(0, eighth)
        def _(sub):
            at = pl.ds(pl.multiple_of(label * feats + sub * LANES, LANES), LANES)
            inverse[:, at] = diagonal(place * eighth + sub, k, sub, 0)

    block_of_rows = t // 2
    row_label = jnp.where(low, block_of_rows, labels - 1 - block_of_rows)
    subs = [t % 2 * blk + bb for bb in (b, jnp.bitwise_xor(b, half))]
    diag_place = pick(row_label, [DIRECT[i, i][0] for i in range(labels)])
    diag_task = pick(row_label, [DIRECT[i, i][1] for i in range(labels)])
    inverse_rows = jnp.concatenate(
        [diagonal(diag_place * eighth + sub, diag_task, sub, 1) for sub in subs], axis=0
    )

    for label in range(labels):

        @pl.when(row_label == label)
        def _():
            for j in range(labels):
                cols = slice(j * feats, (j + 1) * feats)
                for s, sub in enumerate(subs):
                    if (label, j) in DIRECT:
                        place, k = DIRECT[label, j]
                        value = g[place * eighth + sub, k * LANES : (k + 1) * LANES, :]
                    else:
                        place, k = DIRECT[j, label]
                        at = pl.ds(pl.multiple_of(sub * LANES, LANES), LANES)
                        value = g[
                            place * eighth : (place + 1) * eighth, k * LANES : (k + 1) * LANES, at
                        ]
                        value = value.reshape(feats, LANES).T
                    mixed[s * rows : (s + 1) * rows, cols] = value

    step = feats // CUTS
    starts = [row_label * feats + sub * LANES for sub in subs]

    def identity(first_col, size):
        at = first_col + lax.broadcasted_iota(jnp.int32, (rows, size), 1)
        row = lax.broadcasted_iota(jnp.int32, (rows, size), 0)
        return jnp.concatenate(
            [(at - start == row).astype(jnp.float32) for start in starts], axis=0
        )

    def scaled(first_col, size):
        at = pl.ds(first_col, size)
        return mixed[:, at].astype(jnp.float32) * (
            factor * inverse_rows
        ) * inverse[:, at] + shift * identity(first_col, size)

    def fold(label, h):
        total = None
        for k in range(labels):
            lhs = left[:, k * feats : (k + 1) * feats]
            if (k, label) in DIRECT:
                place, task = DIRECT[k, label]
                rhs = g[
                    place * eighth : (place + 1) * eighth,
                    task * LANES : (task + 1) * LANES,
                    pl.ds(pl.multiple_of(h * step, LANES), step),
                ].reshape(feats, step)
                product = jnp.dot(lhs, rhs, preferred_element_type=jnp.float32)
            else:
                place, task = DIRECT[label, k]
                few = step // LANES
                rhs = g[
                    pl.ds(place * eighth + h * few, few), task * LANES : (task + 1) * LANES, :
                ].reshape(step, feats)
                product = lax.dot_general(
                    lhs, rhs, (((1,), (1,)), ((), ())), preferred_element_type=jnp.float32
                )
            total = product if total is None else total + product
        return total

    @pl.loop(0, labels * CUTS)
    def _(i):
        start_col = pl.multiple_of(i * step, step)
        at = pl.ds(start_col, step)
        left[:, at] = (scaled(start_col, step) * inverse[:, at]).astype(jnp.bfloat16)

    for label in range(labels):

        @pl.loop(0, CUTS)
        def _(h):
            start_col = pl.multiple_of(label * feats + h * step, step)
            at = pl.ds(start_col, step)
            square[:, at] = fold(label, h) * (inverse[:, at] * factor) + shift * scaled(
                start_col, step
            )

    @pl.loop(0, labels * CUTS)
    def _(i):
        start_col = pl.multiple_of(i * step, step)
        at = pl.ds(start_col, step)
        left[:, at] = (square[:, at] * inverse[:, at]).astype(jnp.bfloat16)

    def swap(label, h):
        to = jnp.where(low, label, labels - 1 - label)
        at = pl.ds(pl.multiple_of(to * feats + h * step, LANES), step)
        index = label * CUTS + h
        return at, remote(
            sent.at[:, at], came.at[:, at], out_sem.at[index], in_sem.at[index], across
        )

    for label in range(labels):

        @pl.loop(0, CUTS)
        def _(h):
            start_col = pl.multiple_of(label * feats + h * step, step)
            at = pl.ds(start_col, step)
            squared = square[:, at]
            cube = fold(label, h) * (inverse[:, at] * factor) + shift * squared
            result = (
                4.0 * identity(start_col, step) - 6.0 * scaled(start_col, step)
                + 4.0 * squared - cube
            )
            to, copy = swap(label, h)
            kept[:, to] = result[:rows]
            sent[:, to] = result[rows:].astype(jnp.bfloat16)
            copy.start()

    for label in range(labels):

        @pl.loop(0, CUTS)
        def _(h):
            _, copy = swap(label, h)
            copy.wait_recv()
            copy.wait_send()

    for copy in pending:
        copy.wait_send()


def cut(length, unit, pieces):
    units = length // unit
    sizes = [(units // pieces + (1 if i < units % pieces else 0)) * unit for i in range(pieces)]
    return [(sum(sizes[:i]), sizes[i]) for i in range(pieces)]


def call(kernel, outs, scratch, collective_id, space, *operands):
    return pl.pallas_call(
        kernel,
        out_shape=outs,
        in_specs=[pl.BlockSpec(memory_space=space)] * len(operands),
        out_specs=[pl.BlockSpec(memory_space=pltpu.VMEM)] * len(outs),
        scratch_shapes=scratch,
        compiler_params=pltpu.CompilerParams(
            collective_id=collective_id, has_side_effects=True, vmem_limit_bytes=60 * 1024 * 1024
        ),
    )(*operands)


def split_body(tok, blk, activations, out_grads):
    depth, feats = activations.shape
    tokens = depth * tok
    width = feats * blk
    rows = width // (tok * blk)
    low = lax.axis_index("blk") < blk // 2
    count = TASKS * CUTS
    wide = feats // CUTS
    bf16, f32 = jnp.bfloat16, jnp.float32
    dma = pltpu.SemaphoreType.DMA
    (mine,) = call(
        functools.partial(gram_kernel, tok, blk),
        [jax.ShapeDtypeStruct((TASKS * rows, feats), bf16)],
        [
            pltpu.VMEM((blk, 2, depth, feats), bf16),
            pltpu.VMEM((depth, feats), bf16),
            pltpu.VMEM((depth, feats), bf16),
            pltpu.VMEM((3, feats // 2, 2 * depth), bf16),
            pltpu.VMEM((count, 2, 2, rows, wide), bf16),
            pltpu.VMEM((count, 2, 2, rows, wide // 2), bf16),
            pltpu.VMEM((count, 2, rows, wide // 2), bf16),
            pltpu.VMEM((count, 2, rows, wide // 2), bf16),
            pltpu.VMEM((count, 2, rows, wide // 2), f32),
            dma((2,)),
            dma((blk, CUTS)), dma((blk, CUTS)),
            dma((CUTS,)), dma((CUTS,)),
            dma((blk, CUTS)), dma((blk, CUTS)),
            dma((count, 2)), dma((count, 2)), dma((count, 2)), dma((count, 2)),
        ],
        0, pl.ANY, activations, out_grads,
    )
    slots = 2 * 3 * 8
    steps = blk * CUTS
    kept, came = call(
        functools.partial(newton_kernel, tok, blk, tokens),
        [jax.ShapeDtypeStruct((rows, width), f32), jax.ShapeDtypeStruct((rows, width), bf16)],
        [
            pltpu.VMEM((2 * tok, TASKS * rows, feats), bf16),
            pltpu.VMEM((2 * rows, width), bf16),
            pltpu.VMEM((2 * rows, width), f32),
            pltpu.VMEM((2 * rows, width), bf16),
            pltpu.VMEM((1, width), f32),
            pltpu.VMEM((rows, width), bf16),
            dma((slots,)), dma((slots,)), dma((slots,)), dma((slots,)), dma,
            dma((steps,)), dma((steps,)),
        ],
        1, pltpu.VMEM, mine,
    )
    came = came.astype(f32)
    return jnp.where(low, kept, came), jnp.where(low, came, kept)


def solution(mesh):
    tok, blk = mesh.shape["tok"], mesh.shape["blk"]
    placed = (P("tok", "blk"), P("tok", "blk"))

    def body(activations, out_grads):
        depth, feats = activations.shape
        whole = max(depth * tok, feats * blk) * feats * blk * activations.dtype.itemsize
        cube = tok == 2 * blk and blk == 4 and feats == tok * LANES
        if whole <= gathered_budget and cube:
            return split_body(tok, blk, activations, out_grads)
        return tiled_body(activations, out_grads)

    return jax.shard_map(
        body,
        mesh=mesh,
        in_specs=placed,
        out_specs=(P(("tok", "blk"), None), P(("tok", "blk"), None)),
        check_vma=False,
    )
```

```python
import functools

import jax
import jax.numpy as jnp
import numpy as np
from jax import lax
from jax.experimental import pallas as pl
from jax.experimental.pallas import tpu as pltpu
from jax.sharding import PartitionSpec as P

damping = 0.3
epsilon = 1e-06
divisor = 2.0
gathered_budget = 32 * 1024 * 1024
LANES = 128
MESH = pl.DeviceIdType.MESH


def column_squares(data):
    values = data.astype(jnp.float32)
    return jnp.sum(values * values, axis=0)


def fold_product(row_block, tile):
    return jnp.dot(
        row_block,
        lax.all_gather(tile, "tok", axis=0, tiled=True),
        preferred_element_type=jnp.float32,
    )


def newton_steps(scaled, identity):
    half = scaled.astype(jnp.bfloat16)
    row_block = lax.all_gather(half, "blk", axis=1, tiled=True)
    square = fold_product(row_block, half)
    cube = fold_product(row_block, square.astype(jnp.bfloat16))
    return 4.0 * identity - 6.0 * scaled + 4.0 * square - cube


def tiled_body(activations, out_grads):
    tok_count = lax.axis_size("tok")
    blk_count = lax.axis_size("blk")
    tok_id = lax.axis_index("tok")
    blk_id = lax.axis_index("blk")
    token_count = activations.shape[0] * tok_count
    tile_cols = activations.shape[1]
    tile_rows = tile_cols * blk_count // tok_count
    row_ids = tok_id * tile_rows + jnp.arange(tile_rows, dtype=jnp.int32)
    col_ids = blk_id * tile_cols + jnp.arange(tile_cols, dtype=jnp.int32)
    identity = (row_ids[:, None] == col_ids[None, :]).astype(jnp.float32)

    def inverse_tile(local):
        full = lax.all_gather(local, "blk", axis=1, tiled=True)
        sums = lax.psum(column_squares(full).astype(jnp.bfloat16), "tok").astype(jnp.float32)
        gram_tile = lax.psum_scatter(
            lax.dot_general(
                full, local, (((0,), (0,)), ((), ())), preferred_element_type=jnp.float32
            ).astype(jnp.bfloat16),
            "tok",
            scatter_dimension=0,
            tiled=True,
        ).astype(jnp.float32)
        inverse = lax.rsqrt(sums / token_count + epsilon)
        inverse_rows = lax.dynamic_slice_in_dim(inverse, tok_id * tile_rows, tile_rows)
        inverse_cols = lax.dynamic_slice_in_dim(inverse, blk_id * tile_cols, tile_cols)
        damped = (
            gram_tile / token_count * inverse_rows[:, None] * inverse_cols[None, :]
            + damping * identity
        )
        result_tile = newton_steps(damped / divisor, identity)
        return lax.all_to_all(
            result_tile.astype(jnp.bfloat16), "blk", split_axis=0, concat_axis=1, tiled=True
        ).astype(result_tile.dtype)

    return inverse_tile(activations), inverse_tile(out_grads)


DIRECT = {
    (0, 0): (0, 0), (0, 1): (0, 1), (0, 3): (0, 2), (1, 3): (0, 3), (3, 3): (0, 4),
    (1, 1): (1, 0), (1, 2): (1, 1), (2, 0): (1, 2), (2, 3): (1, 3), (2, 2): (1, 4),
}
TASKS = 5
EARLY = 2
CUTS = 4
ADD_LAG = 3
END_LAG = 6


def pick(index, values):
    out = values[-1]
    for i in range(len(values) - 2, -1, -1):
        out = jnp.where(index == i, values[i], out)
    return out


def remote(src, dst, send, recv, device):
    return pltpu.make_async_remote_copy(
        src_ref=src, dst_ref=dst, send_sem=send, recv_sem=recv,
        device_id=device, device_id_type=MESH,
    )


def meet(peers):
    barrier = pltpu.get_barrier_semaphore()
    for peer in peers:
        pl.semaphore_signal(barrier, inc=1, device_id=peer, device_id_type=MESH)
    pl.semaphore_wait(barrier, len(peers))


def factor_kernel(
    tok, blk, tokens, acts, grads, kept, came,
    x, other, passed, turned, part, first_in, second_out, second_in, keep,
    g, mixed, square, left, inverse, sent,
    load_sem, near_send, near_recv, pass_send, pass_recv, core_send, core_recv,
    one_send, one_recv, two_send, two_recv,
    hop_send, hop_recv, hand_send, hand_recv, out_sem, in_sem,
):
    t = lax.axis_index("tok")
    b = lax.axis_index("blk")
    low = b < blk // 2
    place = jnp.where(low, b, blk - 1 - b)
    outer = place == 0
    inner = place == 1
    core, col, row = t % 2, t // 2 % 2, t // 4
    mate = (jnp.bitwise_xor(t, 1), b)
    beside = (jnp.bitwise_xor(t, 2), b)
    below = (jnp.bitwise_xor(t, 4), b)
    near = (t, jnp.bitwise_xor(b, 1))
    facing = (t, blk - 1 - b)
    across = (t, jnp.bitwise_xor(b, blk // 2))
    depth, feats = other.shape
    wide = feats // CUTS
    halfway = feats // 2
    count = TASKS * CUTS

    def load(ref, dst, index):
        return pltpu.make_async_copy(ref, dst, load_sem.at[index])

    @pl.when(low)
    def _():
        load(acts, x.at[place, core], 0).start()
        load(grads, other, 1).start()

    @pl.when(jnp.logical_not(low))
    def _():
        load(grads, x.at[place, core], 0).start()
        load(acts, other, 1).start()

    meet([mate, beside, below, near, facing, across])
    load(acts, x.at[place, core], 0).wait()
    load(grads, other, 1).wait()

    def columns(h):
        return pl.ds(pl.multiple_of(h * wide, LANES), wide)

    def to_mate(label, h):
        here = x.at[label, core, :, columns(h)]
        return remote(
            here, here, core_send.at[label, h], core_recv.at[label, h], mate
        )

    def from_mate(label, h):
        there = x.at[label, 1 - core, :, columns(h)]
        return remote(
            there, there, core_send.at[label, h], core_recv.at[label, h], mate
        )

    def along(label, h, src, device):
        return remote(
            src, x.at[label, core, :, columns(h)],
            near_send.at[label, h], near_recv.at[label, h], device,
        )

    def arrived(label, h):
        here = x.at[label, core, :, columns(h)]
        return remote(here, here, near_send.at[label, h], near_recv.at[label, h], near)

    def give(h):
        return remote(
            other.at[:, columns(h)], passed.at[:, columns(h)],
            pass_send.at[h], pass_recv.at[h], near,
        )

    def onward(h):
        return remote(
            passed.at[:, columns(h)], x.at[3, core, :, columns(h)],
            pass_send.at[h], near_recv.at[3, h], facing,
        )

    for h in range(CUTS):
        to_mate(place, h).start()

    @pl.when(outer)
    def _():
        for h in range(CUTS):
            give(h).start()
        for h in range(CUTS):
            along(0, h, x.at[0, core, :, columns(h)], near).start()

    @pl.when(inner)
    def _():
        for h in range(CUTS):
            along(1, h, x.at[1, core, :, columns(h)], near).start()
            along(2, h, other.at[:, columns(h)], facing).start()

    def turn(slot, label):
        for c in range(2):
            for r in range(0, depth, 256):
                turned[slot, :, c * depth + r : c * depth + r + 256] = x[
                    label, c, r : r + 256, pl.ds(pl.multiple_of(core * halfway, LANES), halfway)
                ].T

    def share(label, h):
        arrived(label, h).wait_recv()
        to_mate(label, h).start()

    def piece(n):
        paired = (n >= 2 * CUTS) & (n < 4 * CUTS)
        task = jnp.where(paired, 2 + n % 2, jnp.where(n < 2 * CUTS, n // CUTS, 4))
        h = jnp.where(paired, n // 2 - CUTS, n % CUTS)
        slot = jnp.where(outer, pick(task, [0, 0, 0, 1, 2]), pick(task, [0, 0, 1, 1, 1]))
        label = jnp.where(outer, pick(task, [0, 1, 3, 3, 3]), pick(task, [1, 2, 0, 3, 2]))
        return task, h, slot, label

    def one(n, side):
        if side == 0:
            src, device = part.at[n, :, 1 - col, :, pl.ds(0, wide // 2)], beside
        else:
            src, device = part.at[n, 1 - row, :, :, pl.ds(wide // 2, wide // 2)], below
        return remote(
            src, first_in.at[n, side], one_send.at[n, side], one_recv.at[n, side], device
        )

    def two(n, side):
        return remote(
            second_out.at[n, side], second_in.at[n, side],
            two_send.at[n, side], two_recv.at[n, side], below if side == 0 else beside,
        )

    owners = g.shape[0]
    eighth = owners // 2
    orders = [[[0, 1, 2], [1, 0, 2]], [[2, 0, 1], [2, 1, 0]]]
    moves = [(2, 0), (4, 0), (0, 1)]
    stages = len(moves)
    ranges = []
    for first, last in ((0, EARLY), (EARLY, TASKS)):
        ranges.append([(first * LANES + o, n) for o, n in cut((last - first) * LANES, 16, 2)])

    def owner(device):
        tt, bb = device
        side = jnp.where(low, bb, blk - 1 - bb)
        return side * eighth + tt % 2 * (eighth // 2) + tt // 2

    me = owner((t, b))

    def flip(q, j, steps, tok_bits=0):
        blk_bits = 0
        for s in range(stages):
            if steps >> s & 1:
                dt, db = moves[orders[q][j][s]]
                tok_bits ^= dt
                blk_bits ^= db
        return jnp.bitwise_xor(t, tok_bits), jnp.bitwise_xor(b, blk_bits)

    def spot(q, j, device):
        o, n = ranges[q][j]
        return g.at[owner(device), pl.ds(o, n)]

    def index_of(q, j, steps):
        return (q * 2 + j) * 2**stages + steps

    def hop(q, j, steps, s):
        index = index_of(q, j, steps | 1 << s)
        where = spot(q, j, flip(q, j, steps))
        return remote(
            where, where, hop_send.at[index], hop_recv.at[index], flip(q, j, 1 << s)
        )

    def arrival(q, j, steps):
        index = index_of(q, j, steps)
        where = spot(q, j, flip(q, j, steps))
        return remote(where, where, hop_send.at[index], hop_recv.at[index], flip(q, j, 1))

    def hand(q, j, steps, sender):
        index = index_of(q, j, steps)
        where = spot(q, j, flip(q, j, steps, 0 if sender else 1))
        return remote(where, where, hand_send.at[index], hand_recv.at[index], mate)

    def every(q, steps, s):
        for j in range(2):
            hop(q, j, steps, s).start()

    def landed(q, steps, onward_to=()):
        for j in range(2):
            arrival(q, j, steps).wait_recv()
            for s in onward_to:
                hop(q, j, steps, s).start()
            hand(q, j, steps, True).start()

    for h in range(CUTS):
        from_mate(place, h).wait_recv()
    turn(0, place)

    split = 2 * CUTS
    gap = END_LAG

    def at_step(i):
        inside = (i >= 0) & ((i < split) | ((i >= split + gap) & (i < count + gap)))
        return inside, jnp.where(i < split, i, i - gap)

    @pl.loop(0, count + gap + END_LAG)
    def _(i):
        active, n = at_step(i)

        @pl.when(active & (n >= CUTS) & (n < split))
        def _():
            h = n - CUTS

            @pl.when(inner)
            def _():
                give(h).wait_recv()
                onward(h).start()

            share(place + 1, h)
            from_mate(place + 1, h).wait_recv()

        @pl.when(i == split + gap)
        def _():
            for s in (0, 1):
                every(0, 0, s)
            for j in range(2):
                hand(0, j, 0, True).start()
            turn(1, place + 1)

        @pl.when(i == split + gap + CUTS)
        def _():
            landed(0, 1, (1,))

        @pl.when(i == split + gap + 2 * CUTS)
        def _():
            landed(0, 2)
            landed(0, 3)
            every(0, 0, 2)
            every(0, 1, 2)

        @pl.when(active & (n >= split) & (n < 2 * split) & (n % 2 == 0))
        def _():
            h = n // 2 - CUTS
            arrived(3, h).wait_recv()
            to_mate(3, h).start()

            @pl.when(inner)
            def _():
                along(3, h, x.at[3, core, :, columns(h)], near).start()
                share(0, h)
                from_mate(0, h).wait_recv()

            from_mate(3, h).wait_recv()

        @pl.when(outer & (i == 2 * split + gap))
        def _():
            turn(2, 3)

        @pl.when(active)
        def _():
            task, h, slot, label = piece(n)
            at = pl.ds(pl.multiple_of(h * wide, LANES), wide)
            right = x[label, :, :, at].reshape(2 * depth, wide)
            product = jnp.dot(turned[slot], right, preferred_element_type=jnp.float32)
            part[n] = product.astype(jnp.bfloat16).reshape(2, 2, LANES, wide)
            one(n, 0).start()
            one(n, 1).start()

        adding, m = at_step(i - ADD_LAG)

        @pl.when(adding)
        def _():
            lo, hi = pl.ds(0, wide // 2), pl.ds(wide // 2, wide // 2)
            one(m, 0).wait_recv()
            one(m, 1).wait_recv()
            wider = jnp.float32
            second_out[m, 0] = (
                part[m, 1 - row, col, :, lo].astype(wider)
                + first_in[m, 0, 1 - row].astype(wider)
            ).astype(jnp.bfloat16)
            second_out[m, 1] = (
                part[m, row, 1 - col, :, hi].astype(wider)
                + first_in[m, 1, 1 - col].astype(wider)
            ).astype(jnp.bfloat16)
            two(m, 0).start()
            two(m, 1).start()
            keep[m, 0] = part[m, row, col, :, lo].astype(wider) + first_in[
                m, 0, row
            ].astype(wider)
            keep[m, 1] = part[m, row, col, :, hi].astype(wider) + first_in[
                m, 1, col
            ].astype(wider)

        ending, e = at_step(i - END_LAG)

        @pl.when(ending)
        def _():
            task, h, _, _ = piece(e)
            two(e, 0).wait_recv()
            two(e, 1).wait_recv()
            at_rows = pl.ds(pl.multiple_of(task * LANES, LANES), LANES)
            for side in range(2):
                at = pl.ds(pl.multiple_of(h * wide + side * (wide // 2), LANES), wide // 2)
                total = keep[e, side] + second_in[e, side].astype(jnp.float32)
                g[me, at_rows, at] = total.astype(jnp.bfloat16)

    for s in range(stages):
        every(1, 0, s)
    for j in range(2):
        hand(1, j, 0, True).start()
    every(0, 2, 2)
    every(0, 3, 2)
    landed(1, 1, (1, 2))
    landed(1, 2, (2,))
    landed(1, 3, (2,))
    for steps in range(4, 8):
        landed(0, steps)
    for steps in range(4, 8):
        landed(1, steps)

    for q in range(2):
        for j in range(2):
            for steps in range(2**stages):
                hand(q, j, steps, False).wait_recv()

    half = blk // 2
    feats = g.shape[2]
    width = square.shape[1]
    labels = width // feats
    rows = LANES
    factor = 1.0 / (tokens * divisor)
    shift = damping / divisor
    eye = lax.broadcasted_iota(jnp.int32, (LANES, LANES), 0) == lax.broadcasted_iota(
        jnp.int32, (LANES, LANES), 1
    )

    def diagonal(o, k, sub, axis):
        at = pl.ds(pl.multiple_of(sub * LANES, LANES), LANES)
        own_rows = pl.ds(pl.multiple_of(k * LANES, LANES), LANES)
        block = jnp.where(eye, g[o, own_rows, at].astype(jnp.float32), 0.0)
        total = jnp.sum(block, axis=axis, keepdims=True)
        return lax.rsqrt(total / tokens + epsilon)

    for label in range(labels):
        plane, k = DIRECT[label, label]

        @pl.loop(0, eighth)
        def _(sub):
            at = pl.ds(pl.multiple_of(label * feats + sub * LANES, LANES), LANES)
            inverse[:, at] = diagonal(plane * eighth + sub, k, sub, 0)

    block_of_rows = t // 2
    row_label = jnp.where(low, block_of_rows, labels - 1 - block_of_rows)
    subs = [t % 2 * blk + bb for bb in (b, jnp.bitwise_xor(b, half))]
    diag_place = pick(row_label, [DIRECT[i, i][0] for i in range(labels)])
    diag_task = pick(row_label, [DIRECT[i, i][1] for i in range(labels)])
    inverse_rows = jnp.concatenate(
        [diagonal(diag_place * eighth + sub, diag_task, sub, 1) for sub in subs], axis=0
    )

    for label in range(labels):

        @pl.when(row_label == label)
        def _():
            for j in range(labels):
                cols = slice(j * feats, (j + 1) * feats)
                for s, sub in enumerate(subs):
                    if (label, j) in DIRECT:
                        plane, k = DIRECT[label, j]
                        value = g[plane * eighth + sub, k * LANES : (k + 1) * LANES, :]
                    else:
                        plane, k = DIRECT[j, label]
                        at = pl.ds(pl.multiple_of(sub * LANES, LANES), LANES)
                        value = g[
                            plane * eighth : (plane + 1) * eighth, k * LANES : (k + 1) * LANES, at
                        ]
                        value = value.reshape(feats, LANES).T
                    mixed[s * rows : (s + 1) * rows, cols] = value

    step = feats // CUTS
    starts = [row_label * feats + sub * LANES for sub in subs]

    def identity(first_col, size):
        at = first_col + lax.broadcasted_iota(jnp.int32, (rows, size), 1)
        row = lax.broadcasted_iota(jnp.int32, (rows, size), 0)
        return jnp.concatenate(
            [(at - start == row).astype(jnp.float32) for start in starts], axis=0
        )

    def scaled(first_col, size):
        at = pl.ds(first_col, size)
        return mixed[:, at].astype(jnp.float32) * (
            factor * inverse_rows
        ) * inverse[:, at] + shift * identity(first_col, size)

    def fold(label, h):
        total = None
        for k in range(labels):
            lhs = left[:, k * feats : (k + 1) * feats]
            if (k, label) in DIRECT:
                plane, task = DIRECT[k, label]
                rhs = g[
                    plane * eighth : (plane + 1) * eighth,
                    task * LANES : (task + 1) * LANES,
                    pl.ds(pl.multiple_of(h * step, LANES), step),
                ].reshape(feats, step)
                product = jnp.dot(lhs, rhs, preferred_element_type=jnp.float32)
            else:
                plane, task = DIRECT[label, k]
                few = step // LANES
                rhs = g[
                    pl.ds(plane * eighth + h * few, few), task * LANES : (task + 1) * LANES, :
                ].reshape(step, feats)
                product = lax.dot_general(
                    lhs, rhs, (((1,), (1,)), ((), ())), preferred_element_type=jnp.float32
                )
            total = product if total is None else total + product
        return total

    @pl.loop(0, labels * CUTS)
    def _(i):
        start_col = pl.multiple_of(i * step, step)
        at = pl.ds(start_col, step)
        left[:, at] = (scaled(start_col, step) * inverse[:, at]).astype(jnp.bfloat16)

    for label in range(labels):

        @pl.loop(0, CUTS)
        def _(h):
            start_col = pl.multiple_of(label * feats + h * step, step)
            at = pl.ds(start_col, step)
            square[:, at] = fold(label, h) * (inverse[:, at] * factor) + shift * scaled(
                start_col, step
            )

    @pl.loop(0, labels * CUTS)
    def _(i):
        start_col = pl.multiple_of(i * step, step)
        at = pl.ds(start_col, step)
        left[:, at] = (square[:, at] * inverse[:, at]).astype(jnp.bfloat16)

    def swap(label, h):
        to = jnp.where(low, label, labels - 1 - label)
        at = pl.ds(pl.multiple_of(to * feats + h * step, LANES), step)
        index = label * CUTS + h
        return at, remote(
            sent.at[:, at], came.at[:, at], out_sem.at[index], in_sem.at[index], across
        )

    for label in range(labels):

        @pl.loop(0, CUTS)
        def _(h):
            start_col = pl.multiple_of(label * feats + h * step, step)
            at = pl.ds(start_col, step)
            squared = square[:, at]
            cube = fold(label, h) * (inverse[:, at] * factor) + shift * squared
            result = (
                4.0 * identity(start_col, step) - 6.0 * scaled(start_col, step)
                + 4.0 * squared - cube
            )
            to, copy = swap(label, h)
            kept[:, to] = result[:rows]
            sent[:, to] = result[rows:].astype(jnp.bfloat16)
            copy.start()

    for label in range(labels):

        @pl.loop(0, CUTS)
        def _(h):
            _, copy = swap(label, h)
            copy.wait_recv()
            copy.wait_send()

    @pl.loop(0, count)
    def _(n):
        for side in range(2):
            one(n, side).wait_send()
            two(n, side).wait_send()

    for h in range(CUTS):
        to_mate(place, h).wait_send()
        to_mate(place + 1, h).wait_send()
        to_mate(3, h).wait_send()

    @pl.when(outer)
    def _():
        for h in range(CUTS):
            give(h).wait_send()
            along(0, h, x.at[0, core, :, columns(h)], near).wait_send()

    @pl.when(inner)
    def _():
        for h in range(CUTS):
            along(1, h, x.at[1, core, :, columns(h)], near).wait_send()
            along(2, h, other.at[:, columns(h)], facing).wait_send()
            along(3, h, x.at[3, core, :, columns(h)], near).wait_send()
            onward(h).wait_send()
            to_mate(0, h).wait_send()

    for q in range(2):
        for j in range(2):
            for steps in range(2**stages):
                hand(q, j, steps, True).wait_send()
                if steps:
                    arrival(q, j, steps).wait_send()


def cut(length, unit, pieces):
    units = length // unit
    sizes = [(units // pieces + (1 if i < units % pieces else 0)) * unit for i in range(pieces)]
    return [(sum(sizes[:i]), sizes[i]) for i in range(pieces)]


def call(kernel, outs, scratch, collective_id, space, *operands):
    return pl.pallas_call(
        kernel,
        out_shape=outs,
        in_specs=[pl.BlockSpec(memory_space=space)] * len(operands),
        out_specs=[pl.BlockSpec(memory_space=pltpu.VMEM)] * len(outs),
        scratch_shapes=scratch,
        compiler_params=pltpu.CompilerParams(
            collective_id=collective_id, has_side_effects=True, vmem_limit_bytes=63 * 1024 * 1024
        ),
    )(*operands)


def split_body(tok, blk, activations, out_grads):
    depth, feats = activations.shape
    tokens = depth * tok
    width = feats * blk
    rows = width // (tok * blk)
    low = lax.axis_index("blk") < blk // 2
    count = TASKS * CUTS
    wide = feats // CUTS
    bf16, f32 = jnp.bfloat16, jnp.float32
    dma = pltpu.SemaphoreType.DMA
    steps = blk * CUTS
    slots = 2 * 2 * 8
    kept, came = call(
        functools.partial(factor_kernel, tok, blk, tokens),
        [jax.ShapeDtypeStruct((rows, width), f32), jax.ShapeDtypeStruct((rows, width), bf16)],
        [
            pltpu.VMEM((blk, 2, depth, feats), bf16),
            pltpu.VMEM((depth, feats), bf16),
            pltpu.VMEM((depth, feats), bf16),
            pltpu.VMEM((3, feats // 2, 2 * depth), bf16),
            pltpu.VMEM((count, 2, 2, rows, wide), bf16),
            pltpu.VMEM((count, 2, 2, rows, wide // 2), bf16),
            pltpu.VMEM((count, 2, rows, wide // 2), bf16),
            pltpu.VMEM((count, 2, rows, wide // 2), bf16),
            pltpu.VMEM((count, 2, rows, wide // 2), f32),
            pltpu.VMEM((2 * tok, TASKS * rows, feats), bf16),
            pltpu.VMEM((2 * rows, width), bf16),
            pltpu.VMEM((2 * rows, width), f32),
            pltpu.VMEM((2 * rows, width), bf16),
            pltpu.VMEM((1, width), f32),
            pltpu.VMEM((rows, width), bf16),
            dma((2,)),
            dma((blk, CUTS)), dma((blk, CUTS)),
            dma((CUTS,)), dma((CUTS,)),
            dma((blk, CUTS)), dma((blk, CUTS)),
            dma((count, 2)), dma((count, 2)), dma((count, 2)), dma((count, 2)),
            dma((slots,)), dma((slots,)), dma((slots,)), dma((slots,)),
            dma((steps,)), dma((steps,)),
        ],
        0, pl.ANY, activations, out_grads,
    )
    came = came.astype(f32)
    return jnp.where(low, kept, came), jnp.where(low, came, kept)


def solution(mesh):
    tok, blk = mesh.shape["tok"], mesh.shape["blk"]
    placed = (P("tok", "blk"), P("tok", "blk"))

    def body(activations, out_grads):
        depth, feats = activations.shape
        whole = max(depth * tok, feats * blk) * feats * blk * activations.dtype.itemsize
        cube = tok == 2 * blk and blk == 4 and feats == tok * LANES
        if whole <= gathered_budget and cube:
            return split_body(tok, blk, activations, out_grads)
        return tiled_body(activations, out_grads)

    return jax.shard_map(
        body,
        mesh=mesh,
        in_specs=placed,
        out_specs=(P(("tok", "blk"), None), P(("tok", "blk"), None)),
        check_vma=False,
    )
```

```python
import functools

import jax
import jax.numpy as jnp
import numpy as np
from jax import lax
from jax.experimental import pallas as pl
from jax.experimental.pallas import tpu as pltpu
from jax.sharding import PartitionSpec as P

damping = 0.3
epsilon = 1e-06
divisor = 2.0
gathered_budget = 32 * 1024 * 1024
LANES = 128
MESH = pl.DeviceIdType.MESH


def column_squares(data):
    values = data.astype(jnp.float32)
    return jnp.sum(values * values, axis=0)


def fold_product(row_block, tile):
    return jnp.dot(
        row_block,
        lax.all_gather(tile, "tok", axis=0, tiled=True),
        preferred_element_type=jnp.float32,
    )


def newton_steps(scaled, identity):
    half = scaled.astype(jnp.bfloat16)
    row_block = lax.all_gather(half, "blk", axis=1, tiled=True)
    square = fold_product(row_block, half)
    cube = fold_product(row_block, square.astype(jnp.bfloat16))
    return 4.0 * identity - 6.0 * scaled + 4.0 * square - cube


def tiled_body(activations, out_grads):
    tok_count = lax.axis_size("tok")
    blk_count = lax.axis_size("blk")
    tok_id = lax.axis_index("tok")
    blk_id = lax.axis_index("blk")
    token_count = activations.shape[0] * tok_count
    tile_cols = activations.shape[1]
    tile_rows = tile_cols * blk_count // tok_count
    row_ids = tok_id * tile_rows + jnp.arange(tile_rows, dtype=jnp.int32)
    col_ids = blk_id * tile_cols + jnp.arange(tile_cols, dtype=jnp.int32)
    identity = (row_ids[:, None] == col_ids[None, :]).astype(jnp.float32)

    def inverse_tile(local):
        full = lax.all_gather(local, "blk", axis=1, tiled=True)
        sums = lax.psum(column_squares(full).astype(jnp.bfloat16), "tok").astype(jnp.float32)
        gram_tile = lax.psum_scatter(
            lax.dot_general(
                full, local, (((0,), (0,)), ((), ())), preferred_element_type=jnp.float32
            ).astype(jnp.bfloat16),
            "tok",
            scatter_dimension=0,
            tiled=True,
        ).astype(jnp.float32)
        inverse = lax.rsqrt(sums / token_count + epsilon)
        inverse_rows = lax.dynamic_slice_in_dim(inverse, tok_id * tile_rows, tile_rows)
        inverse_cols = lax.dynamic_slice_in_dim(inverse, blk_id * tile_cols, tile_cols)
        damped = (
            gram_tile / token_count * inverse_rows[:, None] * inverse_cols[None, :]
            + damping * identity
        )
        result_tile = newton_steps(damped / divisor, identity)
        return lax.all_to_all(
            result_tile.astype(jnp.bfloat16), "blk", split_axis=0, concat_axis=1, tiled=True
        ).astype(result_tile.dtype)

    return inverse_tile(activations), inverse_tile(out_grads)


DIRECT = {
    (0, 1): (0, 0), (0, 3): (0, 1), (1, 3): (0, 2),
    (1, 2): (1, 0), (2, 0): (1, 1), (2, 3): (1, 2),
}
DIAGONAL = [(0, 0), (1, 0), (1, 1), (0, 1)]
CUTS = 4
SHORT = 3
COUNT = 2 * SHORT + 3 * CUTS
ADD_LAG = 3
END_LAG = 6


def pick(index, values):
    out = values[-1]
    for i in range(len(values) - 2, -1, -1):
        out = jnp.where(index == i, values[i], out)
    return out


def remote(src, dst, send, recv, device):
    return pltpu.make_async_remote_copy(
        src_ref=src, dst_ref=dst, send_sem=send, recv_sem=recv,
        device_id=device, device_id_type=MESH,
    )


def meet(peers):
    barrier = pltpu.get_barrier_semaphore()
    for peer in peers:
        pl.semaphore_signal(barrier, inc=1, device_id=peer, device_id_type=MESH)
    pl.semaphore_wait(barrier, len(peers))


def factor_kernel(
    tok, blk, tokens, acts, grads, kept, came,
    x, other, passed, turned, part, first_in, second_out, second_in, keep,
    g, diag, mixed, square, left, inverse, sent,
    load_sem, near_send, near_recv, pass_send, pass_recv, core_send, core_recv,
    one_send, one_recv, two_send, two_recv,
    hop_send, hop_recv, hand_send, hand_recv, out_sem, in_sem,
):
    t = lax.axis_index("tok")
    b = lax.axis_index("blk")
    low = b < blk // 2
    place = jnp.where(low, b, blk - 1 - b)
    outer = place == 0
    inner = place == 1
    core, col, row = t % 2, t // 2 % 2, t // 4
    mate = (jnp.bitwise_xor(t, 1), b)
    beside = (jnp.bitwise_xor(t, 2), b)
    below = (jnp.bitwise_xor(t, 4), b)
    near = (t, jnp.bitwise_xor(b, 1))
    facing = (t, blk - 1 - b)
    across = (t, jnp.bitwise_xor(b, blk // 2))
    depth, feats = other.shape
    wide = feats // CUTS
    halfway = feats // 2
    count = COUNT
    first = SHORT
    split = SHORT + CUTS
    tail = split + 2 * CUTS

    def load(ref, dst, index):
        return pltpu.make_async_copy(ref, dst, load_sem.at[index])

    @pl.when(low)
    def _():
        load(acts, x.at[place, core], 0).start()
        load(grads, other, 1).start()

    @pl.when(jnp.logical_not(low))
    def _():
        load(grads, x.at[place, core], 0).start()
        load(acts, other, 1).start()

    meet([mate, beside, below, near, facing, across])
    load(acts, x.at[place, core], 0).wait()
    load(grads, other, 1).wait()

    def columns(h):
        return pl.ds(pl.multiple_of(h * wide, LANES), wide)

    def to_mate(label, h):
        here = x.at[label, core, :, columns(h)]
        return remote(
            here, here, core_send.at[label, h], core_recv.at[label, h], mate
        )

    def from_mate(label, h):
        there = x.at[label, 1 - core, :, columns(h)]
        return remote(
            there, there, core_send.at[label, h], core_recv.at[label, h], mate
        )

    def along(label, h, src, device):
        return remote(
            src, x.at[label, core, :, columns(h)],
            near_send.at[label, h], near_recv.at[label, h], device,
        )

    def arrived(label, h):
        here = x.at[label, core, :, columns(h)]
        return remote(here, here, near_send.at[label, h], near_recv.at[label, h], near)

    def give(h):
        return remote(
            other.at[:, columns(h)], passed.at[:, columns(h)],
            pass_send.at[h], pass_recv.at[h], near,
        )

    def onward(h):
        return remote(
            passed.at[:, columns(h)], x.at[3, core, :, columns(h)],
            pass_send.at[h], near_recv.at[3, h], facing,
        )

    for h in range(CUTS):
        to_mate(place, h).start()

    @pl.when(outer)
    def _():
        for h in range(CUTS):
            give(h).start()
        for h in range(CUTS):
            along(0, h, x.at[0, core, :, columns(h)], near).start()

    @pl.when(inner)
    def _():
        for h in range(CUTS):
            along(1, h, x.at[1, core, :, columns(h)], near).start()
            along(2, h, other.at[:, columns(h)], facing).start()

    def turn(slot, label, side):
        at = pl.ds(pl.multiple_of(side * halfway, LANES), halfway)
        for c in range(2):
            for r in range(0, depth, 256):
                turned[slot, :, c * depth + r : c * depth + r + 256] = x[
                    label, c, r : r + 256, at
                ].T

    def share(label, h):
        arrived(label, h).wait_recv()
        to_mate(label, h).start()

    def piece(n):
        task = jnp.where(
            n < first, 0,
            jnp.where(n < split, 1, jnp.where(n < tail, 2 + (n - split) % 2, 4)),
        )
        h = jnp.where(
            n < first, n,
            jnp.where(
                n < split, n - first, jnp.where(n < tail, (n - split) // 2, n - tail)
            ),
        )
        whole = (task > 0) & (task < 4)
        slot = jnp.where(outer, pick(task, [0, 0, 0, 1, 2]), pick(task, [0, 0, 1, 1, 1]))
        label = jnp.where(outer, pick(task, [0, 1, 3, 3, 3]), pick(task, [1, 2, 0, 3, 2]))
        corner = jnp.logical_not(whole) & (h == 2)
        slot = jnp.where(corner, 3, slot)
        inside = core * (CUTS // 2) + h
        at = jnp.where(whole, h, jnp.where(h == 2, CUTS // 2 + core, inside))
        return task, h, slot, label, at, whole

    def one(n, side):
        if side == 0:
            src, device = part.at[n, :, 1 - col, :, pl.ds(0, wide // 2)], beside
        else:
            src, device = part.at[n, 1 - row, :, :, pl.ds(wide // 2, wide // 2)], below
        return remote(
            src, first_in.at[n, side], one_send.at[n, side], one_recv.at[n, side], device
        )

    def two(n, side):
        return remote(
            second_out.at[n, side], second_in.at[n, side],
            two_send.at[n, side], two_recv.at[n, side], below if side == 0 else beside,
        )

    owners = g.shape[0]
    eighth = owners // 2
    early, late = [[0, 1, 2], [1, 0, 2]], [[2, 0, 1], [2, 1, 0]]
    orders = [early, early, late, late]
    groups = len(orders)
    moves = [(2, 0), (4, 0), (0, 1)]
    stages = len(moves)
    ranges = []
    for ref, at_row, size in (
        (diag, 0, LANES), (g, 0, LANES), (g, LANES, 2 * LANES), (diag, LANES, LANES)
    ):
        ranges.append([(ref, at_row + o, n) for o, n in cut(size, 16, 2)])

    def owner(device):
        tt, bb = device
        side = jnp.where(low, bb, blk - 1 - bb)
        return side * eighth + tt % 2 * (eighth // 2) + tt // 2

    me = owner((t, b))

    def flip(q, j, steps, tok_bits=0):
        blk_bits = 0
        for s in range(stages):
            if steps >> s & 1:
                dt, db = moves[orders[q][j][s]]
                tok_bits ^= dt
                blk_bits ^= db
        return jnp.bitwise_xor(t, tok_bits), jnp.bitwise_xor(b, blk_bits)

    def spot(q, j, device):
        ref, o, n = ranges[q][j]
        return ref.at[owner(device), pl.ds(o, n)]

    def index_of(q, j, steps):
        return (q * 2 + j) * 2**stages + steps

    def hop(q, j, steps, s):
        index = index_of(q, j, steps | 1 << s)
        where = spot(q, j, flip(q, j, steps))
        return remote(
            where, where, hop_send.at[index], hop_recv.at[index], flip(q, j, 1 << s)
        )

    def arrival(q, j, steps):
        index = index_of(q, j, steps)
        where = spot(q, j, flip(q, j, steps))
        return remote(where, where, hop_send.at[index], hop_recv.at[index], flip(q, j, 1))

    def hand(q, j, steps, sender):
        index = index_of(q, j, steps)
        where = spot(q, j, flip(q, j, steps, 0 if sender else 1))
        return remote(where, where, hand_send.at[index], hand_recv.at[index], mate)

    def every(q, steps, s):
        for j in range(2):
            hop(q, j, steps, s).start()

    def landed(q, steps, onward_to=()):
        for j in range(2):
            arrival(q, j, steps).wait_recv()
            for s in onward_to:
                hop(q, j, steps, s).start()
            hand(q, j, steps, True).start()

    def begin(q):
        for s in range(stages):
            every(q, 0, s)
        for j in range(2):
            hand(q, j, 0, True).start()

    def forward(h):
        arrived(3, h).wait_recv()
        to_mate(3, h).start()

        @pl.when(inner)
        def _():
            along(3, h, x.at[3, core, :, columns(h)], near).start()

    for h in range(CUTS):
        from_mate(place, h).wait_recv()
    turn(0, place, core)
    turn(3, place, 0)
    gap = END_LAG

    def at_step(i):
        n = jnp.where(i < first, i, jnp.where(i < split + gap, i - gap, i - 2 * gap))
        low_part = (i >= 0) & (i < first)
        mid_part = (i >= first + gap) & (i < split + gap)
        return low_part | mid_part | ((i >= split + 2 * gap) & (i < count + 2 * gap)), n

    @pl.loop(0, count + 2 * gap + END_LAG)
    def _(i):
        active, n = at_step(i)

        @pl.when(i == first + gap)
        def _():
            for s in (0, 1):
                every(0, 0, s)
            for j in range(2):
                hand(0, j, 0, True).start()

        @pl.when(active & (n >= first) & (n < split))
        def _():
            h = n - first

            @pl.when(inner)
            def _():
                give(h).wait_recv()
                onward(h).start()

            share(place + 1, h)
            from_mate(place + 1, h).wait_recv()

        @pl.when(i == split + gap)
        def _():
            landed(0, 1, (1,))
            turn(1, place + 1, core)

        @pl.when(inner & (i == split + gap + gap // 2))
        def _():
            forward(0)

        @pl.when(i == split + 2 * gap)
        def _():
            landed(0, 2)
            landed(0, 3)
            for s in (0, 1):
                every(1, 0, s)
            for j in range(2):
                hand(1, j, 0, True).start()

        @pl.when(i == split + 2 * gap + CUTS)
        def _():
            landed(1, 1, (1,))

        @pl.when(i == tail + 2 * gap)
        def _():
            every(0, 0, 2)
            every(0, 1, 2)

        @pl.when(i == tail + 2 * gap + SHORT)
        def _():
            landed(1, 2)
            landed(1, 3)

        @pl.when(i == tail + 2 * gap + END_LAG)
        def _():
            begin(2)

        @pl.when(active & (n >= split) & (n < tail) & ((n - split) % 2 == 0))
        def _():
            h = (n - split) // 2

            @pl.when(outer | (h > 0))
            def _():
                forward(h)

            @pl.when(inner)
            def _():
                share(0, h)
                from_mate(0, h).wait_recv()

            from_mate(3, h).wait_recv()

        @pl.when(i == tail + 2 * gap)
        def _():
            turn(3, jnp.where(outer, 3, 2), 0)

            @pl.when(outer)
            def _():
                turn(2, 3, core)

        @pl.when(active)
        def _():
            task, h, slot, label, cut_at, _ = piece(n)
            at = pl.ds(pl.multiple_of(cut_at * wide, LANES), wide)
            right = x[label, :, :, at].reshape(2 * depth, wide)
            product = jnp.dot(turned[slot], right, preferred_element_type=jnp.float32)
            part[n] = product.astype(jnp.bfloat16).reshape(2, 2, LANES, wide)
            one(n, 0).start()
            one(n, 1).start()

        adding, m = at_step(i - ADD_LAG)

        @pl.when(adding)
        def _():
            lo, hi = pl.ds(0, wide // 2), pl.ds(wide // 2, wide // 2)
            one(m, 0).wait_recv()
            one(m, 1).wait_recv()
            wider = jnp.float32
            second_out[m, 0] = (
                part[m, 1 - row, col, :, lo].astype(wider)
                + first_in[m, 0, 1 - row].astype(wider)
            ).astype(jnp.bfloat16)
            second_out[m, 1] = (
                part[m, row, 1 - col, :, hi].astype(wider)
                + first_in[m, 1, 1 - col].astype(wider)
            ).astype(jnp.bfloat16)
            two(m, 0).start()
            two(m, 1).start()
            keep[m, 0] = part[m, row, col, :, lo].astype(wider) + first_in[
                m, 0, row
            ].astype(wider)
            keep[m, 1] = part[m, row, col, :, hi].astype(wider) + first_in[
                m, 1, col
            ].astype(wider)

        ending, e = at_step(i - END_LAG)

        @pl.when(ending)
        def _():
            task, h, _, _, _, whole = piece(e)
            two(e, 0).wait_recv()
            two(e, 1).wait_recv()
            for side in range(2):
                at = pl.ds(pl.multiple_of(h * wide + side * (wide // 2), LANES), wide // 2)
                total = keep[e, side] + second_in[e, side].astype(jnp.float32)
                total = total.astype(jnp.bfloat16)

                @pl.when(whole)
                def _():
                    g[me, pl.ds(pl.multiple_of((task - 1) * LANES, LANES), LANES), at] = total

                @pl.when(jnp.logical_not(whole))
                def _():
                    g_row = pl.multiple_of(task // 4 * LANES, LANES)
                    diag[me, pl.ds(g_row, LANES), at] = total

    def received(q):
        for j in range(2):
            for steps in range(2**stages):
                hand(q, j, steps, False).wait_recv()

    half = blk // 2
    width = square.shape[1]
    labels = width // feats
    rows = LANES
    factor = 1.0 / (tokens * divisor)
    shift = damping / divisor
    eye = lax.broadcasted_iota(jnp.int32, (LANES, LANES), 0) == lax.broadcasted_iota(
        jnp.int32, (LANES, LANES), 1
    )
    quarter = eighth // 2

    def diagonal(plane, k, sub, axis):
        at = pl.ds(pl.multiple_of(sub % quarter * LANES, LANES), LANES)
        own_rows = pl.ds(pl.multiple_of(k * LANES, LANES), LANES)
        block = jnp.where(eye, diag[plane * eighth + sub, own_rows, at].astype(jnp.float32), 0.0)
        total = jnp.sum(block, axis=axis, keepdims=True)
        return lax.rsqrt(total / tokens + epsilon)

    def rebuild(which):
        for label in range(labels):
            plane, k = DIAGONAL[label]
            if k != which:
                continue

            @pl.loop(0, eighth)
            def _(sub):
                at = pl.ds(pl.multiple_of(label * feats + sub * LANES, LANES), LANES)
                inverse[:, at] = diagonal(plane, k, sub, 0)

            own_rows = slice(k * LANES, (k + 1) * LANES)
            ends = [
                slice(plane * eighth + c * quarter, plane * eighth + (c + 1) * quarter)
                for c in range(2)
            ]
            for c in range(2):
                block = diag[ends[c], own_rows, :halfway].reshape(halfway, halfway)
                x[label, c, :, c * halfway : (c + 1) * halfway] = block
                lo = halfway + c * wide
                block = diag[ends[c], own_rows, halfway : halfway + wide].reshape(halfway, wide)
                x[label, 0, :, lo : lo + wide] = block
                x[label, 1, c * wide : (c + 1) * wide, :halfway] = block.T

    begin(3)
    every(0, 2, 2)
    every(0, 3, 2)
    for steps in range(4):
        every(1, steps, 2)
    for h in range(CUTS):
        to_mate(place, h).wait_send()
        to_mate(place + 1, h).wait_send()
        to_mate(3, h).wait_send()

    @pl.when(outer)
    def _():
        for h in range(CUTS):
            give(h).wait_send()
            along(0, h, x.at[0, core, :, columns(h)], near).wait_send()

    @pl.when(inner)
    def _():
        for h in range(CUTS):
            along(1, h, x.at[1, core, :, columns(h)], near).wait_send()
            along(2, h, other.at[:, columns(h)], facing).wait_send()
            along(3, h, x.at[3, core, :, columns(h)], near).wait_send()
            onward(h).wait_send()
            to_mate(0, h).wait_send()

    for q in (2, 3):
        landed(q, 1, (1, 2))
        landed(q, 2, (2,))
        landed(q, 3, (2,))
    for q in range(groups):
        for steps in range(4, 8):
            landed(q, steps)
        if q == 0:
            received(0)
            rebuild(0)
    for q in range(1, groups):
        received(q)
    rebuild(1)

    block_of_rows = t // 2
    row_label = jnp.where(low, block_of_rows, labels - 1 - block_of_rows)
    subs = [t % 2 * blk + bb for bb in (b, jnp.bitwise_xor(b, half))]
    diag_plane = pick(row_label, [d[0] for d in DIAGONAL])
    diag_task = pick(row_label, [d[1] for d in DIAGONAL])
    inverse_rows = jnp.concatenate(
        [diagonal(diag_plane, diag_task, sub, 1) for sub in subs], axis=0
    )

    for label in range(labels):

        @pl.when(row_label == label)
        def _():
            for j in range(labels):
                cols = slice(j * feats, (j + 1) * feats)
                for s, sub in enumerate(subs):
                    if label == j:
                        at = pl.ds(pl.multiple_of(sub % quarter * LANES, LANES), LANES)
                        value = x[label, core, at, :]
                    elif (label, j) in DIRECT:
                        plane, k = DIRECT[label, j]
                        value = g[plane * eighth + sub, k * LANES : (k + 1) * LANES, :]
                    else:
                        plane, k = DIRECT[j, label]
                        at = pl.ds(pl.multiple_of(sub * LANES, LANES), LANES)
                        value = g[
                            plane * eighth : (plane + 1) * eighth, k * LANES : (k + 1) * LANES, at
                        ]
                        value = value.reshape(feats, LANES).T
                    mixed[s * rows : (s + 1) * rows, cols] = value

    step = feats // CUTS
    starts = [row_label * feats + sub * LANES for sub in subs]

    def identity(first_col, size):
        at = first_col + lax.broadcasted_iota(jnp.int32, (rows, size), 1)
        row = lax.broadcasted_iota(jnp.int32, (rows, size), 0)
        return jnp.concatenate(
            [(at - start == row).astype(jnp.float32) for start in starts], axis=0
        )

    def scaled(first_col, size):
        at = pl.ds(first_col, size)
        return mixed[:, at].astype(jnp.float32) * (
            factor * inverse_rows
        ) * inverse[:, at] + shift * identity(first_col, size)

    def fold(label, h):
        total = None
        for k in range(labels):
            lhs = left[:, k * feats : (k + 1) * feats]
            if k == label:
                at = pl.ds(pl.multiple_of(h * step, LANES), step)
                rhs = x[label, :, :, at].reshape(feats, step)
                product = jnp.dot(lhs, rhs, preferred_element_type=jnp.float32)
            elif (k, label) in DIRECT:
                plane, task = DIRECT[k, label]
                rhs = g[
                    plane * eighth : (plane + 1) * eighth,
                    task * LANES : (task + 1) * LANES,
                    pl.ds(pl.multiple_of(h * step, LANES), step),
                ].reshape(feats, step)
                product = jnp.dot(lhs, rhs, preferred_element_type=jnp.float32)
            else:
                plane, task = DIRECT[label, k]
                few = step // LANES
                rhs = g[
                    pl.ds(plane * eighth + h * few, few), task * LANES : (task + 1) * LANES, :
                ].reshape(step, feats)
                product = lax.dot_general(
                    lhs, rhs, (((1,), (1,)), ((), ())), preferred_element_type=jnp.float32
                )
            total = product if total is None else total + product
        return total

    @pl.loop(0, labels * CUTS)
    def _(i):
        start_col = pl.multiple_of(i * step, step)
        at = pl.ds(start_col, step)
        left[:, at] = (scaled(start_col, step) * inverse[:, at]).astype(jnp.bfloat16)

    for label in range(labels):

        @pl.loop(0, CUTS)
        def _(h):
            start_col = pl.multiple_of(label * feats + h * step, step)
            at = pl.ds(start_col, step)
            square[:, at] = fold(label, h) * (inverse[:, at] * factor) + shift * scaled(
                start_col, step
            )

    @pl.loop(0, labels * CUTS)
    def _(i):
        start_col = pl.multiple_of(i * step, step)
        at = pl.ds(start_col, step)
        left[:, at] = (square[:, at] * inverse[:, at]).astype(jnp.bfloat16)

    def swap(label, h):
        to = jnp.where(low, label, labels - 1 - label)
        at = pl.ds(pl.multiple_of(to * feats + h * step, LANES), step)
        index = label * CUTS + h
        return at, remote(
            sent.at[:, at], came.at[:, at], out_sem.at[index], in_sem.at[index], across
        )

    for label in range(labels):

        @pl.loop(0, CUTS)
        def _(h):
            start_col = pl.multiple_of(label * feats + h * step, step)
            at = pl.ds(start_col, step)
            squared = square[:, at]
            cube = fold(label, h) * (inverse[:, at] * factor) + shift * squared
            result = (
                4.0 * identity(start_col, step) - 6.0 * scaled(start_col, step)
                + 4.0 * squared - cube
            )
            to, copy = swap(label, h)
            kept[:, to] = result[:rows]
            sent[:, to] = result[rows:].astype(jnp.bfloat16)
            copy.start()

    @pl.loop(0, count)
    def _(n):
        for side in range(2):
            one(n, side).wait_send()
            two(n, side).wait_send()

    for q in range(groups):
        for j in range(2):
            for steps in range(2**stages):
                hand(q, j, steps, True).wait_send()
                if steps:
                    arrival(q, j, steps).wait_send()

    for label in range(labels):

        @pl.loop(0, CUTS)
        def _(h):
            _, copy = swap(label, h)
            copy.wait_recv()
            copy.wait_send()


def cut(length, unit, pieces):
    units = length // unit
    sizes = [(units // pieces + (1 if i < units % pieces else 0)) * unit for i in range(pieces)]
    return [(sum(sizes[:i]), sizes[i]) for i in range(pieces)]


def call(kernel, outs, scratch, collective_id, space, *operands):
    return pl.pallas_call(
        kernel,
        out_shape=outs,
        in_specs=[pl.BlockSpec(memory_space=space)] * len(operands),
        out_specs=[pl.BlockSpec(memory_space=pltpu.VMEM)] * len(outs),
        scratch_shapes=scratch,
        compiler_params=pltpu.CompilerParams(
            collective_id=collective_id, has_side_effects=True, vmem_limit_bytes=63 * 1024 * 1024
        ),
    )(*operands)


def split_body(tok, blk, activations, out_grads):
    depth, feats = activations.shape
    tokens = depth * tok
    width = feats * blk
    rows = width // (tok * blk)
    low = lax.axis_index("blk") < blk // 2
    count = COUNT
    wide = feats // CUTS
    bf16, f32 = jnp.bfloat16, jnp.float32
    dma = pltpu.SemaphoreType.DMA
    steps = blk * CUTS
    slots = 4 * 2 * 8
    kept, came = call(
        functools.partial(factor_kernel, tok, blk, tokens),
        [jax.ShapeDtypeStruct((rows, width), f32), jax.ShapeDtypeStruct((rows, width), bf16)],
        [
            pltpu.VMEM((blk, 2, depth, feats), bf16),
            pltpu.VMEM((depth, feats), bf16),
            pltpu.VMEM((depth, feats), bf16),
            pltpu.VMEM((4, feats // 2, 2 * depth), bf16),
            pltpu.VMEM((count, 2, 2, rows, wide), bf16),
            pltpu.VMEM((count, 2, 2, rows, wide // 2), bf16),
            pltpu.VMEM((count, 2, rows, wide // 2), bf16),
            pltpu.VMEM((count, 2, rows, wide // 2), bf16),
            pltpu.VMEM((count, 2, rows, wide // 2), f32),
            pltpu.VMEM((2 * tok, 3 * rows, feats), bf16),
            pltpu.VMEM((2 * tok, 2 * rows, feats // CUTS * SHORT), bf16),
            pltpu.VMEM((2 * rows, width), bf16),
            pltpu.VMEM((2 * rows, width), f32),
            pltpu.VMEM((2 * rows, width), bf16),
            pltpu.VMEM((1, width), f32),
            pltpu.VMEM((rows, width), bf16),
            dma((2,)),
            dma((blk, CUTS)), dma((blk, CUTS)),
            dma((CUTS,)), dma((CUTS,)),
            dma((blk, CUTS)), dma((blk, CUTS)),
            dma((count, 2)), dma((count, 2)), dma((count, 2)), dma((count, 2)),
            dma((slots,)), dma((slots,)), dma((slots,)), dma((slots,)),
            dma((steps,)), dma((steps,)),
        ],
        0, pl.ANY, activations, out_grads,
    )
    came = came.astype(f32)
    return jnp.where(low, kept, came), jnp.where(low, came, kept)


def solution(mesh):
    tok, blk = mesh.shape["tok"], mesh.shape["blk"]
    placed = (P("tok", "blk"), P("tok", "blk"))

    def body(activations, out_grads):
        depth, feats = activations.shape
        whole = max(depth * tok, feats * blk) * feats * blk * activations.dtype.itemsize
        cube = tok == 2 * blk and blk == 4 and feats == tok * LANES == 2 * depth
        if whole <= gathered_budget and cube:
            return split_body(tok, blk, activations, out_grads)
        return tiled_body(activations, out_grads)

    return jax.shard_map(
        body,
        mesh=mesh,
        in_specs=placed,
        out_specs=(P(("tok", "blk"), None), P(("tok", "blk"), None)),
        check_vma=False,
    )
```

```python
import functools

import jax
import jax.numpy as jnp
import numpy as np
from jax import lax
from jax.experimental import pallas as pl
from jax.experimental.pallas import tpu as pltpu
from jax.sharding import PartitionSpec as P

damping = 0.3
epsilon = 1e-06
divisor = 2.0
gathered_budget = 32 * 1024 * 1024
LANES = 128
MESH = pl.DeviceIdType.MESH


def column_squares(data):
    values = data.astype(jnp.float32)
    return jnp.sum(values * values, axis=0)


def fold_product(row_block, tile):
    return jnp.dot(
        row_block,
        lax.all_gather(tile, "tok", axis=0, tiled=True),
        preferred_element_type=jnp.float32,
    )


def newton_steps(scaled, identity):
    half = scaled.astype(jnp.bfloat16)
    row_block = lax.all_gather(half, "blk", axis=1, tiled=True)
    square = fold_product(row_block, half)
    cube = fold_product(row_block, square.astype(jnp.bfloat16))
    return 4.0 * identity - 6.0 * scaled + 4.0 * square - cube


def tiled_body(activations, out_grads):
    tok_count = lax.axis_size("tok")
    blk_count = lax.axis_size("blk")
    tok_id = lax.axis_index("tok")
    blk_id = lax.axis_index("blk")
    token_count = activations.shape[0] * tok_count
    tile_cols = activations.shape[1]
    tile_rows = tile_cols * blk_count // tok_count
    row_ids = tok_id * tile_rows + jnp.arange(tile_rows, dtype=jnp.int32)
    col_ids = blk_id * tile_cols + jnp.arange(tile_cols, dtype=jnp.int32)
    identity = (row_ids[:, None] == col_ids[None, :]).astype(jnp.float32)

    def inverse_tile(local):
        full = lax.all_gather(local, "blk", axis=1, tiled=True)
        sums = lax.psum(column_squares(full).astype(jnp.bfloat16), "tok").astype(jnp.float32)
        gram_tile = lax.psum_scatter(
            lax.dot_general(
                full, local, (((0,), (0,)), ((), ())), preferred_element_type=jnp.float32
            ).astype(jnp.bfloat16),
            "tok",
            scatter_dimension=0,
            tiled=True,
        ).astype(jnp.float32)
        inverse = lax.rsqrt(sums / token_count + epsilon)
        inverse_rows = lax.dynamic_slice_in_dim(inverse, tok_id * tile_rows, tile_rows)
        inverse_cols = lax.dynamic_slice_in_dim(inverse, blk_id * tile_cols, tile_cols)
        damped = (
            gram_tile / token_count * inverse_rows[:, None] * inverse_cols[None, :]
            + damping * identity
        )
        result_tile = newton_steps(damped / divisor, identity)
        return lax.all_to_all(
            result_tile.astype(jnp.bfloat16), "blk", split_axis=0, concat_axis=1, tiled=True
        ).astype(result_tile.dtype)

    return inverse_tile(activations), inverse_tile(out_grads)


DIRECT = {
    (0, 1): (0, 0), (0, 3): (0, 1), (1, 3): (0, 2),
    (1, 2): (1, 0), (2, 0): (1, 1), (2, 3): (1, 2),
}
DIAGONAL = [(0, 0), (1, 0), (1, 1), (0, 1)]
CUTS = 4
SHORT = 3
COUNT = 2 * SHORT + 3 * CUTS
ADD_LAG = 3
END_LAG = 6
STEPS = 2


def pick(index, values):
    out = values[-1]
    for i in range(len(values) - 2, -1, -1):
        out = jnp.where(index == i, values[i], out)
    return out


def remote(src, dst, send, recv, device):
    return pltpu.make_async_remote_copy(
        src_ref=src, dst_ref=dst, send_sem=send, recv_sem=recv,
        device_id=device, device_id_type=MESH,
    )


def meet(peers):
    barrier = pltpu.get_barrier_semaphore()
    for peer in peers:
        pl.semaphore_signal(barrier, inc=1, device_id=peer, device_id_type=MESH)
    pl.semaphore_wait(barrier, len(peers))


def factor_kernel(
    tok, blk, tokens, acts, grads, act_out, grad_out,
    x, other, passed, turned, part, first_in, second_out, second_in, keep,
    g, diag, mixed, square, left, cubing, inverse, sent, kept, came, wider_in,
    load_sem, near_send, near_recv, pass_send, pass_recv, core_send, core_recv,
    one_send, one_recv, two_send, two_recv,
    hop_send, hop_recv, hand_send, hand_recv, out_sem, in_sem, kept_sem, came_sem,
):
    t = lax.axis_index("tok")
    b = lax.axis_index("blk")
    low = b < blk // 2
    place = jnp.where(low, b, blk - 1 - b)
    outer = place == 0
    inner = place == 1
    core, col, row = t % 2, t // 2 % 2, t // 4
    mate = (jnp.bitwise_xor(t, 1), b)
    beside = (jnp.bitwise_xor(t, 2), b)
    below = (jnp.bitwise_xor(t, 4), b)
    near = (t, jnp.bitwise_xor(b, 1))
    facing = (t, blk - 1 - b)
    across = (t, jnp.bitwise_xor(b, blk // 2))
    depth, feats = other.shape
    wide = feats // CUTS
    halfway = feats // 2
    count = COUNT
    first = SHORT
    split = SHORT + CUTS
    tail = split + 2 * CUTS

    def load(ref, dst, index):
        return pltpu.make_async_copy(ref, dst, load_sem.at[index])

    @pl.when(low)
    def _():
        load(acts, x.at[place, core], 0).start()
        load(grads, other, 1).start()

    @pl.when(jnp.logical_not(low))
    def _():
        load(grads, x.at[place, core], 0).start()
        load(acts, other, 1).start()

    meet([mate, beside, below, near, facing, across])
    load(acts, x.at[place, core], 0).wait()
    load(grads, other, 1).wait()

    def columns(h):
        return pl.ds(pl.multiple_of(h * wide, LANES), wide)

    def to_mate(label, h):
        here = x.at[label, core, :, columns(h)]
        return remote(
            here, here, core_send.at[label, h], core_recv.at[label, h], mate
        )

    def from_mate(label, h):
        there = x.at[label, 1 - core, :, columns(h)]
        return remote(
            there, there, core_send.at[label, h], core_recv.at[label, h], mate
        )

    def along(label, h, src, device):
        return remote(
            src, x.at[label, core, :, columns(h)],
            near_send.at[label, h], near_recv.at[label, h], device,
        )

    def arrived(label, h):
        here = x.at[label, core, :, columns(h)]
        return remote(here, here, near_send.at[label, h], near_recv.at[label, h], near)

    def give(h):
        return remote(
            other.at[:, columns(h)], passed.at[:, columns(h)],
            pass_send.at[h], pass_recv.at[h], near,
        )

    def onward(h):
        return remote(
            passed.at[:, columns(h)], x.at[3, core, :, columns(h)],
            pass_send.at[h], near_recv.at[3, h], facing,
        )

    for h in range(CUTS):
        to_mate(place, h).start()

    @pl.when(outer)
    def _():
        for h in range(CUTS):
            give(h).start()
        for h in range(CUTS):
            along(0, h, x.at[0, core, :, columns(h)], near).start()

    @pl.when(inner)
    def _():
        for h in range(CUTS):
            along(1, h, x.at[1, core, :, columns(h)], near).start()
            along(2, h, other.at[:, columns(h)], facing).start()

    def turn(slot, label, side):
        at = pl.ds(pl.multiple_of(side * halfway, LANES), halfway)
        for c in range(2):
            for r in range(0, depth, 256):
                turned[slot, :, c * depth + r : c * depth + r + 256] = x[
                    label, c, r : r + 256, at
                ].T

    def share(label, h):
        arrived(label, h).wait_recv()
        to_mate(label, h).start()

    def piece(n):
        task = jnp.where(
            n < first, 0,
            jnp.where(n < split, 1, jnp.where(n < tail, 2 + (n - split) % 2, 4)),
        )
        h = jnp.where(
            n < first, n,
            jnp.where(
                n < split, n - first, jnp.where(n < tail, (n - split) // 2, n - tail)
            ),
        )
        whole = (task > 0) & (task < 4)
        slot = jnp.where(outer, pick(task, [0, 0, 0, 1, 2]), pick(task, [0, 0, 1, 1, 1]))
        label = jnp.where(outer, pick(task, [0, 1, 3, 3, 3]), pick(task, [1, 2, 0, 3, 2]))
        corner = jnp.logical_not(whole) & (h == 2)
        slot = jnp.where(corner, 3, slot)
        inside = core * (CUTS // 2) + h
        at = jnp.where(whole, h, jnp.where(h == 2, CUTS // 2 + core, inside))
        return task, h, slot, label, at, whole

    def one(n, side):
        if side == 0:
            src, device = part.at[n, :, 1 - col, :, pl.ds(0, wide // 2)], beside
        else:
            src, device = part.at[n, 1 - row, :, :, pl.ds(wide // 2, wide // 2)], below
        return remote(
            src, first_in.at[n, side], one_send.at[n, side], one_recv.at[n, side], device
        )

    def two(n, side):
        return remote(
            second_out.at[n, side], second_in.at[n, side],
            two_send.at[n, side], two_recv.at[n, side], below if side == 0 else beside,
        )

    owners = g.shape[0]
    eighth = owners // 2
    early, late = [[0, 1, 2], [1, 0, 2]], [[2, 0, 1], [2, 1, 0]]
    orders = [early, early, late, late]
    groups = len(orders)
    moves = [(2, 0), (4, 0), (0, 1)]
    stages = len(moves)
    ranges = []
    for ref, at_row, size in (
        (diag, 0, LANES), (g, 0, LANES), (g, LANES, 2 * LANES), (diag, LANES, LANES)
    ):
        ranges.append([(ref, at_row + o, n) for o, n in cut(size, 16, 2)])

    def owner(device):
        tt, bb = device
        side = jnp.where(low, bb, blk - 1 - bb)
        return side * eighth + tt % 2 * (eighth // 2) + tt // 2

    me = owner((t, b))

    def flip(q, j, steps, tok_bits=0):
        blk_bits = 0
        for s in range(stages):
            if steps >> s & 1:
                dt, db = moves[orders[q][j][s]]
                tok_bits ^= dt
                blk_bits ^= db
        return jnp.bitwise_xor(t, tok_bits), jnp.bitwise_xor(b, blk_bits)

    def spot(q, j, device):
        ref, o, n = ranges[q][j]
        return ref.at[owner(device), pl.ds(o, n)]

    def index_of(q, j, steps):
        return (q * 2 + j) * 2**stages + steps

    def hop(q, j, steps, s):
        index = index_of(q, j, steps | 1 << s)
        where = spot(q, j, flip(q, j, steps))
        return remote(
            where, where, hop_send.at[index], hop_recv.at[index], flip(q, j, 1 << s)
        )

    def arrival(q, j, steps):
        index = index_of(q, j, steps)
        where = spot(q, j, flip(q, j, steps))
        return remote(where, where, hop_send.at[index], hop_recv.at[index], flip(q, j, 1))

    def hand(q, j, steps, sender):
        index = index_of(q, j, steps)
        where = spot(q, j, flip(q, j, steps, 0 if sender else 1))
        return remote(where, where, hand_send.at[index], hand_recv.at[index], mate)

    def every(q, steps, s):
        for j in range(2):
            hop(q, j, steps, s).start()

    def landed(q, steps, onward_to=()):
        for j in range(2):
            arrival(q, j, steps).wait_recv()
            for s in onward_to:
                hop(q, j, steps, s).start()
            hand(q, j, steps, True).start()

    def begin(q):
        for s in range(stages):
            every(q, 0, s)
        for j in range(2):
            hand(q, j, 0, True).start()

    def forward(h):
        arrived(3, h).wait_recv()
        to_mate(3, h).start()

        @pl.when(inner)
        def _():
            along(3, h, x.at[3, core, :, columns(h)], near).start()

    for h in range(CUTS):
        from_mate(place, h).wait_recv()
    turn(0, place, core)
    turn(3, place, 0)
    gap = END_LAG

    def at_step(i):
        n = jnp.where(i < first, i, jnp.where(i < split + gap, i - gap, i - 2 * gap))
        low_part = (i >= 0) & (i < first)
        mid_part = (i >= first + gap) & (i < split + gap)
        return low_part | mid_part | ((i >= split + 2 * gap) & (i < count + 2 * gap)), n

    @pl.loop(0, count + 2 * gap + END_LAG)
    def _(i):
        active, n = at_step(i)

        @pl.when(i == first + gap)
        def _():
            for s in (0, 1):
                every(0, 0, s)
            for j in range(2):
                hand(0, j, 0, True).start()

        @pl.when(active & (n >= first) & (n < split))
        def _():
            h = n - first

            @pl.when(inner)
            def _():
                give(h).wait_recv()
                onward(h).start()

            share(place + 1, h)
            from_mate(place + 1, h).wait_recv()

        @pl.when(i == split + gap)
        def _():
            landed(0, 1, (1, 2))
            every(0, 0, 2)
            turn(1, place + 1, core)

        @pl.when(inner & (i == split + gap + gap // 2))
        def _():
            forward(0)

        @pl.when(i == split + 2 * gap)
        def _():
            landed(0, 2)
            landed(0, 3)
            for s in (0, 1):
                every(1, 0, s)
            for j in range(2):
                hand(1, j, 0, True).start()

        @pl.when(i == split + 2 * gap + CUTS)
        def _():
            landed(1, 1, (1,))

        @pl.when(i == tail + 2 * gap)
        def _():
            every(0, 2, 2)
            every(0, 3, 2)

        @pl.when(i == tail + 2 * gap + SHORT)
        def _():
            landed(1, 2)
            landed(1, 3)

        @pl.when(i == tail + 2 * gap + END_LAG)
        def _():
            begin(2)

        @pl.when(active & (n >= split) & (n < tail) & ((n - split) % 2 == 0))
        def _():
            h = (n - split) // 2

            @pl.when(outer | (h > 0))
            def _():
                forward(h)

            @pl.when(inner)
            def _():
                share(0, h)
                from_mate(0, h).wait_recv()

            from_mate(3, h).wait_recv()

        @pl.when(i == tail + 2 * gap)
        def _():
            turn(3, jnp.where(outer, 3, 2), 0)

            @pl.when(outer)
            def _():
                turn(2, 3, core)

        @pl.when(active)
        def _():
            task, h, slot, label, cut_at, _ = piece(n)
            at = pl.ds(pl.multiple_of(cut_at * wide, LANES), wide)
            right = x[label, :, :, at].reshape(2 * depth, wide)
            product = jnp.dot(turned[slot], right, preferred_element_type=jnp.float32)
            part[n] = product.astype(jnp.bfloat16).reshape(2, 2, LANES, wide)
            one(n, 0).start()
            one(n, 1).start()

        adding, m = at_step(i - ADD_LAG)

        @pl.when(adding)
        def _():
            lo, hi = pl.ds(0, wide // 2), pl.ds(wide // 2, wide // 2)
            one(m, 0).wait_recv()
            one(m, 1).wait_recv()
            wider = jnp.float32
            second_out[m, 0] = (
                part[m, 1 - row, col, :, lo].astype(wider)
                + first_in[m, 0, 1 - row].astype(wider)
            ).astype(jnp.bfloat16)
            second_out[m, 1] = (
                part[m, row, 1 - col, :, hi].astype(wider)
                + first_in[m, 1, 1 - col].astype(wider)
            ).astype(jnp.bfloat16)
            two(m, 0).start()
            two(m, 1).start()
            keep[m, 0] = part[m, row, col, :, lo].astype(wider) + first_in[
                m, 0, row
            ].astype(wider)
            keep[m, 1] = part[m, row, col, :, hi].astype(wider) + first_in[
                m, 1, col
            ].astype(wider)

        ending, e = at_step(i - END_LAG)

        @pl.when(ending)
        def _():
            task, h, _, _, _, whole = piece(e)
            two(e, 0).wait_recv()
            two(e, 1).wait_recv()
            for side in range(2):
                at = pl.ds(pl.multiple_of(h * wide + side * (wide // 2), LANES), wide // 2)
                total = keep[e, side] + second_in[e, side].astype(jnp.float32)
                total = total.astype(jnp.bfloat16)

                @pl.when(whole)
                def _():
                    g[me, pl.ds(pl.multiple_of((task - 1) * LANES, LANES), LANES), at] = total

                @pl.when(jnp.logical_not(whole))
                def _():
                    g_row = pl.multiple_of(task // 4 * LANES, LANES)
                    diag[me, pl.ds(g_row, LANES), at] = total

    def received(q):
        for j in range(2):
            for steps in range(2**stages):
                hand(q, j, steps, False).wait_recv()

    half = blk // 2
    width = square.shape[1]
    labels = width // feats
    rows = LANES
    factor = 1.0 / (tokens * divisor)
    shift = damping / divisor
    eye = lax.broadcasted_iota(jnp.int32, (LANES, LANES), 0) == lax.broadcasted_iota(
        jnp.int32, (LANES, LANES), 1
    )
    quarter = eighth // 2
    step = feats // STEPS

    def diagonal(plane, k, sub, axis):
        at = pl.ds(pl.multiple_of(sub % quarter * LANES, LANES), LANES)
        own_rows = pl.ds(pl.multiple_of(k * LANES, LANES), LANES)
        block = jnp.where(eye, diag[plane * eighth + sub, own_rows, at].astype(jnp.float32), 0.0)
        total = jnp.sum(block, axis=axis, keepdims=True)
        return lax.rsqrt(total / tokens + epsilon)

    def rebuild(which):
        for label in range(labels):
            plane, k = DIAGONAL[label]
            if k != which:
                continue

            @pl.loop(0, eighth)
            def _(sub):
                at = pl.ds(pl.multiple_of(label * feats + sub * LANES, LANES), LANES)
                inverse[:, at] = diagonal(plane, k, sub, 0)

            own_rows = slice(k * LANES, (k + 1) * LANES)
            ends = [
                slice(plane * eighth + c * quarter, plane * eighth + (c + 1) * quarter)
                for c in range(2)
            ]
            for c in range(2):
                block = diag[ends[c], own_rows, :halfway].reshape(halfway, halfway)
                x[label, c, :, c * halfway : (c + 1) * halfway] = block
                lo = halfway + c * wide
                block = diag[ends[c], own_rows, halfway : halfway + wide].reshape(halfway, wide)
                x[label, 0, :, lo : lo + wide] = block
                x[label, 1, c * wide : (c + 1) * wide, :halfway] = block.T

    begin(3)
    for steps in range(4):
        every(1, steps, 2)
    for h in range(CUTS):
        to_mate(place, h).wait_send()
        to_mate(place + 1, h).wait_send()
        to_mate(3, h).wait_send()

    @pl.when(outer)
    def _():
        for h in range(CUTS):
            give(h).wait_send()
            along(0, h, x.at[0, core, :, columns(h)], near).wait_send()

    @pl.when(inner)
    def _():
        for h in range(CUTS):
            along(1, h, x.at[1, core, :, columns(h)], near).wait_send()
            along(2, h, other.at[:, columns(h)], facing).wait_send()
            along(3, h, x.at[3, core, :, columns(h)], near).wait_send()
            onward(h).wait_send()
            to_mate(0, h).wait_send()

    landed(2, 1, (1, 2))
    landed(2, 2, (2,))
    for steps in range(4, 8):
        landed(0, steps)
    received(0)
    rebuild(0)
    landed(2, 3, (2,))
    landed(3, 1, (1, 2))
    landed(3, 2, (2,))
    landed(3, 3, (2,))
    for q in range(1, groups):
        for steps in range(4, 8):
            landed(q, steps)
    for q in range(1, groups):
        received(q)
    rebuild(1)

    block_of_rows = t // 2
    row_label = jnp.where(low, block_of_rows, labels - 1 - block_of_rows)
    subs = [t % 2 * blk + bb for bb in (b, jnp.bitwise_xor(b, half))]
    diag_plane = pick(row_label, [d[0] for d in DIAGONAL])
    diag_task = pick(row_label, [d[1] for d in DIAGONAL])
    inverse_rows = jnp.concatenate(
        [diagonal(diag_plane, diag_task, sub, 1) for sub in subs], axis=0
    )

    for label in range(labels):

        @pl.when(row_label == label)
        def _():
            for j in range(labels):
                cols = slice(j * feats, (j + 1) * feats)
                for s, sub in enumerate(subs):
                    if label == j:
                        at = pl.ds(pl.multiple_of(sub % quarter * LANES, LANES), LANES)
                        value = x[label, core, at, :]
                    elif (label, j) in DIRECT:
                        plane, k = DIRECT[label, j]
                        value = g[plane * eighth + sub, k * LANES : (k + 1) * LANES, :]
                    else:
                        plane, k = DIRECT[j, label]
                        at = pl.ds(pl.multiple_of(sub * LANES, LANES), LANES)
                        value = g[
                            plane * eighth : (plane + 1) * eighth, k * LANES : (k + 1) * LANES, at
                        ]
                        value = value.reshape(feats, LANES).T
                    mixed[s * rows : (s + 1) * rows, cols] = value

    starts = [row_label * feats + sub * LANES for sub in subs]
    row_scale = factor * inverse_rows

    def identity(first_col, size):
        at = first_col + lax.broadcasted_iota(jnp.int32, (rows, size), 1)
        row = lax.broadcasted_iota(jnp.int32, (rows, size), 0)
        return jnp.concatenate(
            [(at - start == row).astype(jnp.float32) for start in starts], axis=0
        )

    def scaled(at):
        return mixed[:, at].astype(jnp.float32) * row_scale * inverse[:, at]

    def fold(lefts, label, h):
        total = None
        for k in range(labels):
            lhs = lefts[:, k * feats : (k + 1) * feats]
            if k == label:
                at = pl.ds(pl.multiple_of(h * step, LANES), step)
                rhs = x[label, :, :, at].reshape(feats, step)
                product = jnp.dot(lhs, rhs, preferred_element_type=jnp.float32)
            elif (k, label) in DIRECT:
                plane, task = DIRECT[k, label]
                rhs = g[
                    plane * eighth : (plane + 1) * eighth,
                    task * LANES : (task + 1) * LANES,
                    pl.ds(pl.multiple_of(h * step, LANES), step),
                ].reshape(feats, step)
                product = jnp.dot(lhs, rhs, preferred_element_type=jnp.float32)
            else:
                plane, task = DIRECT[label, k]
                few = step // LANES
                rhs = g[
                    pl.ds(plane * eighth + h * few, few), task * LANES : (task + 1) * LANES, :
                ].reshape(step, feats)
                product = lax.dot_general(
                    lhs, rhs, (((1,), (1,)), ((), ())), preferred_element_type=jnp.float32
                )
            total = product if total is None else total + product
        return total

    @pl.loop(0, labels * STEPS)
    def _(i):
        at = pl.ds(pl.multiple_of(i * step, step), step)
        left[:, at] = (scaled(at) * inverse[:, at]).astype(jnp.bfloat16)

    for label in range(labels):

        @pl.loop(0, STEPS)
        def _(h):
            at = pl.ds(pl.multiple_of(label * feats + h * step, step), step)
            squared = fold(left, label, h) * (inverse[:, at] * factor)
            square[:, at] = squared
            cubing[:, at] = (squared * inverse[:, at]).astype(jnp.bfloat16)

    def target(label, h):
        to = jnp.where(low, label, labels - 1 - label)
        return pl.ds(pl.multiple_of(to * feats + h * step, LANES), step), to * STEPS + h

    def swap(label, h):
        at, index = target(label, h)
        return remote(
            sent.at[:, at], came.at[:, at], out_sem.at[index], in_sem.at[index], across
        )

    def store(src, sems, label, h, out):
        at, index = target(label, h)
        return pltpu.make_async_copy(src.at[:, at], out.at[:, at], sems.at[index])

    one_part = 4.0 - 6.0 * shift + 4.0 * shift**2 - shift**3
    linear_part = -6.0 + 8.0 * shift - 3.0 * shift**2
    square_part = 4.0 - 3.0 * shift

    for label in range(labels):

        @pl.loop(0, STEPS)
        def _(h):
            start_col = pl.multiple_of(label * feats + h * step, step)
            at = pl.ds(start_col, step)
            cube = fold(cubing, label, h) * (inverse[:, at] * factor)
            result = (
                one_part * identity(start_col, step) + linear_part * scaled(at)
                + square_part * square[:, at] - cube
            )
            to, _ = target(label, h)
            sent[:, to] = result[rows:].astype(jnp.bfloat16)
            swap(label, h).start()
            kept[:, to] = result[:rows]

            @pl.when(low)
            def _():
                store(kept, kept_sem, label, h, act_out).start()

            @pl.when(jnp.logical_not(low))
            def _():
                store(kept, kept_sem, label, h, grad_out).start()

    @pl.loop(0, count)
    def _(n):
        for side in range(2):
            one(n, side).wait_send()
            two(n, side).wait_send()

    for q in range(groups):
        for j in range(2):
            for steps in range(2**stages):
                hand(q, j, steps, True).wait_send()
                if steps:
                    arrival(q, j, steps).wait_send()

    for label in reversed(range(labels)):

        @pl.loop(0, STEPS)
        def _(h):
            to, _ = target(label, h)
            swap(label, h).wait_recv()
            wider_in[:, to] = came[:, to].astype(jnp.float32)

            @pl.when(low)
            def _():
                store(wider_in, came_sem, label, h, grad_out).start()

            @pl.when(jnp.logical_not(low))
            def _():
                store(wider_in, came_sem, label, h, act_out).start()

            swap(label, h).wait_send()
            store(kept, kept_sem, label, h, act_out).wait()

    for label in range(labels):
        for h in range(STEPS):
            store(wider_in, came_sem, label, h, grad_out).wait()


def cut(length, unit, pieces):
    units = length // unit
    sizes = [(units // pieces + (1 if i < units % pieces else 0)) * unit for i in range(pieces)]
    return [(sum(sizes[:i]), sizes[i]) for i in range(pieces)]


def call(kernel, outs, scratch, *operands):
    return pl.pallas_call(
        kernel,
        out_shape=outs,
        in_specs=[pl.BlockSpec(memory_space=pl.ANY)] * len(operands),
        out_specs=[pl.BlockSpec(memory_space=pl.ANY)] * len(outs),
        scratch_shapes=scratch,
        compiler_params=pltpu.CompilerParams(
            collective_id=0, has_side_effects=True, vmem_limit_bytes=63 * 1024 * 1024
        ),
    )(*operands)


def split_body(tok, blk, activations, out_grads):
    depth, feats = activations.shape
    tokens = depth * tok
    width = feats * blk
    rows = width // (tok * blk)
    count = COUNT
    wide = feats // CUTS
    bf16, f32 = jnp.bfloat16, jnp.float32
    dma = pltpu.SemaphoreType.DMA
    steps = blk * STEPS
    slots = 4 * 2 * 8
    return call(
        functools.partial(factor_kernel, tok, blk, tokens),
        [jax.ShapeDtypeStruct((rows, width), f32)] * 2,
        [
            pltpu.VMEM((blk, 2, depth, feats), bf16),
            pltpu.VMEM((depth, feats), bf16),
            pltpu.VMEM((depth, feats), bf16),
            pltpu.VMEM((4, feats // 2, 2 * depth), bf16),
            pltpu.VMEM((count, 2, 2, rows, wide), bf16),
            pltpu.VMEM((count, 2, 2, rows, wide // 2), bf16),
            pltpu.VMEM((count, 2, rows, wide // 2), bf16),
            pltpu.VMEM((count, 2, rows, wide // 2), bf16),
            pltpu.VMEM((count, 2, rows, wide // 2), f32),
            pltpu.VMEM((2 * tok, 3 * rows, feats), bf16),
            pltpu.VMEM((2 * tok, 2 * rows, feats // CUTS * SHORT), bf16),
            pltpu.VMEM((2 * rows, width), bf16),
            pltpu.VMEM((2 * rows, width), f32),
            pltpu.VMEM((2 * rows, width), bf16),
            pltpu.VMEM((2 * rows, width), bf16),
            pltpu.VMEM((1, width), f32),
            pltpu.VMEM((rows, width), bf16),
            pltpu.VMEM((rows, width), f32),
            pltpu.VMEM((rows, width), bf16),
            pltpu.VMEM((rows, width), f32),
            dma((2,)),
            dma((blk, CUTS)), dma((blk, CUTS)),
            dma((CUTS,)), dma((CUTS,)),
            dma((blk, CUTS)), dma((blk, CUTS)),
            dma((count, 2)), dma((count, 2)), dma((count, 2)), dma((count, 2)),
            dma((slots,)), dma((slots,)), dma((slots,)), dma((slots,)),
            dma((steps,)), dma((steps,)), dma((steps,)), dma((steps,)),
        ],
        activations, out_grads,
    )


def solution(mesh):
    tok, blk = mesh.shape["tok"], mesh.shape["blk"]
    placed = (P("tok", "blk"), P("tok", "blk"))

    def body(activations, out_grads):
        depth, feats = activations.shape
        whole = max(depth * tok, feats * blk) * feats * blk * activations.dtype.itemsize
        cube = tok == 2 * blk and blk == 4 and feats == tok * LANES == 2 * depth
        if whole <= gathered_budget and cube:
            return split_body(tok, blk, activations, out_grads)
        return tiled_body(activations, out_grads)

    return jax.shard_map(
        body,
        mesh=mesh,
        in_specs=placed,
        out_specs=(P(("tok", "blk"), None), P(("tok", "blk"), None)),
        check_vma=False,
    )
```

```python
import functools

import jax
import jax.numpy as jnp
import numpy as np
from jax import lax
from jax.experimental import pallas as pl
from jax.experimental.pallas import tpu as pltpu
from jax.sharding import PartitionSpec as P

damping = 0.3
epsilon = 1e-06
divisor = 2.0
gathered_budget = 32 * 1024 * 1024
LANES = 128
MESH = pl.DeviceIdType.MESH


def column_squares(data):
    values = data.astype(jnp.float32)
    return jnp.sum(values * values, axis=0)


def fold_product(row_block, tile):
    return jnp.dot(
        row_block,
        lax.all_gather(tile, "tok", axis=0, tiled=True),
        preferred_element_type=jnp.float32,
    )


def newton_steps(scaled, identity):
    half = scaled.astype(jnp.bfloat16)
    row_block = lax.all_gather(half, "blk", axis=1, tiled=True)
    square = fold_product(row_block, half)
    cube = fold_product(row_block, square.astype(jnp.bfloat16))
    return 4.0 * identity - 6.0 * scaled + 4.0 * square - cube


def tiled_body(activations, out_grads):
    tok_count = lax.axis_size("tok")
    blk_count = lax.axis_size("blk")
    tok_id = lax.axis_index("tok")
    blk_id = lax.axis_index("blk")
    token_count = activations.shape[0] * tok_count
    tile_cols = activations.shape[1]
    tile_rows = tile_cols * blk_count // tok_count
    row_ids = tok_id * tile_rows + jnp.arange(tile_rows, dtype=jnp.int32)
    col_ids = blk_id * tile_cols + jnp.arange(tile_cols, dtype=jnp.int32)
    identity = (row_ids[:, None] == col_ids[None, :]).astype(jnp.float32)

    def inverse_tile(local):
        full = lax.all_gather(local, "blk", axis=1, tiled=True)
        sums = lax.psum(column_squares(full).astype(jnp.bfloat16), "tok").astype(jnp.float32)
        gram_tile = lax.psum_scatter(
            lax.dot_general(
                full, local, (((0,), (0,)), ((), ())), preferred_element_type=jnp.float32
            ).astype(jnp.bfloat16),
            "tok",
            scatter_dimension=0,
            tiled=True,
        ).astype(jnp.float32)
        inverse = lax.rsqrt(sums / token_count + epsilon)
        inverse_rows = lax.dynamic_slice_in_dim(inverse, tok_id * tile_rows, tile_rows)
        inverse_cols = lax.dynamic_slice_in_dim(inverse, blk_id * tile_cols, tile_cols)
        damped = (
            gram_tile / token_count * inverse_rows[:, None] * inverse_cols[None, :]
            + damping * identity
        )
        result_tile = newton_steps(damped / divisor, identity)
        return lax.all_to_all(
            result_tile.astype(jnp.bfloat16), "blk", split_axis=0, concat_axis=1, tiled=True
        ).astype(result_tile.dtype)

    return inverse_tile(activations), inverse_tile(out_grads)


DIRECT = {
    (0, 1): (0, 0), (0, 3): (0, 1), (1, 3): (0, 2),
    (1, 2): (1, 0), (2, 0): (1, 1), (2, 3): (1, 2),
}
DIAGONAL = [(0, 0), (1, 0), (1, 1), (0, 1)]
CUTS = 4
SHORT = 3
COUNT = 2 * SHORT + 3 * CUTS
ADD_LAG = 3
END_LAG = 6
STEPS = 2


def pick(index, values):
    out = values[-1]
    for i in range(len(values) - 2, -1, -1):
        out = jnp.where(index == i, values[i], out)
    return out


def remote(src, dst, send, recv, device):
    return pltpu.make_async_remote_copy(
        src_ref=src, dst_ref=dst, send_sem=send, recv_sem=recv,
        device_id=device, device_id_type=MESH,
    )


def meet(peers):
    barrier = pltpu.get_barrier_semaphore()
    for peer in peers:
        pl.semaphore_signal(barrier, inc=1, device_id=peer, device_id_type=MESH)
    pl.semaphore_wait(barrier, len(peers))


def factor_kernel(
    tok, blk, tokens, acts, grads, act_out, grad_out,
    x, other, passed, turned, part, first_in, second_out, second_in, keep,
    g, diag, mixed, square, left, cubing, inverse, sent, kept, came, wider_in,
    load_sem, near_send, near_recv, pass_send, pass_recv, core_send, core_recv,
    one_send, one_recv, two_send, two_recv,
    hop_send, hop_recv, hand_send, hand_recv, out_sem, in_sem, kept_sem, came_sem,
):
    t = lax.axis_index("tok")
    b = lax.axis_index("blk")
    low = b < blk // 2
    place = jnp.where(low, b, blk - 1 - b)
    outer = place == 0
    inner = place == 1
    core, col, row = t % 2, t // 2 % 2, t // 4
    mate = (jnp.bitwise_xor(t, 1), b)
    beside = (jnp.bitwise_xor(t, 2), b)
    below = (jnp.bitwise_xor(t, 4), b)
    near = (t, jnp.bitwise_xor(b, 1))
    facing = (t, blk - 1 - b)
    across = (t, jnp.bitwise_xor(b, blk // 2))
    depth, feats = other.shape
    wide = feats // CUTS
    halfway = feats // 2
    count = COUNT
    first = SHORT
    split = SHORT + CUTS
    tail = split + 2 * CUTS

    def load(ref, dst, index):
        return pltpu.make_async_copy(ref, dst, load_sem.at[index])

    @pl.when(low)
    def _():
        load(acts, x.at[place, core], 0).start()
        load(grads, other, 1).start()

    @pl.when(jnp.logical_not(low))
    def _():
        load(grads, x.at[place, core], 0).start()
        load(acts, other, 1).start()

    meet([mate, beside, below, near, facing, across])
    load(acts, x.at[place, core], 0).wait()
    load(grads, other, 1).wait()

    def columns(h):
        return pl.ds(pl.multiple_of(h * wide, LANES), wide)

    def to_mate(label, h):
        here = x.at[label, core, :, columns(h)]
        return remote(
            here, here, core_send, core_recv.at[label, h], mate
        )

    def from_mate(label, h):
        there = x.at[label, 1 - core, :, columns(h)]
        return remote(
            there, there, core_send, core_recv.at[label, h], mate
        )

    def along(label, h, src, device):
        return remote(
            src, x.at[label, core, :, columns(h)],
            near_send, near_recv.at[label, h], device,
        )

    def arrived(label, h):
        here = x.at[label, core, :, columns(h)]
        return remote(here, here, near_send, near_recv.at[label, h], near)

    def give(h):
        return remote(
            other.at[:, columns(h)], passed.at[:, columns(h)],
            pass_send, pass_recv.at[h], near,
        )

    def onward(h):
        return remote(
            passed.at[:, columns(h)], x.at[3, core, :, columns(h)],
            pass_send, near_recv.at[3, h], facing,
        )

    for h in range(CUTS):
        to_mate(place, h).start()

    @pl.when(outer)
    def _():
        for h in range(CUTS):
            give(h).start()
        for h in range(CUTS):
            along(0, h, x.at[0, core, :, columns(h)], near).start()

    @pl.when(inner)
    def _():
        for h in range(CUTS):
            along(1, h, x.at[1, core, :, columns(h)], near).start()
            along(2, h, other.at[:, columns(h)], facing).start()

    def turn(slot, label, side):
        at = pl.ds(pl.multiple_of(side * halfway, LANES), halfway)
        for c in range(2):
            for r in range(0, depth, 256):
                turned[slot, :, c * depth + r : c * depth + r + 256] = x[
                    label, c, r : r + 256, at
                ].T

    def share(label, h):
        arrived(label, h).wait_recv()
        to_mate(label, h).start()

    def piece(n):
        task = jnp.where(
            n < first, 0,
            jnp.where(n < split, 1, jnp.where(n < tail, 2 + (n - split) % 2, 4)),
        )
        h = jnp.where(
            n < first, n,
            jnp.where(
                n < split, n - first, jnp.where(n < tail, (n - split) // 2, n - tail)
            ),
        )
        whole = (task > 0) & (task < 4)
        slot = jnp.where(outer, pick(task, [0, 0, 0, 1, 2]), pick(task, [0, 0, 1, 1, 1]))
        label = jnp.where(outer, pick(task, [0, 1, 3, 3, 3]), pick(task, [1, 2, 0, 3, 2]))
        corner = jnp.logical_not(whole) & (h == 2)
        slot = jnp.where(corner, 3, slot)
        inside = core * (CUTS // 2) + h
        at = jnp.where(whole, h, jnp.where(h == 2, CUTS // 2 + core, inside))
        return task, h, slot, label, at, whole

    def both(ref, sem):
        remote(ref, ref, sem, sem, mate).wait_recv()

    def sent_all(ref, sem):
        remote(ref, ref, sem, sem, mate).wait_send()

    def one(n, side):
        if side == 0:
            src, device = part.at[n, :, 1 - col, :, pl.ds(0, wide // 2)], beside
        else:
            src, device = part.at[n, 1 - row, :, :, pl.ds(wide // 2, wide // 2)], below
        return remote(
            src, first_in.at[n, side], one_send, one_recv.at[n], device
        )

    def two(n, side):
        return remote(
            second_out.at[n, side], second_in.at[n, side],
            two_send, two_recv.at[n], below if side == 0 else beside,
        )

    owners = g.shape[0]
    eighth = owners // 2
    early, late = [[0, 1, 2], [1, 0, 2]], [[2, 0, 1], [2, 1, 0]]
    orders = [early, early, late, late]
    groups = len(orders)
    moves = [(2, 0), (4, 0), (0, 1)]
    stages = len(moves)
    ranges = []
    for ref, at_row, size in (
        (diag, 0, LANES), (g, 0, LANES), (g, LANES, 2 * LANES), (diag, LANES, LANES)
    ):
        ranges.append([(ref, at_row + o, n) for o, n in cut(size, 16, 2)])

    def owner(device):
        tt, bb = device
        side = jnp.where(low, bb, blk - 1 - bb)
        return side * eighth + tt % 2 * (eighth // 2) + tt // 2

    me = owner((t, b))

    def flip(q, j, steps, tok_bits=0):
        blk_bits = 0
        for s in range(stages):
            if steps >> s & 1:
                dt, db = moves[orders[q][j][s]]
                tok_bits ^= dt
                blk_bits ^= db
        return jnp.bitwise_xor(t, tok_bits), jnp.bitwise_xor(b, blk_bits)

    def spot(q, j, device):
        ref, o, n = ranges[q][j]
        return ref.at[owner(device), pl.ds(o, n)]

    kinds = [0, 1, 1, 0]

    def whole_rows(q, owner_at):
        ref, o, n = ranges[q][0]
        return ref.at[owner_at, pl.ds(o, n + ranges[q][1][2])]

    def hop(q, j, steps, s):
        where = spot(q, j, flip(q, j, steps))
        return remote(
            where, where, hop_send.at[kinds[q]], hop_recv.at[q, steps | 1 << s],
            flip(q, j, 1 << s),
        )

    def hand(q, j, steps):
        where = spot(q, j, flip(q, j, steps))
        return remote(where, where, hand_send.at[kinds[q]], hand_recv.at[q], mate)

    def every(q, steps, s):
        for j in range(2):
            hop(q, j, steps, s).start()

    def landed(q, steps, onward_to=()):
        both(whole_rows(q, me), hop_recv.at[q, steps])
        for j in range(2):
            for s in onward_to:
                hop(q, j, steps, s).start()
            hand(q, j, steps).start()

    def begin(q):
        for s in range(stages):
            every(q, 0, s)
        for j in range(2):
            hand(q, j, 0).start()

    def forward(h):
        arrived(3, h).wait_recv()
        to_mate(3, h).start()

        @pl.when(inner)
        def _():
            along(3, h, x.at[3, core, :, columns(h)], near).start()

    for h in range(CUTS):
        from_mate(place, h).wait_recv()
    turn(0, place, core)
    turn(3, place, 0)
    gap = END_LAG

    def at_step(i):
        n = jnp.where(i < first, i, jnp.where(i < split + gap, i - gap, i - 2 * gap))
        low_part = (i >= 0) & (i < first)
        mid_part = (i >= first + gap) & (i < split + gap)
        return low_part | mid_part | ((i >= split + 2 * gap) & (i < count + 2 * gap)), n

    @pl.loop(0, count + 2 * gap + END_LAG)
    def _(i):
        active, n = at_step(i)

        @pl.when(i == first + gap)
        def _():
            for s in (0, 1):
                every(0, 0, s)
            for j in range(2):
                hand(0, j, 0).start()

        @pl.when(active & (n >= first) & (n < split))
        def _():
            h = n - first

            @pl.when(inner)
            def _():
                give(h).wait_recv()
                onward(h).start()

            share(place + 1, h)
            from_mate(place + 1, h).wait_recv()

        @pl.when(i == split + gap)
        def _():
            landed(0, 1, (1, 2))
            every(0, 0, 2)
            turn(1, place + 1, core)

        @pl.when(inner & (i == split + gap + gap // 2))
        def _():
            forward(0)

        @pl.when(i == split + 2 * gap)
        def _():
            landed(0, 2)
            landed(0, 3)
            for s in (0, 1):
                every(1, 0, s)
            for j in range(2):
                hand(1, j, 0).start()

        @pl.when(i == split + 2 * gap + CUTS)
        def _():
            landed(1, 1, (1,))

        @pl.when(i == tail + 2 * gap)
        def _():
            every(0, 2, 2)
            every(0, 3, 2)

        @pl.when(i == tail + 2 * gap + SHORT)
        def _():
            landed(1, 2)
            landed(1, 3)

        @pl.when(i == tail + 2 * gap + END_LAG)
        def _():
            begin(2)

        @pl.when(active & (n >= split) & (n < tail) & ((n - split) % 2 == 0))
        def _():
            h = (n - split) // 2

            @pl.when(outer | (h > 0))
            def _():
                forward(h)

            @pl.when(inner)
            def _():
                share(0, h)
                from_mate(0, h).wait_recv()

            from_mate(3, h).wait_recv()

        @pl.when(i == tail + 2 * gap)
        def _():
            turn(3, jnp.where(outer, 3, 2), 0)

            @pl.when(outer)
            def _():
                turn(2, 3, core)

        @pl.when(active)
        def _():
            task, h, slot, label, cut_at, _ = piece(n)
            at = pl.ds(pl.multiple_of(cut_at * wide, LANES), wide)
            right = x[label, :, :, at].reshape(2 * depth, wide)
            product = jnp.dot(turned[slot], right, preferred_element_type=jnp.float32)
            part[n] = product.astype(jnp.bfloat16).reshape(2, 2, LANES, wide)
            one(n, 0).start()
            one(n, 1).start()

        adding, m = at_step(i - ADD_LAG)

        @pl.when(adding)
        def _():
            lo, hi = pl.ds(0, wide // 2), pl.ds(wide // 2, wide // 2)
            both(first_in.at[m], one_recv.at[m])
            wider = jnp.float32
            second_out[m, 0] = (
                part[m, 1 - row, col, :, lo].astype(wider)
                + first_in[m, 0, 1 - row].astype(wider)
            ).astype(jnp.bfloat16)
            second_out[m, 1] = (
                part[m, row, 1 - col, :, hi].astype(wider)
                + first_in[m, 1, 1 - col].astype(wider)
            ).astype(jnp.bfloat16)
            two(m, 0).start()
            two(m, 1).start()
            keep[m, 0] = part[m, row, col, :, lo].astype(wider) + first_in[
                m, 0, row
            ].astype(wider)
            keep[m, 1] = part[m, row, col, :, hi].astype(wider) + first_in[
                m, 1, col
            ].astype(wider)

        ending, e = at_step(i - END_LAG)

        @pl.when(ending)
        def _():
            task, h, _, _, _, whole = piece(e)
            both(second_in.at[e], two_recv.at[e])
            for side in range(2):
                at = pl.ds(pl.multiple_of(h * wide + side * (wide // 2), LANES), wide // 2)
                total = keep[e, side] + second_in[e, side].astype(jnp.float32)
                total = total.astype(jnp.bfloat16)

                @pl.when(whole)
                def _():
                    g[me, pl.ds(pl.multiple_of((task - 1) * LANES, LANES), LANES), at] = total

                @pl.when(jnp.logical_not(whole))
                def _():
                    g_row = pl.multiple_of(task // 4 * LANES, LANES)
                    diag[me, pl.ds(g_row, LANES), at] = total

    def received(q):
        both(whole_rows(q, pl.ds(0, 2**stages)), hand_recv.at[q])

    half = blk // 2
    width = square.shape[1]
    labels = width // feats
    rows = LANES
    factor = 1.0 / (tokens * divisor)
    shift = damping / divisor
    eye = lax.broadcasted_iota(jnp.int32, (LANES, LANES), 0) == lax.broadcasted_iota(
        jnp.int32, (LANES, LANES), 1
    )
    quarter = eighth // 2
    step = feats // STEPS

    def diagonal(plane, k, sub, axis):
        at = pl.ds(pl.multiple_of(sub % quarter * LANES, LANES), LANES)
        own_rows = pl.ds(pl.multiple_of(k * LANES, LANES), LANES)
        block = jnp.where(eye, diag[plane * eighth + sub, own_rows, at].astype(jnp.float32), 0.0)
        total = jnp.sum(block, axis=axis, keepdims=True)
        return lax.rsqrt(total / tokens + epsilon)

    def rebuild(which):
        for label in range(labels):
            plane, k = DIAGONAL[label]
            if k != which:
                continue

            @pl.loop(0, eighth)
            def _(sub):
                at = pl.ds(pl.multiple_of(label * feats + sub * LANES, LANES), LANES)
                inverse[:, at] = diagonal(plane, k, sub, 0)

            own_rows = slice(k * LANES, (k + 1) * LANES)
            ends = [
                slice(plane * eighth + c * quarter, plane * eighth + (c + 1) * quarter)
                for c in range(2)
            ]
            for c in range(2):
                block = diag[ends[c], own_rows, :halfway].reshape(halfway, halfway)
                x[label, c, :, c * halfway : (c + 1) * halfway] = block
                lo = halfway + c * wide
                block = diag[ends[c], own_rows, halfway : halfway + wide].reshape(halfway, wide)
                x[label, 0, :, lo : lo + wide] = block
                x[label, 1, c * wide : (c + 1) * wide, :halfway] = block.T

    begin(3)
    for steps in range(4):
        every(1, steps, 2)
    sent_all(other, pass_send)

    @pl.when(outer)
    def _():
        sent_all(x.at[pl.ds(0, 3), 0], core_send)
        sent_all(x.at[pl.ds(0, 1), 0], near_send)

    @pl.when(inner)
    def _():
        sent_all(x.at[pl.ds(0, 4), 0], core_send)
        sent_all(x.at[pl.ds(0, 3), 0], near_send)

    landed(2, 1, (1, 2))
    landed(2, 2, (2,))
    for steps in range(4, 8):
        landed(0, steps)
    received(0)
    rebuild(0)
    landed(2, 3, (2,))
    landed(3, 1, (1, 2))
    landed(3, 2, (2,))
    landed(3, 3, (2,))
    for q in range(1, groups):
        for steps in range(4, 8):
            landed(q, steps)
    for q in range(1, groups):
        received(q)
    rebuild(1)

    block_of_rows = t // 2
    row_label = jnp.where(low, block_of_rows, labels - 1 - block_of_rows)
    subs = [t % 2 * blk + bb for bb in (b, jnp.bitwise_xor(b, half))]
    diag_plane = pick(row_label, [d[0] for d in DIAGONAL])
    diag_task = pick(row_label, [d[1] for d in DIAGONAL])
    inverse_rows = jnp.concatenate(
        [diagonal(diag_plane, diag_task, sub, 1) for sub in subs], axis=0
    )

    for label in range(labels):

        @pl.when(row_label == label)
        def _():
            for j in range(labels):
                cols = slice(j * feats, (j + 1) * feats)
                for s, sub in enumerate(subs):
                    if label == j:
                        at = pl.ds(pl.multiple_of(sub % quarter * LANES, LANES), LANES)
                        value = x[label, core, at, :]
                    elif (label, j) in DIRECT:
                        plane, k = DIRECT[label, j]
                        value = g[plane * eighth + sub, k * LANES : (k + 1) * LANES, :]
                    else:
                        plane, k = DIRECT[j, label]
                        at = pl.ds(pl.multiple_of(sub * LANES, LANES), LANES)
                        value = g[
                            plane * eighth : (plane + 1) * eighth, k * LANES : (k + 1) * LANES, at
                        ]
                        value = value.reshape(feats, LANES).T
                    mixed[s * rows : (s + 1) * rows, cols] = value

    starts = [row_label * feats + sub * LANES for sub in subs]
    row_scale = factor * inverse_rows

    def identity(first_col, size):
        at = first_col + lax.broadcasted_iota(jnp.int32, (rows, size), 1)
        row = lax.broadcasted_iota(jnp.int32, (rows, size), 0)
        return jnp.concatenate(
            [(at - start == row).astype(jnp.float32) for start in starts], axis=0
        )

    def scaled(at):
        return mixed[:, at].astype(jnp.float32) * row_scale * inverse[:, at]

    def fold(lefts, label, h):
        total = None
        for k in range(labels):
            lhs = lefts[:, k * feats : (k + 1) * feats]
            if k == label:
                at = pl.ds(pl.multiple_of(h * step, LANES), step)
                rhs = x[label, :, :, at].reshape(feats, step)
                product = jnp.dot(lhs, rhs, preferred_element_type=jnp.float32)
            elif (k, label) in DIRECT:
                plane, task = DIRECT[k, label]
                rhs = g[
                    plane * eighth : (plane + 1) * eighth,
                    task * LANES : (task + 1) * LANES,
                    pl.ds(pl.multiple_of(h * step, LANES), step),
                ].reshape(feats, step)
                product = jnp.dot(lhs, rhs, preferred_element_type=jnp.float32)
            else:
                plane, task = DIRECT[label, k]
                few = step // LANES
                rhs = g[
                    pl.ds(plane * eighth + h * few, few), task * LANES : (task + 1) * LANES, :
                ].reshape(step, feats)
                product = lax.dot_general(
                    lhs, rhs, (((1,), (1,)), ((), ())), preferred_element_type=jnp.float32
                )
            total = product if total is None else total + product
        return total

    @pl.loop(0, labels * STEPS)
    def _(i):
        at = pl.ds(pl.multiple_of(i * step, step), step)
        left[:, at] = (scaled(at) * inverse[:, at]).astype(jnp.bfloat16)

    for label in range(labels):

        @pl.loop(0, STEPS)
        def _(h):
            at = pl.ds(pl.multiple_of(label * feats + h * step, step), step)
            squared = fold(left, label, h) * (inverse[:, at] * factor)
            square[:, at] = squared
            cubing[:, at] = (squared * inverse[:, at]).astype(jnp.bfloat16)

    def target(label, h):
        to = jnp.where(low, label, labels - 1 - label)
        return pl.ds(pl.multiple_of(to * feats + h * step, LANES), step), to * STEPS + h

    def swap(label, h):
        at, index = target(label, h)
        return remote(
            sent.at[:, at], came.at[:, at], out_sem, in_sem.at[index], across
        )

    def store(src, sems, label, h, out):
        at, _ = target(label, h)
        return pltpu.make_async_copy(src.at[:, at], out.at[:, at], sems)

    one_part = 4.0 - 6.0 * shift + 4.0 * shift**2 - shift**3
    linear_part = -6.0 + 8.0 * shift - 3.0 * shift**2
    square_part = 4.0 - 3.0 * shift

    for label in range(labels):

        @pl.loop(0, STEPS)
        def _(h):
            start_col = pl.multiple_of(label * feats + h * step, step)
            at = pl.ds(start_col, step)
            cube = fold(cubing, label, h) * (inverse[:, at] * factor)
            result = (
                one_part * identity(start_col, step) + linear_part * scaled(at)
                + square_part * square[:, at] - cube
            )
            to, _ = target(label, h)
            sent[:, to] = result[rows:].astype(jnp.bfloat16)
            swap(label, h).start()
            kept[:, to] = result[:rows]

            @pl.when(low)
            def _():
                store(kept, kept_sem, label, h, act_out).start()

            @pl.when(jnp.logical_not(low))
            def _():
                store(kept, kept_sem, label, h, grad_out).start()

    sent_all(first_in, one_send)
    sent_all(second_in, two_send)
    for kind, ref in enumerate((diag, g)):
        sent_all(ref.at[pl.ds(0, 2**stages - 1)], hop_send.at[kind])
        sent_all(ref.at[pl.ds(0, 2**stages)], hand_send.at[kind])

    for label in reversed(range(labels)):

        @pl.loop(0, STEPS)
        def _(h):
            to, _ = target(label, h)
            swap(label, h).wait_recv()
            wider_in[:, to] = came[:, to].astype(jnp.float32)

            @pl.when(low)
            def _():
                store(wider_in, came_sem, label, h, grad_out).start()

            @pl.when(jnp.logical_not(low))
            def _():
                store(wider_in, came_sem, label, h, act_out).start()

    sent_all(sent, out_sem)
    pltpu.make_async_copy(kept, act_out, kept_sem).wait()
    pltpu.make_async_copy(wider_in, grad_out, came_sem).wait()


def cut(length, unit, pieces):
    units = length // unit
    sizes = [(units // pieces + (1 if i < units % pieces else 0)) * unit for i in range(pieces)]
    return [(sum(sizes[:i]), sizes[i]) for i in range(pieces)]


def call(kernel, outs, scratch, *operands):
    return pl.pallas_call(
        kernel,
        out_shape=outs,
        in_specs=[pl.BlockSpec(memory_space=pl.ANY)] * len(operands),
        out_specs=[pl.BlockSpec(memory_space=pl.ANY)] * len(outs),
        scratch_shapes=scratch,
        compiler_params=pltpu.CompilerParams(
            collective_id=0, has_side_effects=True, vmem_limit_bytes=63 * 1024 * 1024
        ),
    )(*operands)


def split_body(tok, blk, activations, out_grads):
    depth, feats = activations.shape
    tokens = depth * tok
    width = feats * blk
    rows = width // (tok * blk)
    count = COUNT
    wide = feats // CUTS
    bf16, f32 = jnp.bfloat16, jnp.float32
    dma = pltpu.SemaphoreType.DMA
    steps = blk * STEPS
    return call(
        functools.partial(factor_kernel, tok, blk, tokens),
        [jax.ShapeDtypeStruct((rows, width), f32)] * 2,
        [
            pltpu.VMEM((blk, 2, depth, feats), bf16),
            pltpu.VMEM((depth, feats), bf16),
            pltpu.VMEM((depth, feats), bf16),
            pltpu.VMEM((4, feats // 2, 2 * depth), bf16),
            pltpu.VMEM((count, 2, 2, rows, wide), bf16),
            pltpu.VMEM((count, 2, 2, rows, wide // 2), bf16),
            pltpu.VMEM((count, 2, rows, wide // 2), bf16),
            pltpu.VMEM((count, 2, rows, wide // 2), bf16),
            pltpu.VMEM((count, 2, rows, wide // 2), f32),
            pltpu.VMEM((2 * tok, 3 * rows, feats), bf16),
            pltpu.VMEM((2 * tok, 2 * rows, feats // CUTS * SHORT), bf16),
            pltpu.VMEM((2 * rows, width), bf16),
            pltpu.VMEM((2 * rows, width), f32),
            pltpu.VMEM((2 * rows, width), bf16),
            pltpu.VMEM((2 * rows, width), bf16),
            pltpu.VMEM((1, width), f32),
            pltpu.VMEM((rows, width), bf16),
            pltpu.VMEM((rows, width), f32),
            pltpu.VMEM((rows, width), bf16),
            pltpu.VMEM((rows, width), f32),
            dma((2,)),
            dma, dma((blk, CUTS)), dma, dma((CUTS,)), dma, dma((blk, CUTS)),
            dma, dma((count,)), dma, dma((count,)),
            dma((2,)), dma((4, 8)), dma((2,)), dma((4,)),
            dma, dma((steps,)), dma, dma,
        ],
        activations, out_grads,
    )


def solution(mesh):
    tok, blk = mesh.shape["tok"], mesh.shape["blk"]
    placed = (P("tok", "blk"), P("tok", "blk"))

    def body(activations, out_grads):
        depth, feats = activations.shape
        whole = max(depth * tok, feats * blk) * feats * blk * activations.dtype.itemsize
        cube = tok == 2 * blk and blk == 4 and feats == tok * LANES == 2 * depth
        if whole <= gathered_budget and cube:
            return split_body(tok, blk, activations, out_grads)
        return tiled_body(activations, out_grads)

    return jax.shard_map(
        body,
        mesh=mesh,
        in_specs=placed,
        out_specs=(P(("tok", "blk"), None), P(("tok", "blk"), None)),
        check_vma=False,
    )
```

```python
import functools

import jax
import jax.numpy as jnp
import numpy as np
from jax import lax
from jax.experimental import pallas as pl
from jax.experimental.pallas import tpu as pltpu
from jax.sharding import PartitionSpec as P

damping = 0.3
epsilon = 1e-06
divisor = 2.0
gathered_budget = 32 * 1024 * 1024
LANES = 128
MESH = pl.DeviceIdType.MESH


def column_squares(data):
    values = data.astype(jnp.float32)
    return jnp.sum(values * values, axis=0)


def fold_product(row_block, tile):
    return jnp.dot(
        row_block,
        lax.all_gather(tile, "tok", axis=0, tiled=True),
        preferred_element_type=jnp.float32,
    )


def newton_steps(scaled, identity):
    half = scaled.astype(jnp.bfloat16)
    row_block = lax.all_gather(half, "blk", axis=1, tiled=True)
    square = fold_product(row_block, half)
    cube = fold_product(row_block, square.astype(jnp.bfloat16))
    return 4.0 * identity - 6.0 * scaled + 4.0 * square - cube


def tiled_body(activations, out_grads):
    tok_count = lax.axis_size("tok")
    blk_count = lax.axis_size("blk")
    tok_id = lax.axis_index("tok")
    blk_id = lax.axis_index("blk")
    token_count = activations.shape[0] * tok_count
    tile_cols = activations.shape[1]
    tile_rows = tile_cols * blk_count // tok_count
    row_ids = tok_id * tile_rows + jnp.arange(tile_rows, dtype=jnp.int32)
    col_ids = blk_id * tile_cols + jnp.arange(tile_cols, dtype=jnp.int32)
    identity = (row_ids[:, None] == col_ids[None, :]).astype(jnp.float32)

    def inverse_tile(local):
        full = lax.all_gather(local, "blk", axis=1, tiled=True)
        sums = lax.psum(column_squares(full).astype(jnp.bfloat16), "tok").astype(jnp.float32)
        gram_tile = lax.psum_scatter(
            lax.dot_general(
                full, local, (((0,), (0,)), ((), ())), preferred_element_type=jnp.float32
            ).astype(jnp.bfloat16),
            "tok",
            scatter_dimension=0,
            tiled=True,
        ).astype(jnp.float32)
        inverse = lax.rsqrt(sums / token_count + epsilon)
        inverse_rows = lax.dynamic_slice_in_dim(inverse, tok_id * tile_rows, tile_rows)
        inverse_cols = lax.dynamic_slice_in_dim(inverse, blk_id * tile_cols, tile_cols)
        damped = (
            gram_tile / token_count * inverse_rows[:, None] * inverse_cols[None, :]
            + damping * identity
        )
        result_tile = newton_steps(damped / divisor, identity)
        return lax.all_to_all(
            result_tile.astype(jnp.bfloat16), "blk", split_axis=0, concat_axis=1, tiled=True
        ).astype(result_tile.dtype)

    return inverse_tile(activations), inverse_tile(out_grads)


DIRECT = {
    (0, 1): (0, 0), (0, 3): (0, 1), (1, 3): (0, 2),
    (1, 2): (1, 0), (2, 0): (1, 1), (2, 3): (1, 2),
}
DIAGONAL = [(0, 0), (1, 0), (1, 1), (0, 1)]
CUTS = 4
SHORT = 3
COUNT = 2 * SHORT + 3 * CUTS
ADD_LAG = 3
END_LAG = 6
STEPS = 2


def pick(index, values):
    out = values[-1]
    for i in range(len(values) - 2, -1, -1):
        out = jnp.where(index == i, values[i], out)
    return out


def remote(src, dst, send, recv, device):
    return pltpu.make_async_remote_copy(
        src_ref=src, dst_ref=dst, send_sem=send, recv_sem=recv,
        device_id=device, device_id_type=MESH,
    )


def meet(peers):
    barrier = pltpu.get_barrier_semaphore()
    for peer in peers:
        pl.semaphore_signal(barrier, inc=1, device_id=peer, device_id_type=MESH)
    pl.semaphore_wait(barrier, len(peers))


def factor_kernel(
    tok, blk, tokens, acts, grads, act_out, grad_out,
    x, other, passed, turned, part, first_in, second_out, second_in, keep,
    g, diag, mixed, square, left, cubing, inverse, sent, kept, came, wider_in,
    load_sem, near_send, near_recv, pass_send, pass_recv, core_send, core_recv,
    one_send, one_recv, two_send, two_recv,
    hop_send, hop_recv, hand_send, hand_recv, out_sem, in_sem, kept_sem, came_sem,
):
    t = lax.axis_index("tok")
    b = lax.axis_index("blk")
    low = b < blk // 2
    place = jnp.where(low, b, blk - 1 - b)
    outer = place == 0
    inner = place == 1
    core, col, row = t % 2, t // 2 % 2, t // 4
    mate = (jnp.bitwise_xor(t, 1), b)
    beside = (jnp.bitwise_xor(t, 2), b)
    below = (jnp.bitwise_xor(t, 4), b)
    near = (t, jnp.bitwise_xor(b, 1))
    facing = (t, blk - 1 - b)
    across = (t, jnp.bitwise_xor(b, blk // 2))
    depth, feats = other.shape
    wide = feats // CUTS
    halfway = feats // 2
    count = COUNT
    first = SHORT
    split = SHORT + CUTS
    tail = split + 2 * CUTS

    def load(ref, dst, index):
        return pltpu.make_async_copy(ref, dst, load_sem.at[index])

    @pl.when(low)
    def _():
        load(acts, x.at[place, core], 0).start()
        load(grads, other, 1).start()

    @pl.when(jnp.logical_not(low))
    def _():
        load(grads, x.at[place, core], 0).start()
        load(acts, other, 1).start()

    meet([mate, beside, below, near, facing, across])
    load(acts, x.at[place, core], 0).wait()
    load(grads, other, 1).wait()

    def columns(h):
        return pl.ds(pl.multiple_of(h * wide, LANES), wide)

    def to_mate(label, h):
        here = x.at[label, core, :, columns(h)]
        return remote(
            here, here, core_send, core_recv.at[label, h], mate
        )

    def from_mate(label, h):
        there = x.at[label, 1 - core, :, columns(h)]
        return remote(
            there, there, core_send, core_recv.at[label, h], mate
        )

    def along(label, h, src, device):
        return remote(
            src, x.at[label, core, :, columns(h)],
            near_send, near_recv.at[label, h], device,
        )

    def arrived(label, h):
        here = x.at[label, core, :, columns(h)]
        return remote(here, here, near_send, near_recv.at[label, h], near)

    def give(h):
        return remote(
            other.at[:, columns(h)], passed.at[:, columns(h)],
            pass_send, pass_recv.at[h], near,
        )

    def onward(h):
        return remote(
            passed.at[:, columns(h)], x.at[3, core, :, columns(h)],
            pass_send, near_recv.at[3, h], facing,
        )

    for h in range(CUTS):
        to_mate(place, h).start()

    @pl.when(outer)
    def _():
        for h in range(CUTS):
            give(h).start()
        for h in range(CUTS):
            along(0, h, x.at[0, core, :, columns(h)], near).start()

    @pl.when(inner)
    def _():
        for h in range(CUTS):
            along(1, h, x.at[1, core, :, columns(h)], near).start()
            along(2, h, other.at[:, columns(h)], facing).start()

    def turn(slot, label, side):
        at = pl.ds(pl.multiple_of(side * halfway, LANES), halfway)
        for c in range(2):
            for r in range(0, depth, 256):
                turned[slot, :, c * depth + r : c * depth + r + 256] = x[
                    label, c, r : r + 256, at
                ].T

    def share(label, h):
        arrived(label, h).wait_recv()
        to_mate(label, h).start()

    def piece(n):
        task = jnp.where(
            n < first, 0,
            jnp.where(n < split, 1, jnp.where(n < tail, 2 + (n - split) % 2, 4)),
        )
        h = jnp.where(
            n < first, n,
            jnp.where(
                n < split, n - first, jnp.where(n < tail, (n - split) // 2, n - tail)
            ),
        )
        whole = (task > 0) & (task < 4)
        slot = jnp.where(outer, pick(task, [0, 0, 0, 1, 2]), pick(task, [0, 0, 1, 1, 1]))
        label = jnp.where(outer, pick(task, [0, 1, 3, 3, 3]), pick(task, [1, 2, 0, 3, 2]))
        corner = jnp.logical_not(whole) & (h == 2)
        slot = jnp.where(corner, 3, slot)
        inside = core * (CUTS // 2) + h
        at = jnp.where(whole, h, jnp.where(h == 2, CUTS // 2 + core, inside))
        return task, h, slot, label, at, whole

    def both(ref, sem):
        remote(ref, ref, sem, sem, mate).wait_recv()

    def sent_all(ref, sem):
        remote(ref, ref, sem, sem, mate).wait_send()

    def one(n, side):
        if side == 0:
            src, device = part.at[n, :, 1 - col, :, pl.ds(0, wide // 2)], beside
        else:
            src, device = part.at[n, 1 - row, :, :, pl.ds(wide // 2, wide // 2)], below
        return remote(
            src, first_in.at[n, side], one_send, one_recv.at[n], device
        )

    def two(n, side):
        return remote(
            second_out.at[n, side], second_in.at[n, side],
            two_send, two_recv.at[n], below if side == 0 else beside,
        )

    owners = g.shape[0]
    eighth = owners // 2
    early, late = [[0, 1, 2], [1, 0, 2]], [[2, 0, 1], [2, 1, 0]]
    orders = [early, early, late, late]
    groups = len(orders)
    moves = [(2, 0), (4, 0), (0, 1)]
    stages = len(moves)
    ranges = []
    for ref, at_row, size in (
        (diag, 0, LANES), (g, 0, LANES), (g, LANES, 2 * LANES), (diag, LANES, LANES)
    ):
        ranges.append([(ref, at_row + o, n) for o, n in cut(size, 16, 2)])

    def owner(device):
        tt, bb = device
        side = jnp.where(low, bb, blk - 1 - bb)
        return side * eighth + tt % 2 * (eighth // 2) + tt // 2

    me = owner((t, b))

    def flip(q, j, steps, tok_bits=0):
        blk_bits = 0
        for s in range(stages):
            if steps >> s & 1:
                dt, db = moves[orders[q][j][s]]
                tok_bits ^= dt
                blk_bits ^= db
        return jnp.bitwise_xor(t, tok_bits), jnp.bitwise_xor(b, blk_bits)

    def spot(q, j, device):
        ref, o, n = ranges[q][j]
        return ref.at[owner(device), pl.ds(o, n)]

    kinds = [0, 1, 1, 0]

    def whole_rows(q, owner_at):
        ref, o, n = ranges[q][0]
        return ref.at[owner_at, pl.ds(o, n + ranges[q][1][2])]

    def hop(q, j, steps, s):
        where = spot(q, j, flip(q, j, steps))
        return remote(
            where, where, hop_send.at[kinds[q]], hop_recv.at[q, steps | 1 << s],
            flip(q, j, 1 << s),
        )

    def hand(q, j, steps):
        where = spot(q, j, flip(q, j, steps))
        return remote(where, where, hand_send.at[kinds[q]], hand_recv.at[q], mate)

    def every(q, steps, s):
        for j in range(2):
            hop(q, j, steps, s).start()

    def landed(q, steps, onward_to=()):
        both(whole_rows(q, me), hop_recv.at[q, steps])
        for j in range(2):
            for s in onward_to:
                hop(q, j, steps, s).start()
            hand(q, j, steps).start()

    def begin(q):
        for s in range(stages):
            every(q, 0, s)
        for j in range(2):
            hand(q, j, 0).start()

    def forward(h):
        arrived(3, h).wait_recv()
        to_mate(3, h).start()

        @pl.when(inner)
        def _():
            along(3, h, x.at[3, core, :, columns(h)], near).start()

    for h in range(CUTS):
        from_mate(place, h).wait_recv()
    turn(0, place, core)
    turn(3, place, 0)
    gap = END_LAG

    def at_step(i):
        n = jnp.where(i < first, i, jnp.where(i < split + gap, i - gap, i - 2 * gap))
        low_part = (i >= 0) & (i < first)
        mid_part = (i >= first + gap) & (i < split + gap)
        return low_part | mid_part | ((i >= split + 2 * gap) & (i < count + 2 * gap)), n

    @pl.loop(0, count + 2 * gap + END_LAG)
    def _(i):
        active, n = at_step(i)

        @pl.when(i == first + gap)
        def _():
            for s in (0, 1):
                every(0, 0, s)
            for j in range(2):
                hand(0, j, 0).start()

        @pl.when(active & (n >= first) & (n < split))
        def _():
            h = n - first

            @pl.when(inner)
            def _():
                give(h).wait_recv()
                onward(h).start()

            share(place + 1, h)
            from_mate(place + 1, h).wait_recv()

        @pl.when(i == split + gap)
        def _():
            landed(0, 1, (1, 2))
            every(0, 0, 2)
            turn(1, place + 1, core)

        @pl.when(inner & (i == split + gap + gap // 2))
        def _():
            forward(0)

        @pl.when(i == split + 2 * gap)
        def _():
            landed(0, 2)
            landed(0, 3)
            for s in (0, 1):
                every(1, 0, s)
            for j in range(2):
                hand(1, j, 0).start()

        @pl.when(i == split + 2 * gap + CUTS)
        def _():
            landed(1, 1, (1,))

        @pl.when(i == tail + 2 * gap)
        def _():
            every(0, 2, 2)
            every(0, 3, 2)

        @pl.when(i == tail + 2 * gap + SHORT)
        def _():
            landed(1, 2)
            landed(1, 3)

        @pl.when(i == tail + 2 * gap + END_LAG)
        def _():
            begin(2)

        @pl.when(active & (n >= split) & (n < tail) & ((n - split) % 2 == 0))
        def _():
            h = (n - split) // 2

            @pl.when(outer | (h > 0))
            def _():
                forward(h)

            @pl.when(inner)
            def _():
                share(0, h)
                from_mate(0, h).wait_recv()

            from_mate(3, h).wait_recv()

        @pl.when(i == tail + 2 * gap)
        def _():
            turn(3, jnp.where(outer, 3, 2), 0)

            @pl.when(outer)
            def _():
                turn(2, 3, core)

        @pl.when(active)
        def _():
            task, h, slot, label, cut_at, _ = piece(n)
            at = pl.ds(pl.multiple_of(cut_at * wide, LANES), wide)
            right = x[label, :, :, at].reshape(2 * depth, wide)
            product = jnp.dot(turned[slot], right, preferred_element_type=jnp.float32)
            part[n] = product.astype(jnp.bfloat16).reshape(2, 2, LANES, wide)
            one(n, 0).start()
            one(n, 1).start()

        adding, m = at_step(i - ADD_LAG)

        @pl.when(adding)
        def _():
            lo, hi = pl.ds(0, wide // 2), pl.ds(wide // 2, wide // 2)
            both(first_in.at[m], one_recv.at[m])
            wider = jnp.float32
            second_out[m, 0] = (
                part[m, 1 - row, col, :, lo].astype(wider)
                + first_in[m, 0, 1 - row].astype(wider)
            ).astype(jnp.bfloat16)
            second_out[m, 1] = (
                part[m, row, 1 - col, :, hi].astype(wider)
                + first_in[m, 1, 1 - col].astype(wider)
            ).astype(jnp.bfloat16)
            two(m, 0).start()
            two(m, 1).start()
            keep[m, 0] = part[m, row, col, :, lo].astype(wider) + first_in[
                m, 0, row
            ].astype(wider)
            keep[m, 1] = part[m, row, col, :, hi].astype(wider) + first_in[
                m, 1, col
            ].astype(wider)

        ending, e = at_step(i - END_LAG)

        @pl.when(ending)
        def _():
            task, h, _, _, _, whole = piece(e)
            both(second_in.at[e], two_recv.at[e])
            for side in range(2):
                at = pl.ds(pl.multiple_of(h * wide + side * (wide // 2), LANES), wide // 2)
                total = keep[e, side] + second_in[e, side].astype(jnp.float32)
                total = total.astype(jnp.bfloat16)

                @pl.when(whole)
                def _():
                    g[me, pl.ds(pl.multiple_of((task - 1) * LANES, LANES), LANES), at] = total

                @pl.when(jnp.logical_not(whole))
                def _():
                    g_row = pl.multiple_of(task // 4 * LANES, LANES)
                    diag[me, pl.ds(g_row, LANES), at] = total

    def received(q):
        both(whole_rows(q, pl.ds(0, 2**stages)), hand_recv.at[q])

    half = blk // 2
    width = square.shape[1]
    labels = width // feats
    rows = LANES
    factor = 1.0 / (tokens * divisor)
    shift = damping / divisor
    eye = lax.broadcasted_iota(jnp.int32, (LANES, LANES), 0) == lax.broadcasted_iota(
        jnp.int32, (LANES, LANES), 1
    )
    quarter = eighth // 2
    step = feats // STEPS

    def diagonal(plane, k, sub, axis):
        at = pl.ds(pl.multiple_of(sub % quarter * LANES, LANES), LANES)
        own_rows = pl.ds(pl.multiple_of(k * LANES, LANES), LANES)
        block = jnp.where(eye, diag[plane * eighth + sub, own_rows, at].astype(jnp.float32), 0.0)
        total = jnp.sum(block, axis=axis, keepdims=True)
        return lax.rsqrt(total / tokens + epsilon)

    def rebuild(which):
        for label in range(labels):
            plane, k = DIAGONAL[label]
            if k != which:
                continue

            @pl.loop(0, eighth)
            def _(sub):
                at = pl.ds(pl.multiple_of(label * feats + sub * LANES, LANES), LANES)
                inverse[:, at] = diagonal(plane, k, sub, 0)

            own_rows = slice(k * LANES, (k + 1) * LANES)
            ends = [
                slice(plane * eighth + c * quarter, plane * eighth + (c + 1) * quarter)
                for c in range(2)
            ]
            for c in range(2):
                block = diag[ends[c], own_rows, :halfway].reshape(halfway, halfway)
                x[label, c, :, c * halfway : (c + 1) * halfway] = block
                lo = halfway + c * wide
                block = diag[ends[c], own_rows, halfway : halfway + wide].reshape(halfway, wide)
                x[label, 0, :, lo : lo + wide] = block
                x[label, 1, c * wide : (c + 1) * wide, :halfway] = block.T

    begin(3)
    for steps in range(4):
        every(1, steps, 2)
    sent_all(other, pass_send)

    @pl.when(outer)
    def _():
        sent_all(x.at[pl.ds(0, 3), 0], core_send)
        sent_all(x.at[pl.ds(0, 1), 0], near_send)

    @pl.when(inner)
    def _():
        sent_all(x.at[pl.ds(0, 4), 0], core_send)
        sent_all(x.at[pl.ds(0, 3), 0], near_send)

    landed(2, 1, (1, 2))
    landed(2, 2, (2,))
    for steps in range(4, 8):
        landed(0, steps)
    received(0)
    rebuild(0)
    landed(2, 3, (2,))
    landed(3, 1, (1, 2))
    landed(3, 2, (2,))
    landed(3, 3, (2,))
    for q in range(1, groups):
        for steps in range(4, 8):
            landed(q, steps)
    for q in range(1, groups):
        received(q)
    rebuild(1)

    block_of_rows = t // 2
    row_label = jnp.where(low, block_of_rows, labels - 1 - block_of_rows)
    subs = [t % 2 * blk + bb for bb in (b, jnp.bitwise_xor(b, half))]
    diag_plane = pick(row_label, [d[0] for d in DIAGONAL])
    diag_task = pick(row_label, [d[1] for d in DIAGONAL])
    inverse_rows = jnp.concatenate(
        [diagonal(diag_plane, diag_task, sub, 1) for sub in subs], axis=0
    )

    for label in range(labels):

        @pl.when(row_label == label)
        def _():
            for j in range(labels):
                cols = slice(j * feats, (j + 1) * feats)
                for s, sub in enumerate(subs):
                    if label == j:
                        at = pl.ds(pl.multiple_of(sub % quarter * LANES, LANES), LANES)
                        value = x[label, core, at, :]
                    elif (label, j) in DIRECT:
                        plane, k = DIRECT[label, j]
                        value = g[plane * eighth + sub, k * LANES : (k + 1) * LANES, :]
                    else:
                        plane, k = DIRECT[j, label]
                        at = pl.ds(pl.multiple_of(sub * LANES, LANES), LANES)
                        value = g[
                            plane * eighth : (plane + 1) * eighth, k * LANES : (k + 1) * LANES, at
                        ]
                        value = value.reshape(feats, LANES).T
                    mixed[s * rows : (s + 1) * rows, cols] = value

    starts = [row_label * feats + sub * LANES for sub in subs]
    row_scale = factor * inverse_rows

    def share_of(part):
        return slice(part * rows, (part + 1) * rows)

    def identity(part, first_col, size):
        at = first_col + lax.broadcasted_iota(jnp.int32, (rows, size), 1)
        row = lax.broadcasted_iota(jnp.int32, (rows, size), 0)
        return (at - starts[part] == row).astype(jnp.float32)

    def scaled(part, at):
        own_rows = share_of(part)
        return mixed[own_rows, at].astype(jnp.float32) * row_scale[own_rows] * inverse[:, at]

    def fold(lefts, part, label, h):
        total = None
        for k in range(labels):
            lhs = lefts[share_of(part), k * feats : (k + 1) * feats]
            if k == label:
                at = pl.ds(pl.multiple_of(h * step, LANES), step)
                rhs = x[label, :, :, at].reshape(feats, step)
                product = jnp.dot(lhs, rhs, preferred_element_type=jnp.float32)
            elif (k, label) in DIRECT:
                plane, task = DIRECT[k, label]
                rhs = g[
                    plane * eighth : (plane + 1) * eighth,
                    task * LANES : (task + 1) * LANES,
                    pl.ds(pl.multiple_of(h * step, LANES), step),
                ].reshape(feats, step)
                product = jnp.dot(lhs, rhs, preferred_element_type=jnp.float32)
            else:
                plane, task = DIRECT[label, k]
                few = step // LANES
                rhs = g[
                    pl.ds(plane * eighth + h * few, few), task * LANES : (task + 1) * LANES, :
                ].reshape(step, feats)
                product = lax.dot_general(
                    lhs, rhs, (((1,), (1,)), ((), ())), preferred_element_type=jnp.float32
                )
            total = product if total is None else total + product
        return total

    def square_rows(part):
        own_rows = share_of(part)

        @pl.loop(0, labels * STEPS)
        def _(i):
            at = pl.ds(pl.multiple_of(i * step, step), step)
            left[own_rows, at] = (scaled(part, at) * inverse[:, at]).astype(jnp.bfloat16)

        for label in range(labels):

            @pl.loop(0, STEPS)
            def _(h):
                at = pl.ds(pl.multiple_of(label * feats + h * step, step), step)
                squared = fold(left, part, label, h) * (inverse[:, at] * factor)
                square[own_rows, at] = squared
                cubing[own_rows, at] = (squared * inverse[:, at]).astype(jnp.bfloat16)

    def target(label, h):
        to = jnp.where(low, label, labels - 1 - label)
        return pl.ds(pl.multiple_of(to * feats + h * step, LANES), step), to * STEPS + h

    def swap(label, h):
        at, index = target(label, h)
        return remote(
            sent.at[:, at], came.at[:, at], out_sem, in_sem.at[index], across
        )

    def store(src, sems, label, h, out):
        at, _ = target(label, h)
        return pltpu.make_async_copy(src.at[:, at], out.at[:, at], sems)

    one_part = 4.0 - 6.0 * shift + 4.0 * shift**2 - shift**3
    linear_part = -6.0 + 8.0 * shift - 3.0 * shift**2
    square_part = 4.0 - 3.0 * shift

    def cube_chunk(part, label, h):
        start_col = pl.multiple_of(label * feats + h * step, step)
        at = pl.ds(start_col, step)
        cube = fold(cubing, part, label, h) * (inverse[:, at] * factor)
        return (
            one_part * identity(part, start_col, step) + linear_part * scaled(part, at)
            + square_part * square[share_of(part), at] - cube
        )

    square_rows(1)
    for label in range(labels):

        @pl.loop(0, STEPS)
        def _(h):
            to, _ = target(label, h)
            sent[:, to] = cube_chunk(1, label, h).astype(jnp.bfloat16)
            swap(label, h).start()

    square_rows(0)
    for label in range(labels):

        @pl.loop(0, STEPS)
        def _(h):
            to, _ = target(label, h)
            kept[:, to] = cube_chunk(0, label, h)

            @pl.when(low)
            def _():
                store(kept, kept_sem, label, h, act_out).start()

            @pl.when(jnp.logical_not(low))
            def _():
                store(kept, kept_sem, label, h, grad_out).start()

    sent_all(first_in, one_send)
    sent_all(second_in, two_send)
    for kind, ref in enumerate((diag, g)):
        sent_all(ref.at[pl.ds(0, 2**stages - 1)], hop_send.at[kind])
        sent_all(ref.at[pl.ds(0, 2**stages)], hand_send.at[kind])

    for label in reversed(range(labels)):

        @pl.loop(0, STEPS)
        def _(h):
            to, _ = target(label, h)
            swap(label, h).wait_recv()
            wider_in[:, to] = came[:, to].astype(jnp.float32)

            @pl.when(low)
            def _():
                store(wider_in, came_sem, label, h, grad_out).start()

            @pl.when(jnp.logical_not(low))
            def _():
                store(wider_in, came_sem, label, h, act_out).start()

    sent_all(sent, out_sem)
    pltpu.make_async_copy(kept, act_out, kept_sem).wait()
    pltpu.make_async_copy(wider_in, grad_out, came_sem).wait()


def cut(length, unit, pieces):
    units = length // unit
    sizes = [(units // pieces + (1 if i < units % pieces else 0)) * unit for i in range(pieces)]
    return [(sum(sizes[:i]), sizes[i]) for i in range(pieces)]


def call(kernel, outs, scratch, *operands):
    return pl.pallas_call(
        kernel,
        out_shape=outs,
        in_specs=[pl.BlockSpec(memory_space=pl.ANY)] * len(operands),
        out_specs=[pl.BlockSpec(memory_space=pl.ANY)] * len(outs),
        scratch_shapes=scratch,
        compiler_params=pltpu.CompilerParams(
            collective_id=0, has_side_effects=True, vmem_limit_bytes=63 * 1024 * 1024
        ),
    )(*operands)


def split_body(tok, blk, activations, out_grads):
    depth, feats = activations.shape
    tokens = depth * tok
    width = feats * blk
    rows = width // (tok * blk)
    count = COUNT
    wide = feats // CUTS
    bf16, f32 = jnp.bfloat16, jnp.float32
    dma = pltpu.SemaphoreType.DMA
    steps = blk * STEPS
    return call(
        functools.partial(factor_kernel, tok, blk, tokens),
        [jax.ShapeDtypeStruct((rows, width), f32)] * 2,
        [
            pltpu.VMEM((blk, 2, depth, feats), bf16),
            pltpu.VMEM((depth, feats), bf16),
            pltpu.VMEM((depth, feats), bf16),
            pltpu.VMEM((4, feats // 2, 2 * depth), bf16),
            pltpu.VMEM((count, 2, 2, rows, wide), bf16),
            pltpu.VMEM((count, 2, 2, rows, wide // 2), bf16),
            pltpu.VMEM((count, 2, rows, wide // 2), bf16),
            pltpu.VMEM((count, 2, rows, wide // 2), bf16),
            pltpu.VMEM((count, 2, rows, wide // 2), f32),
            pltpu.VMEM((2 * tok, 3 * rows, feats), bf16),
            pltpu.VMEM((2 * tok, 2 * rows, feats // CUTS * SHORT), bf16),
            pltpu.VMEM((2 * rows, width), bf16),
            pltpu.VMEM((2 * rows, width), f32),
            pltpu.VMEM((2 * rows, width), bf16),
            pltpu.VMEM((2 * rows, width), bf16),
            pltpu.VMEM((1, width), f32),
            pltpu.VMEM((rows, width), bf16),
            pltpu.VMEM((rows, width), f32),
            pltpu.VMEM((rows, width), bf16),
            pltpu.VMEM((rows, width), f32),
            dma((2,)),
            dma, dma((blk, CUTS)), dma, dma((CUTS,)), dma, dma((blk, CUTS)),
            dma, dma((count,)), dma, dma((count,)),
            dma((2,)), dma((4, 8)), dma((2,)), dma((4,)),
            dma, dma((steps,)), dma, dma,
        ],
        activations, out_grads,
    )


def solution(mesh):
    tok, blk = mesh.shape["tok"], mesh.shape["blk"]
    placed = (P("tok", "blk"), P("tok", "blk"))

    def body(activations, out_grads):
        depth, feats = activations.shape
        whole = max(depth * tok, feats * blk) * feats * blk * activations.dtype.itemsize
        cube = tok == 2 * blk and blk == 4 and feats == tok * LANES == 2 * depth
        if whole <= gathered_budget and cube:
            return split_body(tok, blk, activations, out_grads)
        return tiled_body(activations, out_grads)

    return jax.shard_map(
        body,
        mesh=mesh,
        in_specs=placed,
        out_specs=(P(("tok", "blk"), None), P(("tok", "blk"), None)),
        check_vma=False,
    )
```

```python
import functools

import jax
import jax.numpy as jnp
import numpy as np
from jax import lax
from jax.experimental import pallas as pl
from jax.experimental.pallas import tpu as pltpu
from jax.sharding import PartitionSpec as P

damping = 0.3
epsilon = 1e-06
divisor = 2.0
gathered_budget = 32 * 1024 * 1024
LANES = 128
MESH = pl.DeviceIdType.MESH


def column_squares(data):
    values = data.astype(jnp.float32)
    return jnp.sum(values * values, axis=0)


def fold_product(row_block, tile):
    return jnp.dot(
        row_block,
        lax.all_gather(tile, "tok", axis=0, tiled=True),
        preferred_element_type=jnp.float32,
    )


def newton_steps(scaled, identity):
    half = scaled.astype(jnp.bfloat16)
    row_block = lax.all_gather(half, "blk", axis=1, tiled=True)
    square = fold_product(row_block, half)
    cube = fold_product(row_block, square.astype(jnp.bfloat16))
    return 4.0 * identity - 6.0 * scaled + 4.0 * square - cube


def tiled_body(activations, out_grads):
    tok_count = lax.axis_size("tok")
    blk_count = lax.axis_size("blk")
    tok_id = lax.axis_index("tok")
    blk_id = lax.axis_index("blk")
    token_count = activations.shape[0] * tok_count
    tile_cols = activations.shape[1]
    tile_rows = tile_cols * blk_count // tok_count
    row_ids = tok_id * tile_rows + jnp.arange(tile_rows, dtype=jnp.int32)
    col_ids = blk_id * tile_cols + jnp.arange(tile_cols, dtype=jnp.int32)
    identity = (row_ids[:, None] == col_ids[None, :]).astype(jnp.float32)

    def inverse_tile(local):
        full = lax.all_gather(local, "blk", axis=1, tiled=True)
        sums = lax.psum(column_squares(full).astype(jnp.bfloat16), "tok").astype(jnp.float32)
        gram_tile = lax.psum_scatter(
            lax.dot_general(
                full, local, (((0,), (0,)), ((), ())), preferred_element_type=jnp.float32
            ).astype(jnp.bfloat16),
            "tok",
            scatter_dimension=0,
            tiled=True,
        ).astype(jnp.float32)
        inverse = lax.rsqrt(sums / token_count + epsilon)
        inverse_rows = lax.dynamic_slice_in_dim(inverse, tok_id * tile_rows, tile_rows)
        inverse_cols = lax.dynamic_slice_in_dim(inverse, blk_id * tile_cols, tile_cols)
        damped = (
            gram_tile / token_count * inverse_rows[:, None] * inverse_cols[None, :]
            + damping * identity
        )
        result_tile = newton_steps(damped / divisor, identity)
        return lax.all_to_all(
            result_tile.astype(jnp.bfloat16), "blk", split_axis=0, concat_axis=1, tiled=True
        ).astype(result_tile.dtype)

    return inverse_tile(activations), inverse_tile(out_grads)


DIRECT = {
    (0, 1): (0, 0), (0, 3): (0, 1), (1, 3): (0, 2),
    (1, 2): (1, 0), (2, 0): (1, 1), (2, 3): (1, 2),
}
DIAGONAL = [(0, 0), (1, 0), (1, 1), (0, 1)]
CUTS = 4
SHORT = 3
COUNT = 2 * SHORT + 3 * CUTS
ADD_LAG = 3
END_LAG = 6
STEPS = 2


def pick(index, values):
    out = values[-1]
    for i in range(len(values) - 2, -1, -1):
        out = jnp.where(index == i, values[i], out)
    return out


def remote(src, dst, send, recv, device):
    return pltpu.make_async_remote_copy(
        src_ref=src, dst_ref=dst, send_sem=send, recv_sem=recv,
        device_id=device, device_id_type=MESH,
    )


def meet(peers):
    barrier = pltpu.get_barrier_semaphore()
    for peer in peers:
        pl.semaphore_signal(barrier, inc=1, device_id=peer, device_id_type=MESH)
    pl.semaphore_wait(barrier, len(peers))


def factor_kernel(
    tok, blk, tokens, acts, grads, act_out, grad_out,
    x, other, passed, turned, part, first_in, second_out, second_in, keep,
    g, diag, mixed, square, left, cubing, inverse, sent, kept, came, wider_in,
    load_sem, near_send, near_recv, pass_send, pass_recv, core_send, core_recv,
    one_send, one_recv, two_send, two_recv,
    hop_send, hop_recv, hand_send, hand_recv, out_sem, in_sem, kept_sem, came_sem,
):
    t = lax.axis_index("tok")
    b = lax.axis_index("blk")
    low = b < blk // 2
    place = jnp.where(low, b, blk - 1 - b)
    outer = place == 0
    inner = place == 1
    core, col, row = t % 2, t // 2 % 2, t // 4
    mate = (jnp.bitwise_xor(t, 1), b)
    beside = (jnp.bitwise_xor(t, 2), b)
    below = (jnp.bitwise_xor(t, 4), b)
    near = (t, jnp.bitwise_xor(b, 1))
    facing = (t, blk - 1 - b)
    across = (t, jnp.bitwise_xor(b, blk // 2))
    depth, feats = other.shape
    wide = feats // CUTS
    halfway = feats // 2
    count = COUNT
    first = SHORT
    split = SHORT + CUTS
    tail = split + 2 * CUTS

    def load(ref, dst, index):
        return pltpu.make_async_copy(ref, dst, load_sem.at[index])

    @pl.when(low)
    def _():
        load(acts, x.at[place, core], 0).start()
        load(grads, other, 1).start()

    @pl.when(jnp.logical_not(low))
    def _():
        load(grads, x.at[place, core], 0).start()
        load(acts, other, 1).start()

    meet([mate, beside, below, near, facing, across])
    load(acts, x.at[place, core], 0).wait()
    load(grads, other, 1).wait()

    def columns(h):
        return pl.ds(pl.multiple_of(h * wide, LANES), wide)

    def to_mate(label, h):
        here = x.at[label, core, :, columns(h)]
        return remote(
            here, here, core_send, core_recv.at[label, h], mate
        )

    def from_mate(label, h):
        there = x.at[label, 1 - core, :, columns(h)]
        return remote(
            there, there, core_send, core_recv.at[label, h], mate
        )

    def along(label, h, src, device):
        return remote(
            src, x.at[label, core, :, columns(h)],
            near_send, near_recv.at[label, h], device,
        )

    def arrived(label, h):
        here = x.at[label, core, :, columns(h)]
        return remote(here, here, near_send, near_recv.at[label, h], near)

    def give(h):
        return remote(
            other.at[:, columns(h)], passed.at[:, columns(h)],
            pass_send, pass_recv.at[h], near,
        )

    def onward(h):
        return remote(
            passed.at[:, columns(h)], x.at[3, core, :, columns(h)],
            pass_send, near_recv.at[3, h], facing,
        )

    for h in range(CUTS):
        to_mate(place, h).start()

    @pl.when(outer)
    def _():
        for h in range(CUTS):
            give(h).start()
        for h in range(CUTS):
            along(0, h, x.at[0, core, :, columns(h)], near).start()

    @pl.when(inner)
    def _():
        for h in range(CUTS):
            along(1, h, x.at[1, core, :, columns(h)], near).start()
            along(2, h, other.at[:, columns(h)], facing).start()

    def turn(slot, label, side):
        at = pl.ds(pl.multiple_of(side * halfway, LANES), halfway)
        for c in range(2):
            for r in range(0, depth, 256):
                turned[slot, :, c * depth + r : c * depth + r + 256] = x[
                    label, c, r : r + 256, at
                ].T

    def share(label, h):
        arrived(label, h).wait_recv()
        to_mate(label, h).start()

    def piece(n):
        task = jnp.where(
            n < first, 0,
            jnp.where(n < split, 1, jnp.where(n < tail, 2 + (n - split) % 2, 4)),
        )
        h = jnp.where(
            n < first, n,
            jnp.where(
                n < split, n - first, jnp.where(n < tail, (n - split) // 2, n - tail)
            ),
        )
        whole = (task > 0) & (task < 4)
        slot = jnp.where(outer, pick(task, [0, 0, 0, 1, 2]), pick(task, [0, 0, 1, 1, 1]))
        label = jnp.where(outer, pick(task, [0, 1, 3, 3, 3]), pick(task, [1, 2, 0, 3, 2]))
        corner = jnp.logical_not(whole) & (h == 2)
        slot = jnp.where(corner, 3, slot)
        inside = core * (CUTS // 2) + h
        at = jnp.where(whole, h, jnp.where(h == 2, CUTS // 2 + core, inside))
        return task, h, slot, label, at, whole

    def both(ref, sem):
        remote(ref, ref, sem, sem, mate).wait_recv()

    def sent_all(ref, sem):
        remote(ref, ref, sem, sem, mate).wait_send()

    def one(n, side):
        if side == 0:
            src, device = part.at[n, :, 1 - col, :, pl.ds(0, wide // 2)], beside
        else:
            src, device = part.at[n, 1 - row, :, :, pl.ds(wide // 2, wide // 2)], below
        return remote(
            src, first_in.at[n, side], one_send, one_recv.at[n], device
        )

    def two(n, side):
        return remote(
            second_out.at[n, side], second_in.at[n, side],
            two_send, two_recv.at[n], below if side == 0 else beside,
        )

    owners = g.shape[0]
    eighth = owners // 2
    early, late = [[0, 1, 2], [1, 0, 2]], [[2, 0, 1], [2, 1, 0]]
    orders = [early, early, late, late]
    groups = len(orders)
    moves = [(2, 0), (4, 0), (0, 1)]
    stages = len(moves)
    ranges = []
    for ref, at_row, size in (
        (diag, 0, LANES), (g, 0, LANES), (g, LANES, 2 * LANES), (diag, LANES, LANES)
    ):
        ranges.append([(ref, at_row + o, n) for o, n in cut(size, 16, 2)])

    def owner(device):
        tt, bb = device
        side = jnp.where(low, bb, blk - 1 - bb)
        return side * eighth + tt % 2 * (eighth // 2) + tt // 2

    me = owner((t, b))

    def flip(q, j, steps, tok_bits=0):
        blk_bits = 0
        for s in range(stages):
            if steps >> s & 1:
                dt, db = moves[orders[q][j][s]]
                tok_bits ^= dt
                blk_bits ^= db
        return jnp.bitwise_xor(t, tok_bits), jnp.bitwise_xor(b, blk_bits)

    def spot(q, j, device):
        ref, o, n = ranges[q][j]
        return ref.at[owner(device), pl.ds(o, n)]

    kinds = [0, 1, 1, 0]

    def whole_rows(q, owner_at):
        ref, o, n = ranges[q][0]
        return ref.at[owner_at, pl.ds(o, n + ranges[q][1][2])]

    def hop(q, j, steps, s):
        where = spot(q, j, flip(q, j, steps))
        return remote(
            where, where, hop_send.at[kinds[q]], hop_recv.at[q, steps | 1 << s],
            flip(q, j, 1 << s),
        )

    def hand(q, j, steps):
        where = spot(q, j, flip(q, j, steps))
        return remote(where, where, hand_send.at[kinds[q]], hand_recv.at[q], mate)

    def every(q, steps, s):
        for j in range(2):
            hop(q, j, steps, s).start()

    def landed(q, steps, onward_to=()):
        both(whole_rows(q, me), hop_recv.at[q, steps])
        for j in range(2):
            for s in onward_to:
                hop(q, j, steps, s).start()
            hand(q, j, steps).start()

    def begin(q):
        for s in range(stages):
            every(q, 0, s)
        for j in range(2):
            hand(q, j, 0).start()

    def forward(h):
        arrived(3, h).wait_recv()
        to_mate(3, h).start()

        @pl.when(inner)
        def _():
            along(3, h, x.at[3, core, :, columns(h)], near).start()

    for h in range(CUTS):
        from_mate(place, h).wait_recv()
    turn(0, place, core)
    turn(3, place, 0)
    gap = END_LAG

    def at_step(i):
        n = jnp.where(i < first, i, jnp.where(i < split + gap, i - gap, i - 2 * gap))
        low_part = (i >= 0) & (i < first)
        mid_part = (i >= first + gap) & (i < split + gap)
        return low_part | mid_part | ((i >= split + 2 * gap) & (i < count + 2 * gap)), n

    @pl.loop(0, count + 2 * gap + END_LAG)
    def _(i):
        active, n = at_step(i)

        @pl.when(i == first + gap)
        def _():
            for s in (0, 1):
                every(0, 0, s)
            for j in range(2):
                hand(0, j, 0).start()

        @pl.when(active & (n >= first) & (n < split))
        def _():
            h = n - first

            @pl.when(inner)
            def _():
                give(h).wait_recv()
                onward(h).start()

            share(place + 1, h)
            from_mate(place + 1, h).wait_recv()

        @pl.when(i == split + gap)
        def _():
            landed(0, 1, (1, 2))
            every(0, 0, 2)
            turn(1, place + 1, core)

        @pl.when(inner & (i == split + gap + gap // 2))
        def _():
            forward(0)

        @pl.when(i == split + 2 * gap)
        def _():
            landed(0, 2)
            landed(0, 3)
            for s in (0, 1):
                every(1, 0, s)

            @pl.when(outer)
            def _():
                every(1, 0, 2)

            for j in range(2):
                hand(1, j, 0).start()

        @pl.when(i == split + 2 * gap + CUTS)
        def _():
            landed(1, 1, (1,))

        @pl.when(i == tail + 2 * gap)
        def _():
            every(0, 2, 2)
            every(0, 3, 2)

        @pl.when(i == tail + 2 * gap + SHORT)
        def _():
            landed(1, 2)
            landed(1, 3)

        @pl.when(i == tail + 2 * gap + END_LAG)
        def _():
            begin(2)

        @pl.when(active & (n >= split) & (n < tail) & ((n - split) % 2 == 0))
        def _():
            h = (n - split) // 2

            @pl.when(outer | (h > 0))
            def _():
                forward(h)

            @pl.when(inner)
            def _():
                share(0, h)
                from_mate(0, h).wait_recv()

            from_mate(3, h).wait_recv()

        @pl.when(i == tail + 2 * gap)
        def _():
            turn(3, jnp.where(outer, 3, 2), 0)

            @pl.when(outer)
            def _():
                turn(2, 3, core)

        @pl.when(active)
        def _():
            task, h, slot, label, cut_at, _ = piece(n)
            at = pl.ds(pl.multiple_of(cut_at * wide, LANES), wide)
            right = x[label, :, :, at].reshape(2 * depth, wide)
            product = jnp.dot(turned[slot], right, preferred_element_type=jnp.float32)
            part[n] = product.astype(jnp.bfloat16).reshape(2, 2, LANES, wide)
            one(n, 0).start()
            one(n, 1).start()

        adding, m = at_step(i - ADD_LAG)

        @pl.when(adding)
        def _():
            lo, hi = pl.ds(0, wide // 2), pl.ds(wide // 2, wide // 2)
            both(first_in.at[m], one_recv.at[m])
            wider = jnp.float32
            second_out[m, 0] = (
                part[m, 1 - row, col, :, lo].astype(wider)
                + first_in[m, 0, 1 - row].astype(wider)
            ).astype(jnp.bfloat16)
            second_out[m, 1] = (
                part[m, row, 1 - col, :, hi].astype(wider)
                + first_in[m, 1, 1 - col].astype(wider)
            ).astype(jnp.bfloat16)
            two(m, 0).start()
            two(m, 1).start()
            keep[m, 0] = part[m, row, col, :, lo].astype(wider) + first_in[
                m, 0, row
            ].astype(wider)
            keep[m, 1] = part[m, row, col, :, hi].astype(wider) + first_in[
                m, 1, col
            ].astype(wider)

        ending, e = at_step(i - END_LAG)

        @pl.when(ending)
        def _():
            task, h, _, _, _, whole = piece(e)
            both(second_in.at[e], two_recv.at[e])
            for side in range(2):
                at = pl.ds(pl.multiple_of(h * wide + side * (wide // 2), LANES), wide // 2)
                total = keep[e, side] + second_in[e, side].astype(jnp.float32)
                total = total.astype(jnp.bfloat16)

                @pl.when(whole)
                def _():
                    g[me, pl.ds(pl.multiple_of((task - 1) * LANES, LANES), LANES), at] = total

                @pl.when(jnp.logical_not(whole))
                def _():
                    g_row = pl.multiple_of(task // 4 * LANES, LANES)
                    diag[me, pl.ds(g_row, LANES), at] = total

    def received(q):
        both(whole_rows(q, pl.ds(0, 2**stages)), hand_recv.at[q])

    half = blk // 2
    width = square.shape[1]
    labels = width // feats
    rows = LANES
    factor = 1.0 / (tokens * divisor)
    shift = damping / divisor
    eye = lax.broadcasted_iota(jnp.int32, (LANES, LANES), 0) == lax.broadcasted_iota(
        jnp.int32, (LANES, LANES), 1
    )
    quarter = eighth // 2
    step = feats // STEPS

    def diagonal(plane, k, sub, axis):
        at = pl.ds(pl.multiple_of(sub % quarter * LANES, LANES), LANES)
        own_rows = pl.ds(pl.multiple_of(k * LANES, LANES), LANES)
        block = jnp.where(eye, diag[plane * eighth + sub, own_rows, at].astype(jnp.float32), 0.0)
        total = jnp.sum(block, axis=axis, keepdims=True)
        return lax.rsqrt(total / tokens + epsilon)

    def rebuild(which):
        for label in range(labels):
            plane, k = DIAGONAL[label]
            if k != which:
                continue

            @pl.loop(0, eighth)
            def _(sub):
                at = pl.ds(pl.multiple_of(label * feats + sub * LANES, LANES), LANES)
                inverse[:, at] = diagonal(plane, k, sub, 0)

            own_rows = slice(k * LANES, (k + 1) * LANES)
            ends = [
                slice(plane * eighth + c * quarter, plane * eighth + (c + 1) * quarter)
                for c in range(2)
            ]
            for c in range(2):
                block = diag[ends[c], own_rows, :halfway].reshape(halfway, halfway)
                x[label, c, :, c * halfway : (c + 1) * halfway] = block
                lo = halfway + c * wide
                block = diag[ends[c], own_rows, halfway : halfway + wide].reshape(halfway, wide)
                x[label, 0, :, lo : lo + wide] = block
                x[label, 1, c * wide : (c + 1) * wide, :halfway] = block.T

    begin(3)

    @pl.when(inner)
    def _():
        every(1, 0, 2)

    for steps in range(1, 4):
        every(1, steps, 2)
    sent_all(other, pass_send)

    @pl.when(outer)
    def _():
        sent_all(x.at[pl.ds(0, 3), 0], core_send)
        sent_all(x.at[pl.ds(0, 1), 0], near_send)

    @pl.when(inner)
    def _():
        sent_all(x.at[pl.ds(0, 4), 0], core_send)
        sent_all(x.at[pl.ds(0, 3), 0], near_send)

    landed(2, 1, (1, 2))
    landed(2, 2, (2,))
    for steps in range(4, 8):
        landed(0, steps)
    received(0)
    rebuild(0)
    landed(2, 3, (2,))
    landed(3, 1, (1, 2))
    landed(3, 2, (2,))
    landed(3, 3, (2,))
    for q in range(1, groups):
        for steps in range(4, 8):
            landed(q, steps)
    for q in range(1, groups):
        received(q)
    rebuild(1)

    block_of_rows = t // 2
    row_label = jnp.where(low, block_of_rows, labels - 1 - block_of_rows)
    subs = [t % 2 * blk + bb for bb in (b, jnp.bitwise_xor(b, half))]
    diag_plane = pick(row_label, [d[0] for d in DIAGONAL])
    diag_task = pick(row_label, [d[1] for d in DIAGONAL])
    inverse_rows = jnp.concatenate(
        [diagonal(diag_plane, diag_task, sub, 1) for sub in subs], axis=0
    )

    for label in range(labels):

        @pl.when(row_label == label)
        def _():
            for j in range(labels):
                cols = slice(j * feats, (j + 1) * feats)
                for s, sub in enumerate(subs):
                    if label == j:
                        at = pl.ds(pl.multiple_of(sub % quarter * LANES, LANES), LANES)
                        value = x[label, core, at, :]
                    elif (label, j) in DIRECT:
                        plane, k = DIRECT[label, j]
                        value = g[plane * eighth + sub, k * LANES : (k + 1) * LANES, :]
                    else:
                        plane, k = DIRECT[j, label]
                        at = pl.ds(pl.multiple_of(sub * LANES, LANES), LANES)
                        value = g[
                            plane * eighth : (plane + 1) * eighth, k * LANES : (k + 1) * LANES, at
                        ]
                        value = value.reshape(feats, LANES).T
                    mixed[s * rows : (s + 1) * rows, cols] = value

    starts = [row_label * feats + sub * LANES for sub in subs]
    row_scale = factor * inverse_rows

    def share_of(part):
        return slice(part * rows, (part + 1) * rows)

    def identity(part, first_col, size):
        at = first_col + lax.broadcasted_iota(jnp.int32, (rows, size), 1)
        row = lax.broadcasted_iota(jnp.int32, (rows, size), 0)
        return (at - starts[part] == row).astype(jnp.float32)

    def scaled(part, at):
        own_rows = share_of(part)
        return mixed[own_rows, at].astype(jnp.float32) * row_scale[own_rows] * inverse[:, at]

    def fold(lefts, part, label, h):
        total = None
        for k in range(labels):
            lhs = lefts[share_of(part), k * feats : (k + 1) * feats]
            if k == label:
                at = pl.ds(pl.multiple_of(h * step, LANES), step)
                rhs = x[label, :, :, at].reshape(feats, step)
                product = jnp.dot(lhs, rhs, preferred_element_type=jnp.float32)
            elif (k, label) in DIRECT:
                plane, task = DIRECT[k, label]
                rhs = g[
                    plane * eighth : (plane + 1) * eighth,
                    task * LANES : (task + 1) * LANES,
                    pl.ds(pl.multiple_of(h * step, LANES), step),
                ].reshape(feats, step)
                product = jnp.dot(lhs, rhs, preferred_element_type=jnp.float32)
            else:
                plane, task = DIRECT[label, k]
                few = step // LANES
                rhs = g[
                    pl.ds(plane * eighth + h * few, few), task * LANES : (task + 1) * LANES, :
                ].reshape(step, feats)
                product = lax.dot_general(
                    lhs, rhs, (((1,), (1,)), ((), ())), preferred_element_type=jnp.float32
                )
            total = product if total is None else total + product
        return total

    def square_rows(part):
        own_rows = share_of(part)

        @pl.loop(0, labels * STEPS)
        def _(i):
            at = pl.ds(pl.multiple_of(i * step, step), step)
            left[own_rows, at] = (scaled(part, at) * inverse[:, at]).astype(jnp.bfloat16)

        for label in range(labels):

            @pl.loop(0, STEPS)
            def _(h):
                at = pl.ds(pl.multiple_of(label * feats + h * step, step), step)
                squared = fold(left, part, label, h) * (inverse[:, at] * factor)
                square[own_rows, at] = squared
                cubing[own_rows, at] = (squared * inverse[:, at]).astype(jnp.bfloat16)

    def target(label, h):
        to = jnp.where(low, label, labels - 1 - label)
        return pl.ds(pl.multiple_of(to * feats + h * step, LANES), step), to * STEPS + h

    def swap(label, h):
        at, index = target(label, h)
        return remote(
            sent.at[:, at], came.at[:, at], out_sem, in_sem.at[index], across
        )

    def store(src, sems, label, h, out):
        at, _ = target(label, h)
        return pltpu.make_async_copy(src.at[:, at], out.at[:, at], sems)

    one_part = 4.0 - 6.0 * shift + 4.0 * shift**2 - shift**3
    linear_part = -6.0 + 8.0 * shift - 3.0 * shift**2
    square_part = 4.0 - 3.0 * shift

    def cube_chunk(part, label, h):
        start_col = pl.multiple_of(label * feats + h * step, step)
        at = pl.ds(start_col, step)
        cube = fold(cubing, part, label, h) * (inverse[:, at] * factor)
        return (
            one_part * identity(part, start_col, step) + linear_part * scaled(part, at)
            + square_part * square[share_of(part), at] - cube
        )

    square_rows(1)
    for label in [labels - 1, *range(labels - 1)]:

        @pl.loop(0, STEPS)
        def _(h):
            to, _ = target(label, h)
            sent[:, to] = cube_chunk(1, label, h).astype(jnp.bfloat16)
            swap(label, h).start()

    square_rows(0)
    for label in range(labels):

        @pl.loop(0, STEPS)
        def _(h):
            to, _ = target(label, h)
            kept[:, to] = cube_chunk(0, label, h)

            @pl.when(low)
            def _():
                store(kept, kept_sem, label, h, act_out).start()

            @pl.when(jnp.logical_not(low))
            def _():
                store(kept, kept_sem, label, h, grad_out).start()

    sent_all(first_in, one_send)
    sent_all(second_in, two_send)
    for kind, ref in enumerate((diag, g)):
        sent_all(ref.at[pl.ds(0, 2**stages - 1)], hop_send.at[kind])
        sent_all(ref.at[pl.ds(0, 2**stages)], hand_send.at[kind])

    for label in [0, *reversed(range(1, labels))]:

        @pl.loop(0, STEPS)
        def _(h):
            to, _ = target(label, h)
            swap(label, h).wait_recv()
            wider_in[:, to] = came[:, to].astype(jnp.float32)

            @pl.when(low)
            def _():
                store(wider_in, came_sem, label, h, grad_out).start()

            @pl.when(jnp.logical_not(low))
            def _():
                store(wider_in, came_sem, label, h, act_out).start()

    sent_all(sent, out_sem)
    pltpu.make_async_copy(kept, act_out, kept_sem).wait()
    pltpu.make_async_copy(wider_in, grad_out, came_sem).wait()


def cut(length, unit, pieces):
    units = length // unit
    sizes = [(units // pieces + (1 if i < units % pieces else 0)) * unit for i in range(pieces)]
    return [(sum(sizes[:i]), sizes[i]) for i in range(pieces)]


def call(kernel, outs, scratch, *operands):
    return pl.pallas_call(
        kernel,
        out_shape=outs,
        in_specs=[pl.BlockSpec(memory_space=pl.ANY)] * len(operands),
        out_specs=[pl.BlockSpec(memory_space=pl.ANY)] * len(outs),
        scratch_shapes=scratch,
        compiler_params=pltpu.CompilerParams(
            collective_id=0, has_side_effects=True, vmem_limit_bytes=63 * 1024 * 1024
        ),
    )(*operands)


def split_body(tok, blk, activations, out_grads):
    depth, feats = activations.shape
    tokens = depth * tok
    width = feats * blk
    rows = width // (tok * blk)
    count = COUNT
    wide = feats // CUTS
    bf16, f32 = jnp.bfloat16, jnp.float32
    dma = pltpu.SemaphoreType.DMA
    steps = blk * STEPS
    return call(
        functools.partial(factor_kernel, tok, blk, tokens),
        [jax.ShapeDtypeStruct((rows, width), f32)] * 2,
        [
            pltpu.VMEM((blk, 2, depth, feats), bf16),
            pltpu.VMEM((depth, feats), bf16),
            pltpu.VMEM((depth, feats), bf16),
            pltpu.VMEM((4, feats // 2, 2 * depth), bf16),
            pltpu.VMEM((count, 2, 2, rows, wide), bf16),
            pltpu.VMEM((count, 2, 2, rows, wide // 2), bf16),
            pltpu.VMEM((count, 2, rows, wide // 2), bf16),
            pltpu.VMEM((count, 2, rows, wide // 2), bf16),
            pltpu.VMEM((count, 2, rows, wide // 2), f32),
            pltpu.VMEM((2 * tok, 3 * rows, feats), bf16),
            pltpu.VMEM((2 * tok, 2 * rows, feats // CUTS * SHORT), bf16),
            pltpu.VMEM((2 * rows, width), bf16),
            pltpu.VMEM((2 * rows, width), f32),
            pltpu.VMEM((2 * rows, width), bf16),
            pltpu.VMEM((2 * rows, width), bf16),
            pltpu.VMEM((1, width), f32),
            pltpu.VMEM((rows, width), bf16),
            pltpu.VMEM((rows, width), f32),
            pltpu.VMEM((rows, width), bf16),
            pltpu.VMEM((rows, width), f32),
            dma((2,)),
            dma, dma((blk, CUTS)), dma, dma((CUTS,)), dma, dma((blk, CUTS)),
            dma, dma((count,)), dma, dma((count,)),
            dma((2,)), dma((4, 8)), dma((2,)), dma((4,)),
            dma, dma((steps,)), dma, dma,
        ],
        activations, out_grads,
    )


def solution(mesh):
    tok, blk = mesh.shape["tok"], mesh.shape["blk"]
    placed = (P("tok", "blk"), P("tok", "blk"))

    def body(activations, out_grads):
        depth, feats = activations.shape
        whole = max(depth * tok, feats * blk) * feats * blk * activations.dtype.itemsize
        cube = tok == 2 * blk and blk == 4 and feats == tok * LANES == 2 * depth
        if whole <= gathered_budget and cube:
            return split_body(tok, blk, activations, out_grads)
        return tiled_body(activations, out_grads)

    return jax.shard_map(
        body,
        mesh=mesh,
        in_specs=placed,
        out_specs=(P(("tok", "blk"), None), P(("tok", "blk"), None)),
        check_vma=False,
    )
```
